256 devices in a mesh: ga: 256 (over z, y, x, core).
Axes of the slice: x: 4, y: 4, z: 8, core: 2. Of those that a mesh axis runs over, the one named last changes fastest.
Arguments:
- text_states: bfloat16 [4096, 512], P('ga')
- text_proj: bfloat16 [512, 1024], replicated
- gallery: bfloat16 [131072, 1024], P('ga')
- logit_scale: float32 [1], replicated
Outputs:
- output 1: bfloat16 [4096, 131072], P(None, 'ga')
- output 2: float32 [4096], replicated
All inputs are finite; a program needn't handle non-finite values.
Results may differ from the reference program's by a relative error of at most 0.0023.
Values are sent between devices in bfloat16 or wider.
A program may use at most 768 MiB of HBM per device.

```python
import jax
import jax.numpy as jnp
from jax import lax

QUERIES = 4096
GALLERY = 131072
WT = 512
EMB = 1024
QBLOCK = 16


def setup_inputs(seed: int = 0) -> dict:
    base_key = jax.random.key(seed)
    k_text, k_proj, k_noise, k_dirs, k_scale = jax.random.split(base_key, 5)
    text_states = jax.random.normal(k_text, (QUERIES, WT), jnp.float32)
    text_proj = jax.random.normal(k_proj, (WT, EMB), jnp.float32) * WT ** -0.5
    anchors = jax.random.normal(k_dirs, (2, EMB), jnp.float32)
    anchors = anchors / jnp.sqrt(jnp.sum(anchors * anchors, axis=1, keepdims=True))
    angles = jnp.pi * jnp.arange(GALLERY, dtype=jnp.float32) / GALLERY
    gallery = (jax.random.normal(k_noise, (GALLERY, EMB), jnp.float32) * EMB ** -0.5
               + jnp.cos(angles)[:, None] * anchors[0] + jnp.sin(angles)[:, None] * anchors[1])
    gallery = gallery / jnp.sqrt(jnp.sum(gallery * gallery, axis=1, keepdims=True))
    logit_scale = (0.5 * jnp.log(2.0 * EMB) + jnp.log(1.5)
                   + jax.random.uniform(k_scale, (1,), jnp.float32, -0.2, 0.2)).astype(jnp.float32)
    return {
        "text_states": text_states.astype(jnp.bfloat16),
        "text_proj": text_proj.astype(jnp.bfloat16),
        "gallery": gallery.astype(jnp.bfloat16),
        "logit_scale": logit_scale,
    }


def reference(text_states, text_proj, gallery, logit_scale):
    proj_out = jnp.dot(text_states, text_proj, preferred_element_type=jnp.float32)
    unit_q = proj_out / jnp.sqrt(jnp.sum(proj_out * proj_out, axis=1, keepdims=True))
    query_emb = unit_q.astype(jnp.bfloat16)
    logit_mult = jnp.exp(logit_scale[0])
    positions = jnp.arange(GALLERY, dtype=jnp.float32) / GALLERY
    blocks = query_emb.reshape(QUERIES // QBLOCK, QBLOCK, EMB)

    def score_block(query_block):
        scores = logit_mult * jnp.dot(query_block, gallery.T, preferred_element_type=jnp.float32)
        row_max = jnp.max(scores, axis=1, keepdims=True)
        exp_vals = jnp.exp(scores - row_max)
        prob_vals = exp_vals / jnp.sum(exp_vals, axis=1, keepdims=True)
        return prob_vals.astype(jnp.bfloat16), jnp.sum(prob_vals * positions, axis=1)

    prob_blocks, rank_blocks = lax.map(score_block, blocks)
    return prob_blocks.reshape(QUERIES, GALLERY), rank_blocks.reshape(QUERIES)
```

```python
import functools

import jax
import jax.numpy as jnp
from jax import lax
from jax.experimental import pallas as pl
from jax.experimental.pallas import tpu as pltpu
from jax.sharding import PartitionSpec as P

MESH = pl.DeviceIdType.MESH
NX, NY, NZ, NC = 4, 4, 8, 2
F32, BF16 = jnp.float32, jnp.bfloat16


def gather_score_kernel(x_hbm, w_hbm, g_hbm, t_ref,
                        e_ref, fac_ref, rank_ref,
                        xs, wv, gv, stat, part, zpart, done,
                        in_sem, x_send, x_recv, y_send, y_recv,
                        r_send, r_recv, l_send, l_recv, d_send, d_recv,
                        s1_send, s1_recv, s2_send, s2_recv, s3_send, s3_recv):
    me = lax.axis_index("ga")
    c = lax.rem(me, NC)
    x = lax.rem(me // 2, NX)
    y = lax.rem(me // 8, NY)
    z = me // 32
    pi = lax.rem(me, 32)

    def dev(zz, yy, xx, cc):
        return ((zz * NY + yy) * NX + xx) * NC + cc

    load_x = pltpu.make_async_copy(x_hbm, xs.at[z, y, x, c], in_sem.at[0])
    load_w = pltpu.make_async_copy(w_hbm, wv, in_sem.at[1])
    load_g = pltpu.make_async_copy(g_hbm, gv, in_sem.at[2])
    load_x.start()
    load_w.start()
    load_g.start()

    zr = lax.rem(z + 1, NZ)
    zl = lax.rem(z + NZ - 1, NZ)
    sib = dev(z, y, x, 1 - c)
    x_peers = [dev(z, y, lax.rem(x + d, NX), c) for d in range(1, NX)]
    y_peers = [dev(z, lax.rem(y + d, NY), x, c) for d in range(1, NY)]
    right, left = dev(zr, y, x, c), dev(zl, y, x, c)

    barrier = pltpu.get_barrier_semaphore()
    for p in [sib, right, left] + x_peers + y_peers:
        pl.semaphore_signal(barrier, inc=1, device_id=(p,), device_id_type=MESH)
    pl.semaphore_wait(barrier, 9)
    load_x.wait()

    def rcopy(src, dst, ss, rs, p):
        return pltpu.make_async_remote_copy(src_ref=src, dst_ref=dst, send_sem=ss, recv_sem=rs,
                                            device_id=(p,), device_id_type=MESH)

    own = xs.at[z, y, x, c]
    for d in range(1, NX):
        rcopy(own, own, x_send.at[d - 1], x_recv.at[d - 1], x_peers[d - 1]).start()

    def row(zz, j):
        return xs.at[zz, lax.rem(y + j, NY), :, c]

    def to_right(zz, s, j):
        return rcopy(row(zz, j), row(zz, j), r_send.at[s * 4 + j], r_recv.at[s * 4 + j], right)

    def to_left(zz, s, j):
        return rcopy(row(zz, j), row(zz, j), l_send.at[s * 4 + j], l_recv.at[s * 4 + j], left)

    def to_sib(zz, p, j):
        return rcopy(row(zz, j), row(zz, j), d_send.at[p * 4 + j], d_recv.at[p * 4 + j], sib)

    for d in range(1, NX):
        rcopy(own, own, x_send.at[d - 1], x_recv.at[d - 1], x_peers[d - 1]).wait_recv()
    my_row = row(z, 0)
    for d in range(1, NY):
        rcopy(my_row, my_row, y_send.at[d - 1], y_recv.at[NY - d - 1], y_peers[d - 1]).start()
    to_right(z, 0, 0).start()
    to_left(z, 0, 0).start()
    to_sib(z, 0, 0).start()
    for j in range(1, NY):
        rcopy(row(z, j), row(z, j), y_send.at[0], y_recv.at[j - 1], sib).wait_recv()
        to_right(z, 0, j).start()
        to_left(z, 0, j).start()
        to_sib(z, 0, j).start()

    load_w.wait()
    load_g.wait()
    mult = jnp.exp(t_ref[...])
    col = lax.broadcasted_iota(jnp.int32, (1, 512), 1) + me * 512
    pos = col.astype(F32) / (256 * 512.0)
    lane = lax.broadcasted_iota(jnp.int32, (256, 128), 1)

    def unit(u):
        a = u - 2
        s = a // 4
        jr = lax.rem(jnp.maximum(a, 0), 4)
        head = u < 2
        last = u >= 14
        z1 = jnp.where(head, z, lax.rem(z + 2 * NZ - 1 - s, NZ))
        z2 = jnp.where(head, z, lax.rem(z + 1 + s, NZ))
        j1 = jnp.where(head, 2 * u, jr)
        j2 = jnp.where(head, 2 * u + 1, jnp.where(last, jr + 2, jr))
        p1 = jnp.where(head, 0, jnp.where(last, 7, 1 + s))
        p2 = jnp.where(head, 0, jnp.where(last, 7, 4 + s))
        return (z1, j1, p1), (z2, j2, p2)

    def wait_sib(zz, p, j):
        other = xs.at[zz, lax.rem(y + j, NY), :, 1 - c]
        rcopy(other, other, d_send.at[p * 4 + j], d_recv.at[p * 4 + j], sib).wait_recv()

    def owner_copy(gq):
        return rcopy(stat.at[gq], part.at[pi], s1_send.at[gq], s1_recv.at[pi], z * 32 + gq)

    def send_stats(u):
        for zz, j, _ in unit(u):
            gq = zz * 4 + lax.rem(y + j, NY)

            @pl.when(gq != pi)
            def _():
                owner_copy(gq).start()

            @pl.when(gq == pi)
            def _():
                part[pi] = stat[pi]

    def compute(u):
        (z1, j1, p1), (z2, j2, p2) = unit(u)
        wait_sib(z1, p1, j1)
        wait_sib(z2, p2, j2)
        y1, y2 = lax.rem(y + j1, NY), lax.rem(y + j2, NY)
        rows = jnp.concatenate([xs[z1, y1].reshape(128, 512), xs[z2, y2].reshape(128, 512)], axis=0)
        proj = jnp.dot(rows, wv[...], preferred_element_type=F32)
        inv = 1.0 / jnp.sqrt(jnp.sum(proj * proj, axis=1, keepdims=True))
        q = (proj * inv).astype(BF16)
        sc = mult * lax.dot_general(q, gv[...], (((1,), (1,)), ((), ())), preferred_element_type=F32)
        m = jnp.max(sc, axis=1, keepdims=True)
        ev = jnp.exp(sc - m)
        zs = jnp.sum(ev, axis=1, keepdims=True)
        rs = jnp.sum(ev * pos, axis=1, keepdims=True)
        e_ref[z1 * 4 + y1] = ev[:128]
        e_ref[z2 * 4 + y2] = ev[128:]
        cols = jnp.where(lane == 0, m, jnp.where(lane == 1, zs, rs))
        stat[z1 * 4 + y1] = cols[:128].T[:8]
        stat[z2 * 4 + y2] = cols[128:].T[:8]

    def body(i, carry):
        @pl.when(i < 14)
        def _():
            s = i // 4
            j1 = lax.rem(i, 4)
            j2 = jnp.where(i >= 12, j1 + 2, j1)
            z1 = lax.rem(z + 2 * NZ - 1 - s, NZ)
            z2 = lax.rem(z + 1 + s, NZ)
            to_right(z1, s, j1).wait_recv()

            @pl.when(jnp.logical_or(i < 8, jnp.logical_and(i < 12, j1 < 2)))
            def _():
                to_right(z1, s + 1, j1).start()

            to_sib(z1, jnp.where(i >= 12, 7, 1 + s), j1).start()
            to_left(z2, s, j2).wait_recv()

            @pl.when(jnp.logical_or(i < 8, jnp.logical_and(i < 12, j2 >= 2)))
            def _():
                to_left(z2, s + 1, j2).start()

            to_sib(z2, jnp.where(i >= 12, 7, 4 + s), j2).start()

        compute(i)

        @pl.when(i >= 1)
        def _():
            send_stats(i - 1)

        return carry

    lax.fori_loop(0, 16, body, 0)
    send_stats(15)

    def wait_part(k, carry):
        @pl.when(k != pi)
        def _():
            rcopy(part.at[k], part.at[k], s1_send.at[0], s1_recv.at[k], sib).wait_recv()
        return carry

    lax.fori_loop(0, 32, wait_part, 0)

    def merge(ref):
        ms = ref[:, 0, :]
        m = jnp.max(ms, axis=0, keepdims=True)
        wgt = jnp.exp(ms - m)
        return m, jnp.sum(wgt * ref[:, 1, :], axis=0, keepdims=True), jnp.sum(wgt * ref[:, 2, :], axis=0, keepdims=True)

    sub = lax.broadcasted_iota(jnp.int32, (8, 128), 0)

    def tile(a, b, d):
        return jnp.where(sub == 0, a, jnp.where(sub == 1, b, d))

    t1 = tile(*merge(part))
    zpart[z] = t1
    z_peers = [dev(lax.rem(z + d, NZ), y, x, c) for d in range(1, NZ)]
    for d in range(1, NZ):
        rcopy(zpart.at[z], zpart.at[z], s2_send.at[d - 1], s2_recv.at[NZ - d - 1], z_peers[d - 1]).start()
    for d in range(1, NZ):
        zz = lax.rem(z + d, NZ)
        rcopy(zpart.at[zz], zpart.at[zz], s2_send.at[d - 1], s2_recv.at[d - 1], sib).wait_recv()
    m, zs, rs = merge(zpart)
    done[pi] = tile(m, 1.0 / zs, rs / zs)

    def send_done(k, carry):
        p = lax.rem(pi + k, 32)
        rcopy(done.at[pi], done.at[pi], s3_send.at[k - 1], s3_recv.at[31 - k], z * 32 + p).start()
        return carry

    lax.fori_loop(1, 32, send_done, 0)

    def wait_done(k, carry):
        p = lax.rem(pi + k, 32)
        rcopy(done.at[p], done.at[p], s3_send.at[k - 1], s3_recv.at[k - 1], sib).wait_recv()
        return carry

    lax.fori_loop(1, 32, wait_done, 0)
    fac_ref[...] = jnp.exp(stat[:, 0, :] - done[:, 0, :]) * done[:, 1, :]
    rank_ref[...] = done[:, 2, :]

    for d in range(1, NX):
        rcopy(own, own, x_send.at[d - 1], x_recv.at[d - 1], sib).wait_send()
        rcopy(my_row, my_row, y_send.at[d - 1], y_recv.at[d - 1], sib).wait_send()
    for d in range(1, NZ):
        rcopy(zpart.at[z], zpart.at[z], s2_send.at[d - 1], s2_recv.at[d - 1], sib).wait_send()

    def drain(k, carry):
        rcopy(my_row, my_row, d_send.at[k], d_recv.at[k], sib).wait_send()

        @pl.when(k < 14)
        def _():
            rcopy(my_row, my_row, r_send.at[k], r_recv.at[k], sib).wait_send()

        @pl.when(jnp.logical_or(k < 12, jnp.logical_and(k >= 14, k < 16)))
        def _():
            rcopy(my_row, my_row, l_send.at[k], l_recv.at[k], sib).wait_send()

        @pl.when(k != pi)
        def _():
            rcopy(stat.at[k], part.at[k], s1_send.at[k], s1_recv.at[k], sib).wait_send()

        @pl.when(k < 31)
        def _():
            rcopy(stat.at[k], part.at[k], s3_send.at[k], s3_recv.at[k], sib).wait_send()
        return carry

    lax.fori_loop(0, 32, drain, 0)


def normalise_kernel(e_ref, fac_ref, rank_ref, p_ref, r_ref):
    i = pl.program_id(0)

    def body(k, carry):
        gq = i * 4 + k
        f = jnp.broadcast_to(fac_ref[pl.ds(gq, 1), :], (128, 128)).T
        ev = e_ref[gq]
        for b in range(4):
            p_ref[pl.ds(k * 128, 128), b * 128:(b + 1) * 128] = (ev[:, b * 128:(b + 1) * 128] * f).astype(BF16)
        return carry

    lax.fori_loop(0, 4, body, 0)
    r_ref[...] = rank_ref[...]


def solution(mesh):
    D = pltpu.SemaphoreType.DMA
    VM = pltpu.VMEM

    def per_device(text_states, text_proj, gallery, logit_scale):
        e, fac, rank = pl.pallas_call(
            gather_score_kernel,
            out_shape=(VM((32, 128, 512), F32), VM((32, 128), F32), VM((32, 128), F32)),
            in_specs=[pl.BlockSpec(memory_space=pl.ANY)] * 3 + [pl.BlockSpec(memory_space=VM)],
            out_specs=(pl.BlockSpec(memory_space=VM),) * 3,
            scratch_shapes=[
                VM((NZ, NY, NX, NC, 16, 512), BF16), VM((512, 1024), BF16), VM((512, 1024), BF16),
                VM((32, 8, 128), F32), VM((32, 8, 128), F32), VM((NZ, 8, 128), F32),
                VM((32, 8, 128), F32),
                D((3,)), D((3,)), D((3,)), D((3,)), D((3,)),
                D((16,)), D((16,)), D((16,)), D((16,)), D((32,)), D((32,)),
                D((32,)), D((32,)), D((7,)), D((7,)), D((31,)), D((31,)),
            ],
            compiler_params=pltpu.CompilerParams(collective_id=0, has_side_effects=True,
                                                 vmem_limit_bytes=48 * 1024 * 1024),
        )(text_states, text_proj, gallery, logit_scale.reshape(1, 1))
        prob, rank = pl.pallas_call(
            normalise_kernel,
            grid=(8,),
            out_shape=(jax.ShapeDtypeStruct((4096, 512), BF16), jax.ShapeDtypeStruct((32, 128), F32)),
            in_specs=[pl.BlockSpec(memory_space=VM)] * 3,
            out_specs=(pl.BlockSpec((512, 512), lambda i: (i, 0)), pl.BlockSpec((32, 128), lambda i: (0, 0))),
            compiler_params=pltpu.CompilerParams(vmem_limit_bytes=24 * 1024 * 1024),
        )(e, fac, rank)
        return prob, rank.reshape(4096)

    return jax.shard_map(per_device, mesh=mesh,
                         in_specs=(P("ga", None), P(None, None), P("ga", None), P(None)),
                         out_specs=(P(None, "ga"), P(None)), check_vma=False)
```

```python
import jax
import jax.numpy as jnp
from jax import lax
from jax.experimental import pallas as pl
from jax.experimental.pallas import tpu as pltpu
from jax.sharding import PartitionSpec as P

MESH = pl.DeviceIdType.MESH
NX, NY, NZ, NC = 4, 4, 8, 2
F32, BF16 = jnp.float32, jnp.bfloat16
LOG2E = 1.4426950408889634
F32_MAX = 3.4028235e38
scope = jax.named_scope


def rcopy(src, dst, ss, rs, p):
    return pltpu.make_async_remote_copy(src_ref=src, dst_ref=dst, send_sem=ss, recv_sem=rs,
                                        device_id=(p,), device_id_type=MESH)


def gather_score_kernel(x_hbm, w_hbm, g_hbm, t_ref,
                        e_ref, fac_ref, rank_ref,
                        xs, wv, gv, qown, qsib, stat, part, zpart, done,
                        in_sem, a_send, a_recv, y_send, y_recv,
                        r_send, r_recv, l_send, l_recv, q_send, q_recv,
                        s1_send, s1_recv, s2_send, s2_recv, s3_send, s3_recv):
    me = lax.axis_index("ga")
    c = lax.rem(me, NC)
    x = lax.rem(me // 2, NX)
    y = lax.rem(me // 8, NY)
    z = me // 32
    pi = lax.rem(me, 32)
    core0, core1 = c == 0, c == 1

    def dev(zz, yy, xx, cc):
        return ((zz * NY + yy) * NX + xx) * NC + cc

    def own_block():
        return (jnp.where(core0, z, 2 * x + z // 4), jnp.where(core0, y, lax.rem(z, 4)), jnp.where(core0, x, y))

    u0, u1, u2 = own_block()
    own = xs.at[u0, u1, u2]
    load_x = pltpu.make_async_copy(x_hbm, own, in_sem.at[0])
    load_w = pltpu.make_async_copy(w_hbm, wv, in_sem.at[1])
    load_g = pltpu.make_async_copy(g_hbm, gv, in_sem.at[2])
    load_x.start()
    load_w.start()
    load_g.start()

    sib = dev(z, y, x, 1 - c)
    x_peers = [dev(z, y, lax.rem(x + d, NX), c) for d in range(1, NX)]
    y_peers = [dev(z, lax.rem(y + d, NY), x, c) for d in range(1, NY)]
    z_peers = [dev(lax.rem(z + d, NZ), y, x, c) for d in range(1, NZ)]

    barrier = pltpu.get_barrier_semaphore()

    def greet(peers):
        for p in peers:
            pl.semaphore_signal(barrier, inc=1, device_id=(p,), device_id_type=MESH)
        pl.semaphore_wait(barrier, len(peers))

    with scope("barrier"):
        @pl.when(core0)
        def _():
            greet([sib] + x_peers + y_peers + [z_peers[0], z_peers[-1]])

        @pl.when(core1)
        def _():
            greet([sib] + z_peers + y_peers + [x_peers[0], x_peers[-1]])

        load_x.wait()

    def row(zz, j):
        return xs.at[zz, lax.rem(y + j, NY)]

    def a_right(zz, k, j):
        return rcopy(row(zz, j), row(zz, j), r_send.at[k], r_recv.at[k], z_peers[0])

    def a_left(zz, k, j):
        return rcopy(row(zz, j), row(zz, j), l_send.at[k], l_recv.at[k], z_peers[-1])

    @pl.when(core0)
    def _():
        for d in range(1, NX):
            rcopy(own, own, a_send.at[d - 1], a_recv.at[d - 1], x_peers[d - 1]).start()
        with scope("first"):
            for d in range(1, NX):
                rcopy(own, own, a_send.at[d - 1], a_recv.at[d - 1], x_peers[d - 1]).wait_recv()
        for d in range(1, NY):
            rcopy(row(z, 0), row(z, 0), y_send.at[d - 1], y_recv.at[NY - d - 1], y_peers[d - 1]).start()
        a_right(z, 0, 0).start()
        a_left(z, 0, 0).start()
        for j in range(1, NY):
            with scope("second"):
                rcopy(row(z, j), row(z, j), y_send.at[0], y_recv.at[j - 1], sib).wait_recv()
            a_right(z, j, j).start()
            a_left(z, j, j).start()

    def a_event(e, carry):
        s = e // 4
        j1 = lax.rem(e, 4)
        j2 = jnp.where(e >= 12, j1 + 2, j1)
        z1 = lax.rem(z + 2 * NZ - 1 - s, NZ)
        z2 = lax.rem(z + 1 + s, NZ)
        a_right(z1, s * 4 + j1, j1).wait_recv()

        @pl.when(jnp.logical_or(e < 8, jnp.logical_and(e < 12, j1 < 2)))
        def _():
            a_right(z1, s * 4 + 4 + j1, j1).start()

        a_left(z2, s * 4 + j2, j2).wait_recv()

        @pl.when(jnp.logical_or(e < 8, jnp.logical_and(e < 12, j2 >= 2)))
        def _():
            a_left(z2, s * 4 + 4 + j2, j2).start()

        return carry

    def piece(xx, h, j):
        return xs.at[2 * xx + h, :, lax.rem(y + j, NY)]

    def b_right(xx, h, k, j):
        return rcopy(piece(xx, h, j), piece(xx, h, j), r_send.at[k], r_recv.at[k], x_peers[0])

    def b_left(xx, h, k, j):
        return rcopy(piece(xx, h, j), piece(xx, h, j), l_send.at[k], l_recv.at[k], x_peers[-1])

    @pl.when(core1)
    def _():
        for d in range(1, NZ):
            rcopy(own, own, a_send.at[d - 1], a_recv.at[NZ - d - 1], z_peers[d - 1]).start()
        with scope("first"):
            for d in range(1, NZ):
                rcopy(own, own, a_send.at[d - 1], a_recv.at[d - 1], z_peers[d - 1]).wait_recv()
        for h in range(2):
            for d in range(1, NY):
                rcopy(piece(x, h, 0), piece(x, h, 0), y_send.at[h * 3 + d - 1], y_recv.at[h * 3 + NY - d - 1],
                      y_peers[d - 1]).start()
            b_right(x, h, h * 4, 0).start()
            b_left(x, h, h * 4, 0).start()
        for h in range(2):
            for j in range(1, NY):
                with scope("second"):
                    rcopy(piece(x, h, j), piece(x, h, j), y_send.at[0], y_recv.at[h * 3 + j - 1], sib).wait_recv()
                b_right(x, h, h * 4 + j, j).start()
                b_left(x, h, h * 4 + j, j).start()

    def b_event(e, carry):
        j = lax.rem(e, 4)
        far = e >= 8
        xr = jnp.where(far, lax.rem(x + 2, NX), lax.rem(x + 3, NX))
        xl = jnp.where(far, lax.rem(x + 2, NX), lax.rem(x + 1, NX))
        hr = jnp.where(far, 0, e // 4)
        hl = jnp.where(far, 1, e // 4)
        b_right(xr, hr, e, j).wait_recv()

        @pl.when(e < 4)
        def _():
            b_right(xr, hr, 8 + j, j).start()

        b_left(xl, hl, e, j).wait_recv()

        @pl.when(jnp.logical_and(e >= 4, e < 8))
        def _():
            b_left(xl, hl, 8 + j, j).start()

        return carry

    def events(k):
        with scope("events"):
            @pl.when(core0)
            def _():
                lo = jnp.where(k == 1, 0, jnp.minimum(2 * k, k + 6))
                hi = jnp.minimum(2 * k + 2, k + 7)
                lax.fori_loop(lo, hi, a_event, 0)

            @pl.when(core1)
            def _():
                lax.fori_loop(jnp.minimum(2 * k - 2, 12), jnp.minimum(2 * k, 12), b_event, 0)

    def unit_of(cc0, u):
        odd = lax.rem(u, 2) == 1
        dz = jnp.where(odd, -((u + 1) // 2), (u + 1) // 2)
        za = lax.rem(z + dz + 2 * NZ, NZ)
        dx = jnp.where(u < 2, 0, jnp.where(u >= 6, 2, jnp.where(odd, 1, NX - 1)))
        h = jnp.where(u < 2, u, jnp.where(u >= 6, u - 6, (u - 2) // 2))
        ub = 2 * lax.rem(x + dx, NX) + h
        return jnp.where(cc0, za, ub), jnp.where(cc0, 2 * za, 16 + 2 * ub)

    load_w.wait()
    load_g.wait()
    k2 = jnp.minimum(jnp.exp(t_ref[...]) * LOG2E, F32_MAX)
    col = lax.broadcasted_iota(jnp.int32, (1, 512), 1) + me * 512
    pos = col.astype(F32) / (256 * 512.0)

    def project(u):
        rows = xs[unit_of(core0, u)[0]].reshape(256, 512)
        proj = jnp.dot(rows, wv[...], preferred_element_type=F32)
        inv = 1.0 / jnp.sqrt(jnp.sum(proj * proj, axis=1, keepdims=True))
        qown[u] = (proj * inv).astype(BF16)

    def to_sib(u):
        return rcopy(qown.at[u], qsib.at[u], q_send.at[u], q_recv.at[u], sib)

    def score(q, bases):
        n = 256 * len(bases)
        lane = lax.broadcasted_iota(jnp.int32, (n, 128), 1)
        d = lax.dot_general(q, gv[...], (((1,), (1,)), ((), ())), preferred_element_type=F32)
        dm = jnp.max(d, axis=1, keepdims=True)
        ev = jnp.exp2((d - dm) * k2)
        zs = jnp.sum(ev, axis=1, keepdims=True)
        rs = jnp.sum(ev * pos, axis=1, keepdims=True)
        cols = jnp.where(lane == 0, dm, jnp.where(lane == 1, zs, rs))
        for i, base in enumerate(bases):
            for b in range(2):
                rows = slice(i * 256 + b * 128, i * 256 + b * 128 + 128)
                e_ref[base + b] = ev[rows]
                stat[base + b] = cols[rows].T[:8]

    def base_own(u):
        return unit_of(core0, u)[1]

    def base_sib(u):
        return unit_of(core1, u)[1]

    def score_both(uo, us):
        score(jnp.concatenate([qown[uo], qsib[us]], axis=0), [base_own(uo), base_sib(us)])

    def send_group(gq):
        @pl.when(gq != pi)
        def _():
            rcopy(stat.at[gq], part.at[pi], s1_send.at[gq], s1_recv.at[pi], z * 32 + gq).start()

        @pl.when(gq == pi)
        def _():
            part[pi] = stat[pi]

    def send_own(u, carry):
        send_group(base_own(u))
        send_group(base_own(u) + 1)
        return carry

    def send_sib(u, carry):
        send_group(base_sib(u))
        send_group(base_sib(u) + 1)
        return carry

    project(0)
    to_sib(0).start()
    events(1)
    project(1)
    to_sib(1).start()
    score(qown[0], [base_own(0)])

    def body(k, carry):
        events(k)
        with scope("sibwait"):
            to_sib(k - 2).wait_recv()
        with scope("compute"):
            score_both(k - 1, k - 2)
            project(k)
        to_sib(k).start()

        @pl.when(k >= 5)
        def _():
            lax.fori_loop(jnp.where(k == 5, 0, k - 2), k - 1, send_own, 0)
            lax.fori_loop(jnp.where(k == 5, 0, k - 3), k - 2, send_sib, 0)

        return carry

    lax.fori_loop(2, 8, body, 0)
    with scope("tail6"):
        to_sib(6).wait_recv()
        score_both(7, 6)
    lax.fori_loop(6, 8, send_own, 0)
    lax.fori_loop(5, 7, send_sib, 0)
    with scope("tail7"):
        to_sib(7).wait_recv()
        score(qsib[7], [base_sib(7)])
    send_sib(7, 0)

    def wait_part(k, carry):
        @pl.when(k != pi)
        def _():
            rcopy(part.at[k], part.at[k], s1_send.at[0], s1_recv.at[k], sib).wait_recv()
        return carry

    with scope("s1wait"):
        lax.fori_loop(0, 32, wait_part, 0)

    def merge(ref):
        ms = ref[:, 0, :]
        m = jnp.max(ms, axis=0, keepdims=True)
        wgt = jnp.exp2((ms - m) * k2)
        return m, jnp.sum(wgt * ref[:, 1, :], axis=0, keepdims=True), jnp.sum(wgt * ref[:, 2, :], axis=0, keepdims=True)

    sub = lax.broadcasted_iota(jnp.int32, (8, 128), 0)

    def tile(a, b, d):
        return jnp.where(sub == 0, a, jnp.where(sub == 1, b, d))

    zpart[z] = tile(*merge(part))
    for d in range(1, NZ):
        rcopy(zpart.at[z], zpart.at[z], s2_send.at[d - 1], s2_recv.at[NZ - d - 1], z_peers[d - 1]).start()
    with scope("s2wait"):
        for d in range(1, NZ):
            zz = lax.rem(z + d, NZ)
            rcopy(zpart.at[zz], zpart.at[zz], s2_send.at[d - 1], s2_recv.at[d - 1], sib).wait_recv()
    m, zs, rs = merge(zpart)
    done[pi] = tile(m, 1.0 / zs, rs / zs)

    def send_done(k, carry):
        p = lax.rem(pi + k, 32)
        rcopy(done.at[pi], done.at[pi], s3_send.at[k - 1], s3_recv.at[31 - k], z * 32 + p).start()
        return carry

    with scope("s3send"):
        lax.fori_loop(1, 32, send_done, 0)

    def wait_done(k, carry):
        p = lax.rem(pi + k, 32)
        rcopy(done.at[p], done.at[p], s3_send.at[k - 1], s3_recv.at[k - 1], sib).wait_recv()
        return carry

    with scope("s3wait"):
        lax.fori_loop(1, 32, wait_done, 0)
    fac_ref[...] = jnp.exp2((stat[:, 0, :] - done[:, 0, :]) * k2) * done[:, 1, :]
    rank_ref[...] = done[:, 2, :]

    def sent(ref, sem):
        rcopy(ref, ref, sem, sem, sib).wait_send()

    with scope("drain"):
        small = xs.at[0, 0, 0]
        line = xs.at[0, 0]

        def drain_lines(k, carry):
            sent(line, r_send.at[k])
            sent(line, l_send.at[k])
            return carry

        lax.fori_loop(0, 8, drain_lines, 0)

        @pl.when(core0)
        def _():
            for d in range(3):
                sent(small, a_send.at[d])
                sent(line, y_send.at[d])
            for k in range(8, 12):
                sent(line, r_send.at[k])
                sent(line, l_send.at[k])
            for k in range(12, 14):
                sent(line, r_send.at[k])
                sent(line, l_send.at[k + 2])

        @pl.when(core1)
        def _():
            for d in range(7):
                sent(small, a_send.at[d])
            for d in range(6):
                sent(line, y_send.at[d])
            for k in range(8, 12):
                sent(line, r_send.at[k])
                sent(line, l_send.at[k])

        for d in range(1, NZ):
            sent(zpart.at[0], s2_send.at[d - 1])

        def drain_q(k, carry):
            sent(qown.at[0], q_send.at[k])
            return carry

        lax.fori_loop(0, 8, drain_q, 0)

        def drain(k, carry):
            @pl.when(k != pi)
            def _():
                sent(stat.at[0], s1_send.at[k])

            @pl.when(k < 31)
            def _():
                sent(stat.at[0], s3_send.at[k])
            return carry

        lax.fori_loop(0, 32, drain, 0)


def normalise_kernel(e_ref, fac_ref, rank_ref, p_hbm, r_ref, buf, nat, sem):
    def scaled(gq):
        f = jnp.broadcast_to(fac_ref[pl.ds(gq, 1), :], (128, 128)).T
        ev = e_ref[gq]
        return jnp.concatenate([ev[:, b * 128:(b + 1) * 128] * f for b in range(4)], axis=1).astype(BF16)

    def out_a(u):
        return pltpu.make_async_copy(buf.at[u], p_hbm.at[u, :, :, 0], sem.at[u])

    def out_b(u):
        return pltpu.make_async_copy(buf.at[8 + u], p_hbm.at[pl.ds(lax.rem(u, 2) * 4, 4), :, u // 2, 1], sem.at[8 + u])

    def body(u, carry):
        for part, base in ((u, 2 * u), (8 + u, 16 + 2 * u)):
            for b in range(2):
                buf[part, 2 * b:2 * b + 2] = scaled(base + b).reshape(2, 4, 16, 512)
        out_a(u).start()
        out_b(u).start()
        return carry

    lax.fori_loop(0, 8, body, 0)

    lane = lax.broadcasted_iota(jnp.int32, (32, 128), 1)
    sub = lax.broadcasted_iota(jnp.int32, (32, 128), 0)
    for n in range(32):
        nat[0, n:n + 1] = rank_ref[pl.ds(n // 2, 1), :]
        for xx in range(NX):
            nat[1 + xx, n:n + 1] = rank_ref[pl.ds(16 + xx * 4 + n // 8, 1), :]
    a = nat[0]
    a = jnp.where(lax.rem(sub, 2) == 0, a, pltpu.roll(a, 64, 1))
    out = jnp.where(lane < 16, a, 0.0)
    for xx in range(1, NX):
        out = jnp.where(lane // 16 == 2 * xx, pltpu.roll(a, 16 * xx, 1), out)
    for xx in range(NX):
        b = nat[1 + xx]
        for s in range(8):
            shift = (xx * 32 + 16 - s * 16) % 128
            r = pltpu.roll(b, shift, 1) if shift else b
            out = jnp.where(jnp.logical_and(lax.rem(sub, 8) == s, lane // 16 == 2 * xx + 1), r, out)
    r_ref[...] = out

    def flush(u, carry):
        out_a(u).wait()
        out_b(u).wait()
        return carry

    lax.fori_loop(0, 8, flush, 0)


def solution(mesh):
    D = pltpu.SemaphoreType.DMA
    VM = pltpu.VMEM

    def per_device(text_states, text_proj, gallery, logit_scale):
        e, fac, rank = pl.pallas_call(
            gather_score_kernel,
            out_shape=(VM((32, 128, 512), F32), VM((32, 128), F32), VM((32, 128), F32)),
            in_specs=[pl.BlockSpec(memory_space=pl.ANY)] * 3 + [pl.BlockSpec(memory_space=VM)],
            out_specs=(pl.BlockSpec(memory_space=VM),) * 3,
            scratch_shapes=[
                VM((8, 4, 4, 16, 512), BF16), VM((512, 1024), BF16), VM((512, 1024), BF16),
                VM((8, 256, 1024), BF16), VM((8, 256, 1024), BF16),
                VM((32, 8, 128), F32), VM((32, 8, 128), F32), VM((NZ, 8, 128), F32), VM((32, 8, 128), F32),
                D((3,)), D((7,)), D((7,)), D((6,)), D((6,)),
                D((16,)), D((16,)), D((16,)), D((16,)), D((8,)), D((8,)),
                D((32,)), D((32,)), D((7,)), D((7,)), D((31,)), D((31,)),
            ],
            compiler_params=pltpu.CompilerParams(collective_id=0, has_side_effects=True,
                                                 vmem_limit_bytes=48 * 1024 * 1024),
        )(text_states, text_proj, gallery, logit_scale.reshape(1, 1))
        prob, rank = pl.pallas_call(
            normalise_kernel,
            out_shape=(jax.ShapeDtypeStruct((NZ, NY, NX, NC, 16, 512), BF16), jax.ShapeDtypeStruct((32, 128), F32)),
            in_specs=[pl.BlockSpec(memory_space=VM)] * 3,
            out_specs=(pl.BlockSpec(memory_space=pl.ANY), pl.BlockSpec(memory_space=VM)),
            scratch_shapes=[VM((16, 4, 4, 16, 512), BF16), VM((5, 32, 128), F32), D((16,))],
            compiler_params=pltpu.CompilerParams(vmem_limit_bytes=24 * 1024 * 1024),
        )(e, fac, rank)
        return prob.reshape(4096, 512), rank.reshape(4096)

    return jax.shard_map(per_device, mesh=mesh,
                         in_specs=(P("ga", None), P(None, None), P("ga", None), P(None)),
                         out_specs=(P(None, "ga"), P(None)), check_vma=False)
```

```python
import jax
import jax.numpy as jnp
from jax import lax
from jax.experimental import pallas as pl
from jax.experimental.pallas import tpu as pltpu
from jax.sharding import PartitionSpec as P

MESH = pl.DeviceIdType.MESH
NX, NY, NZ, NC = 4, 4, 8, 2
F32, BF16 = jnp.float32, jnp.bfloat16
LOG2E = 1.4426950408889634
F32_MAX = 3.4028235e38
scope = jax.named_scope


def rcopy(src, dst, ss, rs, p):
    return pltpu.make_async_remote_copy(src_ref=src, dst_ref=dst, send_sem=ss, recv_sem=rs,
                                        device_id=(p,), device_id_type=MESH)


def gather_score_kernel(x_hbm, w_hbm, g_hbm, t_ref,
                        e_ref, fac_ref, rank_ref,
                        xs, wv, gv, qown, qsib, stat, part, zpart, done,
                        in_sem, a_sem, y_send, y_recv, r_send, r_recv, l_send, l_recv,
                        q_send, q_recv, s_send, s_recv):
    me = lax.axis_index("ga")
    c = lax.rem(me, NC)
    x = lax.rem(me // 2, NX)
    y = lax.rem(me // 8, NY)
    z = me // 32
    pi = lax.rem(me, 32)
    core0 = c == 0
    ml = jnp.where(core0, y, x)
    ll = jnp.where(core0, x, y)

    def dev(zz, yy, xx, cc):
        return ((zz * NY + yy) * NX + xx) * NC + cc

    def dev_lm(zz, lc, mc):
        return dev(zz, jnp.where(core0, mc, lc), jnp.where(core0, lc, mc), c)

    def column(lc, mc):
        return lc * 4 + mc

    mine = column(ll, ml)
    own = xs.at[mine, z]
    load_x = pltpu.make_async_copy(x_hbm, own, in_sem.at[0])
    load_w = pltpu.make_async_copy(w_hbm, wv, in_sem.at[1])
    load_g = pltpu.make_async_copy(g_hbm, gv, in_sem.at[2])
    load_x.start()
    load_w.start()
    load_g.start()

    sib = dev(z, y, x, 1 - c)
    z_peers = [dev(lax.rem(z + d, NZ), y, x, c) for d in range(1, NZ)]
    m_peers = [dev_lm(z, ll, lax.rem(ml + d, 4)) for d in range(1, 4)]
    right = dev_lm(z, lax.rem(ll + 1, 4), ml)
    left = dev_lm(z, lax.rem(ll + 3, 4), ml)

    barrier = pltpu.get_barrier_semaphore()
    with scope("barrier"):
        peers = [sib, right, left] + m_peers + z_peers
        for p in peers:
            pl.semaphore_signal(barrier, inc=1, device_id=(p,), device_id_type=MESH)
        pl.semaphore_wait(barrier, len(peers))
        load_x.wait()

    for d in range(1, NZ):
        rcopy(own, own, a_sem.at[0], a_sem.at[1], z_peers[d - 1]).start()
    with scope("first"):
        rcopy(xs.at[0, 0:7], xs.at[0, 0:7], a_sem.at[0], a_sem.at[1], sib).wait_recv()

    def col(lc, j):
        off = jnp.where(j == 0, 0, jnp.where(j == 1, 1, jnp.where(j == 2, 3, 2)))
        return xs.at[column(lc, lax.rem(ml + off, 4))]

    def to_right(lc, j, e):
        return rcopy(col(lc, j), col(lc, j), r_send.at[0], r_recv.at[e], right)

    def to_left(lc, j, e):
        return rcopy(col(lc, j), col(lc, j), l_send.at[0], l_recv.at[e], left)

    lp, lm, lf = lax.rem(ll + 1, 4), lax.rem(ll + 3, 4), lax.rem(ll + 2, 4)

    for d in range(1, 4):
        rcopy(xs.at[mine], xs.at[mine], y_send.at[0], y_recv.at[3 - d], m_peers[d - 1]).start()
    to_right(ll, 0, 0).start()
    to_left(ll, 0, 0).start()

    def mid(j, off):
        with scope("second"):
            rcopy(col(ll, j), col(ll, j), y_send.at[0], y_recv.at[off - 1], sib).wait_recv()
        to_right(ll, j, j).start()
        to_left(ll, j, j).start()

    def event(e):
        to_right(lm, e, e).wait_recv()

        @pl.when(e < 2)
        def _():
            to_right(lm, e, 4 + e).start()

        to_left(lp, e, e).wait_recv()

        @pl.when(e >= 2)
        def _():
            to_left(lp, e, 2 + e).start()

    def unit_of(lc, mc, u):
        far = u >= 6
        odd = lax.rem(u, 2) == 1
        dl = jnp.where(u < 2, 0, jnp.where(far, 2, jnp.where(odd, 1, 3)))
        second = jnp.logical_or(jnp.logical_or(u == 1, u == 7), jnp.logical_or(u == 4, u == 5))
        m1 = lax.rem(mc + jnp.where(second, 3, 0), 4)
        m2 = lax.rem(mc + jnp.where(second, 2, 1), 4)
        return lax.rem(lc + dl, 4), m1, m2

    load_w.wait()
    load_g.wait()
    k2 = jnp.minimum(jnp.exp(t_ref[...]) * LOG2E, F32_MAX)
    place = lax.broadcasted_iota(jnp.int32, (1, 512), 1) + me * 512
    pos = place.astype(F32) / (256 * 512.0)

    def project(u):
        lc, m1, m2 = unit_of(ll, ml, u)
        rows = jnp.concatenate([xs[column(lc, m1)].reshape(128, 512), xs[column(lc, m2)].reshape(128, 512)], axis=0)
        proj = jnp.dot(rows, wv[...], preferred_element_type=F32)
        inv = 1.0 / jnp.sqrt(jnp.sum(proj * proj, axis=1, keepdims=True))
        qown[u] = (proj * inv).astype(BF16)

    def to_sib(u):
        return rcopy(qown.at[u], qsib.at[u], q_send.at[0], q_recv.at[u], sib)

    def score(q, groups):
        n = 128 * len(groups)
        lane = lax.broadcasted_iota(jnp.int32, (n, 128), 1)
        d = lax.dot_general(q, gv[...], (((1,), (1,)), ((), ())), preferred_element_type=F32)
        dm = jnp.max(d, axis=1, keepdims=True)
        ev = jnp.exp2((d - dm) * k2)
        zs = jnp.sum(ev, axis=1, keepdims=True)
        rs = jnp.sum(ev * pos, axis=1, keepdims=True)
        cols = jnp.where(lane == 0, dm, jnp.where(lane == 1, zs, rs))
        for i, gq in enumerate(groups):
            rows = slice(i * 128, i * 128 + 128)
            e_ref[gq] = ev[rows]
            stat[gq] = cols[rows].T[:8]

    def groups_own(u):
        lc, m1, m2 = unit_of(ll, ml, u)
        return [jnp.where(core0, m * 8 + lc * 2, lc * 8 + m * 2 + 1) for m in (m1, m2)]

    def groups_sib(u):
        lc, m1, m2 = unit_of(ml, ll, u)
        return [jnp.where(core0, lc * 8 + m * 2 + 1, m * 8 + lc * 2) for m in (m1, m2)]

    def score_both(uo, us):
        score(jnp.concatenate([qown[uo], qsib[us]], axis=0), groups_own(uo) + groups_sib(us))

    def send_group(gq):
        @pl.when(gq != pi)
        def _():
            rcopy(stat.at[gq], part.at[pi], s_send.at[0], s_recv.at[0], z * 32 + gq).start()

        @pl.when(gq == pi)
        def _():
            part[pi] = stat[pi]

    def send_own(u, carry):
        for gq in groups_own(u):
            send_group(gq)
        return carry

    def send_sib(u, carry):
        for gq in groups_sib(u):
            send_group(gq)
        return carry

    mid(1, 1)
    mid(2, 3)
    project(0)
    to_sib(0).start()
    mid(3, 2)
    with scope("event0"):
        event(0)
    project(1)
    to_sib(1).start()
    score(qown[0], groups_own(0))

    def body(k, carry):
        with scope("events"):
            @pl.when(k <= 4)
            def _():
                event(k - 1)

            @pl.when(k == 6)
            def _():
                for e in range(4, 6):
                    to_right(lf, e - 4, e).wait_recv()

            @pl.when(k == 7)
            def _():
                for e in range(4, 6):
                    to_left(lf, e - 2, e).wait_recv()

        with scope("sibwait"):
            to_sib(k - 2).wait_recv()
        with scope("compute"):
            score_both(k - 1, k - 2)
            project(k)
        to_sib(k).start()

        @pl.when(k >= 5)
        def _():
            lax.fori_loop(jnp.where(k == 5, 0, k - 2), k - 1, send_own, 0)
            lax.fori_loop(jnp.where(k == 5, 0, k - 3), k - 2, send_sib, 0)

        return carry

    lax.fori_loop(2, 8, body, 0)
    with scope("tail6"):
        to_sib(6).wait_recv()
        score_both(7, 6)
    lax.fori_loop(6, 8, send_own, 0)
    lax.fori_loop(5, 7, send_sib, 0)
    with scope("tail7"):
        to_sib(7).wait_recv()
        score(qsib[7], groups_sib(7))
    send_sib(7, 0)

    with scope("s1wait"):
        rcopy(part.at[0:31], part.at[0:31], s_send.at[0], s_recv.at[0], sib).wait_recv()

    def merge(ref):
        ms = ref[:, 0, :]
        m = jnp.max(ms, axis=0, keepdims=True)
        wgt = jnp.exp2((ms - m) * k2)
        return m, jnp.sum(wgt * ref[:, 1, :], axis=0, keepdims=True), jnp.sum(wgt * ref[:, 2, :], axis=0, keepdims=True)

    sub = lax.broadcasted_iota(jnp.int32, (8, 128), 0)

    def tile(a, b, d):
        return jnp.where(sub == 0, a, jnp.where(sub == 1, b, d))

    zpart[z] = tile(*merge(part))
    for d in range(1, NZ):
        rcopy(zpart.at[z], zpart.at[z], s_send.at[1], s_recv.at[1], z_peers[d - 1]).start()
    with scope("s2wait"):
        rcopy(zpart.at[0:7], zpart.at[0:7], s_send.at[1], s_recv.at[1], sib).wait_recv()
    m, zs, rs = merge(zpart)
    done[pi] = tile(m, 1.0 / zs, rs / zs)

    def send_done(k, carry):
        p = lax.rem(pi + k, 32)
        rcopy(done.at[pi], done.at[pi], s_send.at[2], s_recv.at[2], z * 32 + p).start()
        return carry

    with scope("s3send"):
        lax.fori_loop(1, 32, send_done, 0)

    with scope("s3wait"):
        rcopy(done.at[0:31], done.at[0:31], s_send.at[2], s_recv.at[2], sib).wait_recv()
    fac_ref[...] = jnp.exp2((stat[:, 0, :] - done[:, 0, :]) * k2) * done[:, 1, :]
    rank_ref[...] = done[:, 2, :]

    def sent(ref, sem):
        rcopy(ref, ref, sem, sem, sib).wait_send()

    with scope("drain"):
        sent(xs.at[0, 0:7], a_sem.at[0])
        sent(xs.at[0:3], y_send.at[0])
        sent(xs.at[0:6], r_send.at[0])
        sent(xs.at[0:6], l_send.at[0])
        sent(qown, q_send.at[0])
        sent(part.at[0:31], s_send.at[0])
        sent(zpart.at[0:7], s_send.at[1])
        sent(done.at[0:31], s_send.at[2])


def normalise_kernel(e_ref, fac_ref, rank_ref, p_hbm, r_ref, buf, sem):
    def out(gq):
        return pltpu.make_async_copy(buf.at[gq], p_hbm.at[:, gq], sem.at[gq])

    def body(gq, carry):
        f = jnp.broadcast_to(fac_ref[pl.ds(gq, 1), :], (128, 128)).T
        ev = e_ref[gq]
        p = jnp.concatenate([ev[:, b * 128:(b + 1) * 128] * f for b in range(4)], axis=1)
        buf[gq] = p.astype(BF16).reshape(8, 16, 512)
        out(gq).start()
        return carry

    lax.fori_loop(0, 32, body, 0)

    lane = lax.broadcasted_iota(jnp.int32, (8, 128), 1) // 16
    sub = lax.broadcasted_iota(jnp.int32, (8, 128), 0)
    for yy in range(NY):
        r = rank_ref[yy * 8:yy * 8 + 8]
        nat = r
        for d in range(1, 8):
            moved = pltpu.roll(pltpu.roll(r, 16 * d, 1), 8 - d, 0)
            nat = jnp.where(lax.rem(lane - sub + 8, 8) == d, moved, nat)
        r_ref[pl.ds(yy, 8, stride=4), :] = nat

    def flush(gq, carry):
        out(gq).wait()
        return carry

    lax.fori_loop(0, 32, flush, 0)


def solution(mesh):
    D = pltpu.SemaphoreType.DMA
    VM = pltpu.VMEM

    def per_device(text_states, text_proj, gallery, logit_scale):
        e, fac, rank = pl.pallas_call(
            gather_score_kernel,
            out_shape=(VM((32, 128, 512), F32), VM((32, 128), F32), VM((32, 128), F32)),
            in_specs=[pl.BlockSpec(memory_space=pl.ANY)] * 3 + [pl.BlockSpec(memory_space=VM)],
            out_specs=(pl.BlockSpec(memory_space=VM),) * 3,
            scratch_shapes=[
                VM((16, NZ, 16, 512), BF16), VM((512, 1024), BF16), VM((512, 1024), BF16),
                VM((8, 256, 1024), BF16), VM((8, 256, 1024), BF16),
                VM((32, 8, 128), F32), VM((32, 8, 128), F32), VM((NZ, 8, 128), F32), VM((32, 8, 128), F32),
                D((3,)), D((2,)), D((1,)), D((3,)), D((1,)), D((6,)), D((1,)), D((6,)),
                D((1,)), D((8,)), D((3,)), D((3,)),
            ],
            compiler_params=pltpu.CompilerParams(collective_id=0, has_side_effects=True,
                                                 vmem_limit_bytes=48 * 1024 * 1024),
        )(text_states, text_proj, gallery, logit_scale.reshape(1, 1))
        prob, rank = pl.pallas_call(
            normalise_kernel,
            out_shape=(jax.ShapeDtypeStruct((NZ, 32, 16, 512), BF16), jax.ShapeDtypeStruct((32, 128), F32)),
            in_specs=[pl.BlockSpec(memory_space=VM)] * 3,
            out_specs=(pl.BlockSpec(memory_space=pl.ANY), pl.BlockSpec(memory_space=VM)),
            scratch_shapes=[VM((32, NZ, 16, 512), BF16), D((32,))],
            compiler_params=pltpu.CompilerParams(vmem_limit_bytes=24 * 1024 * 1024),
        )(e, fac, rank)
        return prob.reshape(4096, 512), rank.reshape(4096)

    return jax.shard_map(per_device, mesh=mesh,
                         in_specs=(P("ga", None), P(None, None), P("ga", None), P(None)),
                         out_specs=(P(None, "ga"), P(None)), check_vma=False)
```

```python
import jax
import jax.numpy as jnp
from jax import lax
from jax.experimental import pallas as pl
from jax.experimental.pallas import tpu as pltpu
from jax.sharding import PartitionSpec as P

MESH = pl.DeviceIdType.MESH
NX, NY, NZ, NC = 4, 4, 8, 2
F32, BF16 = jnp.float32, jnp.bfloat16
LOG2E = 1.4426950408889634
F32_MAX = 3.4028235e38
scope = jax.named_scope


def rcopy(src, dst, ss, rs, p):
    return pltpu.make_async_remote_copy(src_ref=src, dst_ref=dst, send_sem=ss, recv_sem=rs,
                                        device_id=(p,), device_id_type=MESH)


def gather_score_kernel(x_hbm, w_hbm, g_hbm, t_ref,
                        e_ref, fac_ref, rank_ref,
                        xs, wv, gv, qown, qsib, da, db, stat, part, zpart, done,
                        in_sem, a_sem, y_send, y_recv, r_send, r_recv, l_send, l_recv,
                        q_send, q_recv, s_send, s_recv):
    me = lax.axis_index("ga")
    c = lax.rem(me, NC)
    x = lax.rem(me // 2, NX)
    y = lax.rem(me // 8, NY)
    z = me // 32
    pi = lax.rem(me, 32)
    core0 = c == 0
    ml = jnp.where(core0, y, x)
    ll = jnp.where(core0, x, y)

    def dev(zz, yy, xx, cc):
        return ((zz * NY + yy) * NX + xx) * NC + cc

    def dev_lm(zz, lc, mc):
        return dev(zz, jnp.where(core0, mc, lc), jnp.where(core0, lc, mc), c)

    def column(lc, mc):
        return lc * 4 + mc

    mine = column(ll, ml)
    own = xs.at[mine, z]
    load_x = pltpu.make_async_copy(x_hbm, own, in_sem.at[0])
    load_w = pltpu.make_async_copy(w_hbm, wv, in_sem.at[1])
    load_g = pltpu.make_async_copy(g_hbm, gv, in_sem.at[2])
    load_x.start()
    load_w.start()
    load_g.start()

    sib = dev(z, y, x, 1 - c)
    z_peers = [dev(lax.rem(z + d, NZ), y, x, c) for d in range(1, NZ)]
    m_peers = [dev_lm(z, ll, lax.rem(ml + d, 4)) for d in range(1, 4)]
    right = dev_lm(z, lax.rem(ll + 1, 4), ml)
    left = dev_lm(z, lax.rem(ll + 3, 4), ml)

    barrier = pltpu.get_barrier_semaphore()
    with scope("barrier"):
        peers = [sib, right, left] + m_peers + z_peers
        for p in peers:
            pl.semaphore_signal(barrier, inc=1, device_id=(p,), device_id_type=MESH)
        pl.semaphore_wait(barrier, len(peers))
        load_x.wait()

    for d in range(1, NZ):
        rcopy(own, own, a_sem.at[0], a_sem.at[1], z_peers[d - 1]).start()
    with scope("first"):
        rcopy(xs.at[0, 0:7], xs.at[0, 0:7], a_sem.at[0], a_sem.at[1], sib).wait_recv()

    def col(lc, j):
        off = jnp.where(j == 0, 0, jnp.where(j == 1, 1, jnp.where(j == 2, 3, 2)))
        return xs.at[column(lc, lax.rem(ml + off, 4))]

    def to_right(lc, j, e):
        return rcopy(col(lc, j), col(lc, j), r_send.at[0], r_recv.at[e], right)

    def to_left(lc, j, e):
        return rcopy(col(lc, j), col(lc, j), l_send.at[0], l_recv.at[e], left)

    lp, lm, lf = lax.rem(ll + 1, 4), lax.rem(ll + 3, 4), lax.rem(ll + 2, 4)

    for d in range(1, 4):
        rcopy(xs.at[mine], xs.at[mine], y_send.at[0], y_recv.at[3 - d], m_peers[d - 1]).start()
    to_right(ll, 0, 0).start()
    to_left(ll, 0, 0).start()

    def mid(j, off):
        with scope("second"):
            rcopy(col(ll, j), col(ll, j), y_send.at[0], y_recv.at[off - 1], sib).wait_recv()
        to_right(ll, j, j).start()
        to_left(ll, j, j).start()

    def event(e):
        to_right(lm, e, e).wait_recv()

        @pl.when(e < 2)
        def _():
            to_right(lm, e, 4 + e).start()

        to_left(lp, e, e).wait_recv()

        @pl.when(e >= 2)
        def _():
            to_left(lp, e, 2 + e).start()

    def unit_of(lc, mc, u):
        far = u >= 6
        odd = lax.rem(u, 2) == 1
        dl = jnp.where(u < 2, 0, jnp.where(far, 2, jnp.where(odd, 1, 3)))
        second = jnp.logical_or(jnp.logical_or(u == 1, u == 7), jnp.logical_or(u == 4, u == 5))
        m1 = lax.rem(mc + jnp.where(second, 3, 0), 4)
        m2 = lax.rem(mc + jnp.where(second, 2, 1), 4)
        return lax.rem(lc + dl, 4), m1, m2

    load_w.wait()
    load_g.wait()
    k2 = jnp.minimum(jnp.exp(jnp.full((1, 1), t_ref[0], F32)) * LOG2E, F32_MAX)
    place = lax.broadcasted_iota(jnp.int32, (1, 512), 1) + me * 512
    pos = place.astype(F32) / (256 * 512.0)

    def project(u):
        lc, m1, m2 = unit_of(ll, ml, u)
        rows = jnp.concatenate([xs[column(lc, m1)].reshape(128, 512), xs[column(lc, m2)].reshape(128, 512)], axis=0)
        proj = jnp.dot(rows, wv[...], preferred_element_type=F32)
        inv = 1.0 / jnp.sqrt(jnp.sum(proj * proj, axis=1, keepdims=True))
        qown[u] = (proj * inv).astype(BF16)

    def to_sib(u):
        return rcopy(qown.at[u], qsib.at[u], q_send.at[0], q_recv.at[u], sib)

    def dots(buf, qs):
        q = qs[0] if len(qs) == 1 else jnp.concatenate(qs, axis=0)
        buf[0:256 * len(qs)] = lax.dot_general(q, gv[...], (((1,), (1,)), ((), ())), preferred_element_type=F32)

    def soften(buf, groups):
        n = 128 * len(groups)
        lane = lax.broadcasted_iota(jnp.int32, (n, 128), 1)
        d = buf[0:n]
        dm = jnp.max(d, axis=1, keepdims=True)
        ev = jnp.exp2((d - dm) * k2)
        zs = jnp.sum(ev, axis=1, keepdims=True)
        rs = jnp.sum(ev * pos, axis=1, keepdims=True)
        cols = jnp.where(lane == 0, dm, jnp.where(lane == 1, zs, rs))
        for i, gq in enumerate(groups):
            rows = slice(i * 128, i * 128 + 128)
            e_ref[gq] = ev[rows]
            stat[gq] = cols[rows].T[:8]

    def groups_own(u):
        lc, m1, m2 = unit_of(ll, ml, u)
        return [jnp.where(core0, m * 8 + lc * 2, lc * 8 + m * 2 + 1) for m in (m1, m2)]

    def groups_sib(u):
        lc, m1, m2 = unit_of(ml, ll, u)
        return [jnp.where(core0, lc * 8 + m * 2 + 1, m * 8 + lc * 2) for m in (m1, m2)]

    def groups_both(uo, us):
        return groups_own(uo) + groups_sib(us)

    def send_group(gq):
        @pl.when(gq != pi)
        def _():
            rcopy(stat.at[gq], part.at[pi], s_send.at[0], s_recv.at[0], z * 32 + gq).start()

        @pl.when(gq == pi)
        def _():
            part[pi] = stat[pi]

    def send_own(u, carry):
        for gq in groups_own(u):
            send_group(gq)
        return carry

    def send_sib(u, carry):
        for gq in groups_sib(u):
            send_group(gq)
        return carry

    mid(1, 1)
    mid(2, 3)
    project(0)
    to_sib(0).start()
    mid(3, 2)
    with scope("event0"):
        event(0)
    project(1)
    dots(da, [qown[0]])
    to_sib(1).start()

    def step(k, now, before, first):
        with scope("events"):
            @pl.when(k <= 4)
            def _():
                event(k - 1)

            @pl.when(k == 6)
            def _():
                for e in range(4, 6):
                    to_right(lf, e - 4, e).wait_recv()

            @pl.when(k == 7)
            def _():
                for e in range(4, 6):
                    to_left(lf, e - 2, e).wait_recv()

        with scope("sibwait"):
            to_sib(k - 2).wait_recv()
        with scope("compute"):
            soften(before, groups_own(0) if first else groups_both(k - 2, k - 3))
            project(k)
            dots(now, [qown[k - 1], qsib[k - 2]])
        to_sib(k).start()

    step(2, db, da, True)
    step(3, da, db, False)

    def body(i, carry):
        k = 2 * i
        step(k, db, da, False)

        @pl.when(i == 3)
        def _():
            lax.fori_loop(0, 4, send_own, 0)
            lax.fori_loop(0, 3, send_sib, 0)

        step(k + 1, da, db, False)

        @pl.when(i == 3)
        def _():
            lax.fori_loop(4, 6, send_own, 0)
            lax.fori_loop(3, 5, send_sib, 0)

        return carry

    lax.fori_loop(2, 4, body, 0)
    with scope("tail6"):
        to_sib(6).wait_recv()
        soften(da, groups_both(6, 5))
        dots(db, [qown[7], qsib[6]])
    send_own(6, 0)
    send_sib(5, 0)
    with scope("tail7"):
        to_sib(7).wait_recv()
        soften(db, groups_both(7, 6))
        dots(da, [qsib[7]])
    send_own(7, 0)
    send_sib(6, 0)
    with scope("tail8"):
        soften(da, groups_sib(7))
    send_sib(7, 0)

    with scope("s1wait"):
        rcopy(part.at[0:31], part.at[0:31], s_send.at[0], s_recv.at[0], sib).wait_recv()

    def merge(ref):
        ms = ref[:, 0, :]
        m = jnp.max(ms, axis=0, keepdims=True)
        wgt = jnp.exp2((ms - m) * k2)
        return m, jnp.sum(wgt * ref[:, 1, :], axis=0, keepdims=True), jnp.sum(wgt * ref[:, 2, :], axis=0, keepdims=True)

    sub = lax.broadcasted_iota(jnp.int32, (8, 128), 0)

    def tile(a, b, d):
        return jnp.where(sub == 0, a, jnp.where(sub == 1, b, d))

    zpart[z] = tile(*merge(part))
    for d in range(1, NZ):
        rcopy(zpart.at[z], zpart.at[z], s_send.at[1], s_recv.at[1], z_peers[d - 1]).start()
    with scope("s2wait"):
        rcopy(zpart.at[0:7], zpart.at[0:7], s_send.at[1], s_recv.at[1], sib).wait_recv()
    m, zs, rs = merge(zpart)
    done[pi] = tile(m, 1.0 / zs, rs / zs)

    def send_done(k, carry):
        p = lax.rem(pi + k, 32)
        rcopy(done.at[pi], done.at[pi], s_send.at[2], s_recv.at[2], z * 32 + p).start()
        return carry

    with scope("s3send"):
        lax.fori_loop(1, 32, send_done, 0)

    with scope("s3wait"):
        rcopy(done.at[0:31], done.at[0:31], s_send.at[2], s_recv.at[2], sib).wait_recv()
    fac_ref[...] = jnp.exp2((stat[:, 0, :] - done[:, 0, :]) * k2) * done[:, 1, :]
    rank_ref[...] = done[:, 2, :]

    def sent(ref, sem):
        rcopy(ref, ref, sem, sem, sib).wait_send()

    with scope("drain"):
        sent(xs.at[0, 0:7], a_sem.at[0])
        sent(xs.at[0:3], y_send.at[0])
        sent(xs.at[0:6], r_send.at[0])
        sent(xs.at[0:6], l_send.at[0])
        sent(qown, q_send.at[0])
        sent(part.at[0:31], s_send.at[0])
        sent(zpart.at[0:7], s_send.at[1])
        sent(done.at[0:31], s_send.at[2])


def normalise_kernel(e_ref, fac_ref, rank_ref, p_hbm, r_ref, buf, sem):
    def body(i, carry):
        for j in range(8):
            gq = i * 8 + j
            f = jnp.broadcast_to(fac_ref[pl.ds(gq, 1), :], (128, 128)).T
            ev = e_ref[gq]
            p = jnp.concatenate([ev[:, b * 128:(b + 1) * 128] * f for b in range(4)], axis=1)
            buf[gq] = p.astype(BF16).reshape(8, 16, 512)
        for j in range(8):
            gq = i * 8 + j
            pltpu.make_async_copy(buf.at[gq], p_hbm.at[:, gq], sem.at[i]).start()
        return carry

    lax.fori_loop(0, 4, body, 0)

    lane = lax.broadcasted_iota(jnp.int32, (8, 128), 1) // 16
    sub = lax.broadcasted_iota(jnp.int32, (8, 128), 0)
    for yy in range(NY):
        r = rank_ref[yy * 8:yy * 8 + 8]
        nat = r
        for d in range(1, 8):
            moved = pltpu.roll(pltpu.roll(r, 16 * d, 1), 8 - d, 0)
            nat = jnp.where(lax.rem(lane - sub + 8, 8) == d, moved, nat)
        r_ref[pl.ds(yy, 8, stride=4), :] = nat

    for i in range(4):
        pltpu.make_async_copy(buf.at[0:8], p_hbm.at[:, 0:8], sem.at[i]).wait()


def solution(mesh):
    D = pltpu.SemaphoreType.DMA
    VM = pltpu.VMEM

    def per_device(text_states, text_proj, gallery, logit_scale):
        e, fac, rank = pl.pallas_call(
            gather_score_kernel,
            out_shape=(VM((32, 128, 512), F32), VM((32, 128), F32), VM((32, 128), F32)),
            in_specs=[pl.BlockSpec(memory_space=pl.ANY)] * 3 + [pl.BlockSpec(memory_space=pltpu.SMEM)],
            out_specs=(pl.BlockSpec(memory_space=VM),) * 3,
            scratch_shapes=[
                VM((16, NZ, 16, 512), BF16), VM((512, 1024), BF16), VM((512, 1024), BF16),
                VM((8, 256, 1024), BF16), VM((8, 256, 1024), BF16), VM((512, 512), F32), VM((512, 512), F32),
                VM((32, 8, 128), F32), VM((32, 8, 128), F32), VM((NZ, 8, 128), F32), VM((32, 8, 128), F32),
                D((3,)), D((2,)), D((1,)), D((3,)), D((1,)), D((6,)), D((1,)), D((6,)),
                D((1,)), D((8,)), D((3,)), D((3,)),
            ],
            compiler_params=pltpu.CompilerParams(collective_id=0, has_side_effects=True,
                                                 vmem_limit_bytes=48 * 1024 * 1024),
        )(text_states, text_proj, gallery, logit_scale)
        prob, rank = pl.pallas_call(
            normalise_kernel,
            out_shape=(jax.ShapeDtypeStruct((NZ, 32, 16, 512), BF16), jax.ShapeDtypeStruct((32, 128), F32)),
            in_specs=[pl.BlockSpec(memory_space=VM)] * 3,
            out_specs=(pl.BlockSpec(memory_space=pl.ANY), pl.BlockSpec(memory_space=VM)),
            scratch_shapes=[VM((32, NZ, 16, 512), BF16), D((4,))],
            compiler_params=pltpu.CompilerParams(vmem_limit_bytes=24 * 1024 * 1024),
        )(e, fac, rank)
        return prob.reshape(4096, 512), rank.reshape(4096)

    return jax.shard_map(per_device, mesh=mesh,
                         in_specs=(P("ga", None), P(None, None), P("ga", None), P(None)),
                         out_specs=(P(None, "ga"), P(None)), check_vma=False)
```

```python
import jax
import jax.numpy as jnp
from jax import lax
from jax.experimental import pallas as pl
from jax.experimental.pallas import tpu as pltpu
from jax.sharding import PartitionSpec as P

MESH = pl.DeviceIdType.MESH
NX, NY, NZ, NC = 4, 4, 8, 2
F32, BF16 = jnp.float32, jnp.bfloat16
LOG2E = 1.4426950408889634
F32_MAX = 3.4028235e38
scope = jax.named_scope


def rcopy(src, dst, ss, rs, p):
    return pltpu.make_async_remote_copy(src_ref=src, dst_ref=dst, send_sem=ss, recv_sem=rs,
                                        device_id=(p,), device_id_type=MESH)


def gather_score_kernel(x_hbm, w_hbm, g_hbm, t_ref,
                        e_ref, fac_ref, rank_ref,
                        xs, wv, gv, qown, qsib, da, db, stat, part, zpart, done,
                        in_sem, a_sem, y_send, y_recv, r_send, r_recv, l_send, l_recv,
                        q_send, q_recv, s_send, s_recv):
    me = lax.axis_index("ga")
    c = lax.rem(me, NC)
    x = lax.rem(me // 2, NX)
    y = lax.rem(me // 8, NY)
    z = me // 32
    pi = lax.rem(me, 32)
    core0 = c == 0
    ml = jnp.where(core0, y, x)
    ll = jnp.where(core0, x, y)

    def dev(zz, yy, xx, cc):
        return ((zz * NY + yy) * NX + xx) * NC + cc

    def dev_lm(zz, lc, mc):
        return dev(zz, jnp.where(core0, mc, lc), jnp.where(core0, lc, mc), c)

    def column(lc, mc):
        return lc * 4 + mc

    mine = column(ll, ml)
    own = xs.at[mine, z]
    load_x = pltpu.make_async_copy(x_hbm, own, in_sem.at[0])
    load_w = pltpu.make_async_copy(w_hbm, wv, in_sem.at[1])
    load_g = pltpu.make_async_copy(g_hbm, gv, in_sem.at[2])
    load_x.start()
    load_w.start()
    load_g.start()

    sib = dev(z, y, x, 1 - c)
    z_peers = [dev(lax.rem(z + d, NZ), y, x, c) for d in range(1, NZ)]
    m_next = dev_lm(z, ll, lax.rem(ml + 1, 4))
    m_prev = dev_lm(z, ll, lax.rem(ml + 3, 4))
    right = dev_lm(z, lax.rem(ll + 1, 4), ml)
    left = dev_lm(z, lax.rem(ll + 3, 4), ml)

    barrier = pltpu.get_barrier_semaphore()
    with scope("barrier"):
        peers = [sib, right, left, m_next, m_prev] + z_peers
        for p in peers:
            pl.semaphore_signal(barrier, inc=1, device_id=(p,), device_id_type=MESH)
        pl.semaphore_wait(barrier, len(peers))
        load_x.wait()

    for d in range(1, NZ):
        rcopy(own, own, a_sem.at[0], a_sem.at[1], z_peers[d - 1]).start()
    with scope("first"):
        rcopy(xs.at[0, 0:7], xs.at[0, 0:7], a_sem.at[0], a_sem.at[1], sib).wait_recv()

    def col(lc, j):
        off = jnp.where(j == 0, 0, jnp.where(j == 1, 1, jnp.where(j == 2, 3, 2)))
        return xs.at[column(lc, lax.rem(ml + off, 4))]

    def to_right(lc, j, e):
        return rcopy(col(lc, j), col(lc, j), r_send.at[0], r_recv.at[e], right)

    def to_left(lc, j, e):
        return rcopy(col(lc, j), col(lc, j), l_send.at[0], l_recv.at[e], left)

    lp, lm, lf = lax.rem(ll + 1, 4), lax.rem(ll + 3, 4), lax.rem(ll + 2, 4)

    def to_mid(ref, e, p):
        return rcopy(ref, ref, y_send.at[0], y_recv.at[e], p)

    def half(j, h):
        return col(ll, j).at[4 * h:4 * h + 4]

    to_mid(xs.at[mine], 1, m_next).start()
    to_mid(xs.at[mine], 0, m_prev).start()
    to_right(ll, 0, 0).start()
    to_left(ll, 0, 0).start()

    with scope("second"):
        to_mid(col(ll, 1), 0, sib).wait_recv()
    to_mid(half(1, 0), 2, m_prev).start()
    to_right(ll, 1, 1).start()
    to_left(ll, 1, 1).start()
    with scope("second"):
        to_mid(col(ll, 2), 1, sib).wait_recv()
    to_mid(half(2, 1), 3, m_next).start()
    to_right(ll, 2, 2).start()
    to_left(ll, 2, 2).start()

    def far_column():
        with scope("third"):
            to_mid(half(3, 0), 2, sib).wait_recv()
            to_mid(half(3, 1), 3, sib).wait_recv()
        to_right(ll, 3, 3).start()
        to_left(ll, 3, 3).start()

    def event(e):
        to_right(lm, e, e).wait_recv()

        @pl.when(e < 2)
        def _():
            to_right(lm, e, 4 + e).start()

        to_left(lp, e, e).wait_recv()

        @pl.when(e >= 2)
        def _():
            to_left(lp, e, 2 + e).start()

    def unit_of(lc, mc, u):
        own_u = jnp.logical_or(u == 0, u == 2)
        far = u >= 6
        l1 = lax.rem(lc + jnp.where(own_u, 0, jnp.where(far, 2, 3)), 4)
        l2 = lax.rem(lc + jnp.where(own_u, 0, jnp.where(far, 2, 1)), 4)
        pair2 = jnp.logical_or(u == 2, u == 7)
        ring_off = jnp.where(u == 1, 0, jnp.where(u == 3, 1, jnp.where(u == 4, 3, 2)))
        pair = jnp.logical_or(own_u, far)
        m1 = lax.rem(mc + jnp.where(pair, jnp.where(pair2, 3, 0), ring_off), 4)
        m2 = lax.rem(mc + jnp.where(pair, jnp.where(pair2, 2, 1), ring_off), 4)
        return (l1, m1), (l2, m2)

    load_w.wait()
    load_g.wait()
    k2 = jnp.minimum(jnp.exp(jnp.full((1, 1), t_ref[0], F32)) * LOG2E, F32_MAX)
    place = lax.broadcasted_iota(jnp.int32, (1, 512), 1) + me * 512
    pos = place.astype(F32) / (256 * 512.0)

    def project(u):
        rows = jnp.concatenate([xs[column(lc, mc)].reshape(128, 512) for lc, mc in unit_of(ll, ml, u)], axis=0)
        proj = jnp.dot(rows, wv[...], preferred_element_type=F32)
        inv = 1.0 / jnp.sqrt(jnp.sum(proj * proj, axis=1, keepdims=True))
        qown[u] = (proj * inv).astype(BF16)

    def to_sib(u):
        return rcopy(qown.at[u], qsib.at[u], q_send.at[0], q_recv.at[u], sib)

    def dots(buf, qs):
        q = qs[0] if len(qs) == 1 else jnp.concatenate(qs, axis=0)
        buf[0:256 * len(qs)] = lax.dot_general(q, gv[...], (((1,), (1,)), ((), ())), preferred_element_type=F32)

    def soften(buf, groups):
        n = 128 * len(groups)
        lane = lax.broadcasted_iota(jnp.int32, (n, 128), 1)
        d = buf[0:n]
        dm = jnp.max(d, axis=1, keepdims=True)
        ev = jnp.exp2((d - dm) * k2)
        zs = jnp.sum(ev, axis=1, keepdims=True)
        rs = jnp.sum(ev * pos, axis=1, keepdims=True)
        cols = jnp.where(lane == 0, dm, jnp.where(lane == 1, zs, rs))
        for i, gq in enumerate(groups):
            rows = slice(i * 128, i * 128 + 128)
            e_ref[gq] = ev[rows]
            stat[gq] = cols[rows].T[:4]

    def groups_own(u):
        return [jnp.where(core0, mc * 8 + lc * 2, lc * 8 + mc * 2 + 1) for lc, mc in unit_of(ll, ml, u)]

    def groups_sib(u):
        return [jnp.where(core0, lc * 8 + mc * 2 + 1, mc * 8 + lc * 2) for lc, mc in unit_of(ml, ll, u)]

    def groups_both(uo, us):
        return groups_own(uo) + groups_sib(us)

    def send_group(gq):
        @pl.when(gq != pi)
        def _():
            rcopy(stat.at[gq], part.at[pi], s_send.at[0], s_recv.at[0], z * 32 + gq).start()

        @pl.when(gq == pi)
        def _():
            part[pi] = stat[pi]

    def send_own(u, carry):
        for gq in groups_own(u):
            send_group(gq)
        return carry

    def send_sib(u, carry):
        for gq in groups_sib(u):
            send_group(gq)
        return carry

    project(0)
    to_sib(0).start()
    with scope("event0"):
        event(0)
    project(1)
    dots(da, [qown[0]])
    to_sib(1).start()
    far_column()

    def step(k, now, before, first):
        with scope("events"):
            @pl.when(jnp.logical_and(k >= 3, k <= 5))
            def _():
                event(k - 2)

            @pl.when(k == 6)
            def _():
                for e in range(4, 6):
                    to_right(lf, e - 4, e).wait_recv()

            @pl.when(k == 7)
            def _():
                for e in range(4, 6):
                    to_left(lf, e - 2, e).wait_recv()

        with scope("sibwait"):
            to_sib(k - 2).wait_recv()
        with scope("compute"):
            soften(before, groups_own(0) if first else groups_both(k - 2, k - 3))
            project(k)
            dots(now, [qown[k - 1], qsib[k - 2]])
        to_sib(k).start()

    step(2, db, da, True)
    step(3, da, db, False)

    def body(i, carry):
        k = 2 * i
        step(k, db, da, False)

        @pl.when(i == 3)
        def _():
            lax.fori_loop(0, 4, send_own, 0)
            lax.fori_loop(0, 3, send_sib, 0)

        step(k + 1, da, db, False)

        @pl.when(i == 3)
        def _():
            lax.fori_loop(4, 6, send_own, 0)
            lax.fori_loop(3, 5, send_sib, 0)

        return carry

    lax.fori_loop(2, 4, body, 0)
    with scope("tail6"):
        to_sib(6).wait_recv()
        soften(da, groups_both(6, 5))
        dots(db, [qown[7], qsib[6]])
    send_own(6, 0)
    send_sib(5, 0)
    with scope("tail7"):
        to_sib(7).wait_recv()
        soften(db, groups_both(7, 6))
        dots(da, [qsib[7]])
    send_own(7, 0)
    send_sib(6, 0)
    with scope("tail8"):
        soften(da, groups_sib(7))
    send_sib(7, 0)

    with scope("s1wait"):
        rcopy(part.at[0:31], part.at[0:31], s_send.at[0], s_recv.at[0], sib).wait_recv()

    def merge(ref):
        ms = ref[:, 0, :]
        m = jnp.max(ms, axis=0, keepdims=True)
        wgt = jnp.exp2((ms - m) * k2)
        return m, jnp.sum(wgt * ref[:, 1, :], axis=0, keepdims=True), jnp.sum(wgt * ref[:, 2, :], axis=0, keepdims=True)

    sub = lax.broadcasted_iota(jnp.int32, (4, 128), 0)

    def tile(a, b, d):
        return jnp.where(sub == 0, a, jnp.where(sub == 1, b, d))

    zpart[z] = tile(*merge(part))
    for d in range(1, NZ):
        rcopy(zpart.at[z], zpart.at[z], s_send.at[1], s_recv.at[1], z_peers[d - 1]).start()
    with scope("s2wait"):
        rcopy(zpart.at[0:7], zpart.at[0:7], s_send.at[1], s_recv.at[1], sib).wait_recv()
    m, zs, rs = merge(zpart)
    done[pi] = tile(m, 1.0 / zs, rs / zs)

    def send_done(k, carry):
        p = lax.rem(pi + k, 32)
        rcopy(done.at[pi], done.at[pi], s_send.at[2], s_recv.at[2], z * 32 + p).start()
        return carry

    with scope("s3send"):
        lax.fori_loop(1, 32, send_done, 0)

    with scope("s3wait"):
        rcopy(done.at[0:31], done.at[0:31], s_send.at[2], s_recv.at[2], sib).wait_recv()
    fac_ref[...] = jnp.exp2((stat[:, 0, :] - done[:, 0, :]) * k2) * done[:, 1, :]
    rank_ref[...] = done[:, 2, :]

    def sent(ref, sem):
        rcopy(ref, ref, sem, sem, sib).wait_send()

    with scope("drain"):
        sent(xs.at[0, 0:7], a_sem.at[0])
        sent(xs.at[0:3], y_send.at[0])
        sent(xs.at[0:6], r_send.at[0])
        sent(xs.at[0:6], l_send.at[0])
        sent(qown, q_send.at[0])
        sent(part.at[0:31], s_send.at[0])
        sent(zpart.at[0:7], s_send.at[1])
        sent(done.at[0:31], s_send.at[2])


def normalise_kernel(e_ref, fac_ref, rank_ref, p_hbm, r_ref, buf, sem):
    def body(i, carry):
        for j in range(8):
            gq = i * 8 + j
            f = jnp.broadcast_to(fac_ref[pl.ds(gq, 1), :], (128, 128)).T
            ev = e_ref[gq]
            p = jnp.concatenate([ev[:, b * 128:(b + 1) * 128] * f for b in range(4)], axis=1)
            buf[gq] = p.astype(BF16).reshape(8, 16, 512)
        for j in range(8):
            gq = i * 8 + j
            pltpu.make_async_copy(buf.at[gq], p_hbm.at[:, gq], sem.at[i]).start()
        return carry

    lax.fori_loop(0, 4, body, 0)

    lane = lax.broadcasted_iota(jnp.int32, (8, 128), 1) // 16
    sub = lax.broadcasted_iota(jnp.int32, (8, 128), 0)
    for yy in range(NY):
        r = rank_ref[yy * 8:yy * 8 + 8]
        nat = r
        for d in range(1, 8):
            moved = pltpu.roll(pltpu.roll(r, 16 * d, 1), 8 - d, 0)
            nat = jnp.where(lax.rem(lane - sub + 8, 8) == d, moved, nat)
        r_ref[pl.ds(yy, 8, stride=4), :] = nat

    for i in range(4):
        pltpu.make_async_copy(buf.at[0:8], p_hbm.at[:, 0:8], sem.at[i]).wait()


def solution(mesh):
    D = pltpu.SemaphoreType.DMA
    VM = pltpu.VMEM

    def per_device(text_states, text_proj, gallery, logit_scale):
        e, fac, rank = pl.pallas_call(
            gather_score_kernel,
            out_shape=(VM((32, 128, 512), F32), VM((32, 128), F32), VM((32, 128), F32)),
            in_specs=[pl.BlockSpec(memory_space=pl.ANY)] * 3 + [pl.BlockSpec(memory_space=pltpu.SMEM)],
            out_specs=(pl.BlockSpec(memory_space=VM),) * 3,
            scratch_shapes=[
                VM((16, NZ, 16, 512), BF16), VM((512, 1024), BF16), VM((512, 1024), BF16),
                VM((8, 256, 1024), BF16), VM((8, 256, 1024), BF16), VM((512, 512), F32), VM((512, 512), F32),
                VM((32, 4, 128), F32), VM((32, 4, 128), F32), VM((NZ, 4, 128), F32), VM((32, 4, 128), F32),
                D((3,)), D((2,)), D((1,)), D((4,)), D((1,)), D((6,)), D((1,)), D((6,)),
                D((1,)), D((8,)), D((3,)), D((3,)),
            ],
            compiler_params=pltpu.CompilerParams(collective_id=0, has_side_effects=True,
                                                 vmem_limit_bytes=48 * 1024 * 1024),
        )(text_states, text_proj, gallery, logit_scale)
        prob, rank = pl.pallas_call(
            normalise_kernel,
            out_shape=(jax.ShapeDtypeStruct((NZ, 32, 16, 512), BF16), jax.ShapeDtypeStruct((32, 128), F32)),
            in_specs=[pl.BlockSpec(memory_space=VM)] * 3,
            out_specs=(pl.BlockSpec(memory_space=pl.ANY), pl.BlockSpec(memory_space=VM)),
            scratch_shapes=[VM((32, NZ, 16, 512), BF16), D((4,))],
            compiler_params=pltpu.CompilerParams(vmem_limit_bytes=24 * 1024 * 1024),
        )(e, fac, rank)
        return prob.reshape(4096, 512), rank.reshape(4096)

    return jax.shard_map(per_device, mesh=mesh,
                         in_specs=(P("ga", None), P(None, None), P("ga", None), P(None)),
                         out_specs=(P(None, "ga"), P(None)), check_vma=False)
```

```python
import jax
import jax.numpy as jnp
from jax import lax
from jax.experimental import pallas as pl
from jax.experimental.pallas import tpu as pltpu
from jax.sharding import PartitionSpec as P

MESH = pl.DeviceIdType.MESH
NX, NY, NZ, NC = 4, 4, 8, 2
F32, BF16 = jnp.float32, jnp.bfloat16
LOG2E = 1.4426950408889634
F32_MAX = 3.4028235e38
scope = jax.named_scope


def rcopy(src, dst, ss, rs, p):
    return pltpu.make_async_remote_copy(src_ref=src, dst_ref=dst, send_sem=ss, recv_sem=rs,
                                        device_id=(p,), device_id_type=MESH)


def gather_score_kernel(x_hbm, w_hbm, g_hbm, t_hbm,
                        e_ref, fac_ref, rank_ref,
                        xs, wv, gv, tv, qown, qsib, da, db, stat, part, zpart, done,
                        in_sem, a_sem, y_send, y_recv, r_send, r_recv, l_send, l_recv,
                        q_send, q_recv, s_send, s_recv):
    me = lax.axis_index("ga")
    c = lax.rem(me, NC)
    x = lax.rem(me // 2, NX)
    y = lax.rem(me // 8, NY)
    z = me // 32
    pi = lax.rem(me, 32)
    core0 = c == 0
    ml = jnp.where(core0, y, x)
    ll = jnp.where(core0, x, y)

    def dev(zz, yy, xx, cc):
        return ((zz * NY + yy) * NX + xx) * NC + cc

    def dev_lm(zz, lc, mc):
        return dev(zz, jnp.where(core0, mc, lc), jnp.where(core0, lc, mc), c)

    def column(lc, mc):
        return lc * 4 + mc

    mine = column(ll, ml)
    own = xs.at[mine, z]
    load_x = pltpu.make_async_copy(x_hbm, own, in_sem.at[0])
    load_w = pltpu.make_async_copy(w_hbm, wv, in_sem.at[1])
    load_g = pltpu.make_async_copy(g_hbm, gv, in_sem.at[2])
    load_t = pltpu.make_async_copy(t_hbm, tv, in_sem.at[3])
    load_x.start()
    load_t.start()
    load_w.start()
    load_g.start()

    sib = dev(z, y, x, 1 - c)
    z_peers = [dev(lax.rem(z + d, NZ), y, x, c) for d in range(1, NZ)]
    m_next = dev_lm(z, ll, lax.rem(ml + 1, 4))
    m_prev = dev_lm(z, ll, lax.rem(ml + 3, 4))
    right = dev_lm(z, lax.rem(ll + 1, 4), ml)
    left = dev_lm(z, lax.rem(ll + 3, 4), ml)

    barrier = pltpu.get_barrier_semaphore()
    with scope("barrier"):
        peers = [sib, right, left, m_next, m_prev] + z_peers
        for p in peers:
            pl.semaphore_signal(barrier, inc=1, device_id=(p,), device_id_type=MESH)
        pl.semaphore_wait(barrier, len(peers))
        load_x.wait()

    for d in range(1, NZ):
        rcopy(own, own, a_sem.at[0], a_sem.at[1], z_peers[d - 1]).start()
    with scope("first"):
        rcopy(xs.at[0, 0:7], xs.at[0, 0:7], a_sem.at[0], a_sem.at[1], sib).wait_recv()

    OFF = (0, 1, 3, 2)

    def col(lc, j, h):
        return xs.at[column(lc, lax.rem(ml + OFF[j], 4)), 4 * h:4 * h + 4]

    def to_right(lc, j, h, far=0):
        return rcopy(col(lc, j, h), col(lc, j, h), r_send.at[0], r_recv.at[far * 8 + j * 2 + h], right)

    def to_left(lc, j, h, far=0):
        return rcopy(col(lc, j, h), col(lc, j, h), l_send.at[0], l_recv.at[far * 4 + j * 2 + h], left)

    def to_mid(j, h, e, p):
        return rcopy(col(ll, j, h), col(ll, j, h), y_send.at[0], y_recv.at[e], p)

    lp, lm, lf = lax.rem(ll + 1, 4), lax.rem(ll + 3, 4), lax.rem(ll + 2, 4)

    def round_ring(j, h):
        to_right(ll, j, h).start()
        to_left(ll, j, h).start()

    for h in range(2):
        to_mid(0, h, h, m_prev).start()
        to_mid(0, 1 - h, 3 - h, m_next).start()
    round_ring(0, 0)
    round_ring(0, 1)

    with scope("second"):
        to_mid(1, 0, 0, sib).wait_recv()
    to_mid(1, 0, 4, m_prev).start()
    round_ring(1, 0)
    with scope("second"):
        to_mid(2, 1, 3, sib).wait_recv()
    to_mid(2, 1, 5, m_next).start()
    round_ring(2, 1)
    with scope("second"):
        to_mid(1, 1, 1, sib).wait_recv()
    round_ring(1, 1)
    with scope("second"):
        to_mid(2, 0, 2, sib).wait_recv()
    round_ring(2, 0)

    def far_column():
        for h in range(2):
            with scope("third"):
                to_mid(3, h, 4 + h, sib).wait_recv()
            round_ring(3, h)

    def event(j):
        for i in range(2):
            h = 1 - i if j == 2 else i
            to_right(lm, j, h).wait_recv()
            if j < 2:
                to_right(lm, j, h, 1).start()
            to_left(lp, j, h).wait_recv()
            if j >= 2:
                to_left(lp, j, h, 1).start()

    UNITS = (((0, 0), (0, 1)), ((3, 0), (1, 0)), ((0, 3), (0, 2)), ((3, 1), (1, 1)),
             ((3, 3), (1, 3)), ((3, 2), (1, 2)), ((2, 0), (2, 1)), ((2, 3), (2, 2)))

    def unit_of(lc, mc, u):
        return [(lax.rem(lc + a, 4), lax.rem(mc + b, 4)) for a, b in UNITS[u]]

    load_w.wait()
    load_g.wait()
    load_t.wait()
    k2 = jnp.minimum(jnp.exp(jnp.full((1, 1), tv[0], F32)) * LOG2E, F32_MAX)
    place = lax.broadcasted_iota(jnp.int32, (1, 512), 1) + me * 512
    pos = place.astype(F32) / (256 * 512.0)

    def project(u):
        rows = jnp.concatenate([xs[column(lc, mc)].reshape(128, 512) for lc, mc in unit_of(ll, ml, u)], axis=0)
        proj = jnp.dot(rows, wv[...], preferred_element_type=F32)
        inv = 1.0 / jnp.sqrt(jnp.sum(proj * proj, axis=1, keepdims=True))
        qown[u] = (proj * inv).astype(BF16)

    def to_sib(u):
        return rcopy(qown.at[u], qsib.at[u], q_send.at[0], q_recv.at[u], sib)

    def dots(buf, qs):
        q = qs[0] if len(qs) == 1 else jnp.concatenate(qs, axis=0)
        buf[0:256 * len(qs)] = lax.dot_general(q, gv[...], (((1,), (1,)), ((), ())), preferred_element_type=F32)

    def soften(buf, groups):
        n = 128 * len(groups)
        lane = lax.broadcasted_iota(jnp.int32, (n, 128), 1)
        d = buf[0:n]
        dm = jnp.max(d, axis=1, keepdims=True)
        ev = jnp.exp2((d - dm) * k2)
        zs = jnp.sum(ev, axis=1, keepdims=True)
        rs = jnp.sum(ev * pos, axis=1, keepdims=True)
        cols = jnp.where(lane == 0, dm, jnp.where(lane == 1, zs, rs))
        for i, gq in enumerate(groups):
            rows = slice(i * 128, i * 128 + 128)
            e_ref[gq] = ev[rows]
            stat[gq] = cols[rows].T[:4]

    def groups_own(u):
        return [jnp.where(core0, mc * 8 + lc * 2, lc * 8 + mc * 2 + 1) for lc, mc in unit_of(ll, ml, u)]

    def groups_sib(u):
        return [jnp.where(core0, lc * 8 + mc * 2 + 1, mc * 8 + lc * 2) for lc, mc in unit_of(ml, ll, u)]

    def groups_both(uo, us):
        return groups_own(uo) + groups_sib(us)

    def send_group(gq):
        @pl.when(gq != pi)
        def _():
            rcopy(stat.at[gq], part.at[pi], s_send.at[0], s_recv.at[0], z * 32 + gq).start()

        @pl.when(gq == pi)
        def _():
            part[pi] = stat[pi]

    def send_own(u):
        for gq in groups_own(u):
            send_group(gq)

    def send_sib(u):
        for gq in groups_sib(u):
            send_group(gq)

    project(0)
    to_sib(0).start()
    with scope("event0"):
        event(0)
    project(1)
    dots(da, [qown[0]])
    to_sib(1).start()
    far_column()

    def step(k, now, before):
        with scope("events"):
            if 3 <= k <= 5:
                event(k - 2)
            for h in range(2):
                if k == 6:
                    to_right(lf, 0, h, 1).wait_recv()
                    to_right(lf, 1, h, 1).wait_recv()
                if k == 7:
                    to_left(lf, 2, h, 1).wait_recv()
                    to_left(lf, 3, h, 1).wait_recv()

        with scope("sibwait"):
            to_sib(k - 2).wait_recv()
        with scope("compute"):
            soften(before, groups_own(0) if k == 2 else groups_both(k - 2, k - 3))
            project(k)
            dots(now, [qown[k - 1], qsib[k - 2]])
        to_sib(k).start()

    for k in range(2, 8):
        step(k, db if k % 2 == 0 else da, da if k % 2 == 0 else db)
        if k >= 6:
            for u in range(0 if k == 6 else 4, k - 2):
                send_own(u)
            for u in range(0 if k == 6 else 3, k - 3):
                send_sib(u)
    send_own(5)
    send_sib(4)
    with scope("tail6"):
        to_sib(6).wait_recv()
        soften(da, groups_both(6, 5))
        dots(db, [qown[7], qsib[6]])
    send_own(6)
    send_sib(5)
    with scope("tail7"):
        to_sib(7).wait_recv()
        soften(db, groups_both(7, 6))
        dots(da, [qsib[7]])
    send_own(7)
    send_sib(6)
    with scope("tail8"):
        soften(da, groups_sib(7))
    send_sib(7)

    with scope("s1wait"):
        rcopy(part.at[0:31], part.at[0:31], s_send.at[0], s_recv.at[0], sib).wait_recv()

    def merge(ref):
        ms = ref[:, 0, :]
        m = jnp.max(ms, axis=0, keepdims=True)
        wgt = jnp.exp2((ms - m) * k2)
        return m, jnp.sum(wgt * ref[:, 1, :], axis=0, keepdims=True), jnp.sum(wgt * ref[:, 2, :], axis=0, keepdims=True)

    sub = lax.broadcasted_iota(jnp.int32, (4, 128), 0)

    def tile(a, b, d):
        return jnp.where(sub == 0, a, jnp.where(sub == 1, b, d))

    zpart[z] = tile(*merge(part))
    for d in range(1, NZ):
        rcopy(zpart.at[z], zpart.at[z], s_send.at[1], s_recv.at[1], z_peers[d - 1]).start()
    with scope("s2wait"):
        rcopy(zpart.at[0:7], zpart.at[0:7], s_send.at[1], s_recv.at[1], sib).wait_recv()
    m, zs, rs = merge(zpart)
    done[pi] = tile(m, 1.0 / zs, rs / zs)

    peers = [(dy, dx, dc) for dy in range(4) for dx in range(4) for dc in range(2)][1:]
    peers.sort(key=lambda p: -min(p[0], 4 - p[0]) - min(p[1], 4 - p[1]))
    with scope("s3send"):
        for dy, dx, dc in peers:
            p = dev(z, lax.rem(y + dy, NY), lax.rem(x + dx, NX), lax.rem(c + dc, NC))
            rcopy(done.at[pi], done.at[pi], s_send.at[2], s_recv.at[2], p).start()

    with scope("s3wait"):
        rcopy(done.at[0:31], done.at[0:31], s_send.at[2], s_recv.at[2], sib).wait_recv()
    fac_ref[...] = jnp.exp2((stat[:, 0, :] - done[:, 0, :]) * k2) * done[:, 1, :]
    rank_ref[...] = done[:, 2, :]

    def sent(ref, sem):
        rcopy(ref, ref, sem, sem, sib).wait_send()

    with scope("drain"):
        sent(xs.at[0, 0:7], a_sem.at[0])
        sent(xs.at[0:3], y_send.at[0])
        sent(xs.at[0:6], r_send.at[0])
        sent(xs.at[0:6], l_send.at[0])
        sent(qown, q_send.at[0])
        sent(part.at[0:31], s_send.at[0])
        sent(zpart.at[0:7], s_send.at[1])
        sent(done.at[0:31], s_send.at[2])


def normalise_kernel(e_ref, fac_ref, rank_ref, p_hbm, r_ref, buf, sem):
    def body(i, carry):
        for j in range(8):
            gq = i * 8 + j
            f = jnp.broadcast_to(fac_ref[pl.ds(gq, 1), :], (128, 128)).T
            ev = e_ref[gq]
            p = jnp.concatenate([ev[:, b * 128:(b + 1) * 128] * f for b in range(4)], axis=1)
            buf[gq] = p.astype(BF16).reshape(8, 16, 512)
        for j in range(8):
            gq = i * 8 + j
            pltpu.make_async_copy(buf.at[gq], p_hbm.at[:, gq], sem.at[i]).start()
        return carry

    lax.fori_loop(0, 4, body, 0)

    lane = lax.broadcasted_iota(jnp.int32, (8, 128), 1) // 16
    sub = lax.broadcasted_iota(jnp.int32, (8, 128), 0)
    for yy in range(NY):
        r = rank_ref[yy * 8:yy * 8 + 8]
        nat = r
        for d in range(1, 8):
            moved = pltpu.roll(pltpu.roll(r, 16 * d, 1), 8 - d, 0)
            nat = jnp.where(lax.rem(lane - sub + 8, 8) == d, moved, nat)
        r_ref[pl.ds(yy, 8, stride=4), :] = nat

    for i in range(4):
        pltpu.make_async_copy(buf.at[0:8], p_hbm.at[:, 0:8], sem.at[i]).wait()


def solution(mesh):
    D = pltpu.SemaphoreType.DMA
    VM = pltpu.VMEM

    def per_device(text_states, text_proj, gallery, logit_scale):
        e, fac, rank = pl.pallas_call(
            gather_score_kernel,
            out_shape=(VM((32, 128, 512), F32), VM((32, 128), F32), VM((32, 128), F32)),
            in_specs=[pl.BlockSpec(memory_space=pl.ANY)] * 4,
            out_specs=(pl.BlockSpec(memory_space=VM),) * 3,
            scratch_shapes=[
                VM((16, NZ, 16, 512), BF16), VM((512, 1024), BF16), VM((512, 1024), BF16),
                pltpu.SMEM((1,), F32), VM((8, 256, 1024), BF16), VM((8, 256, 1024), BF16), VM((512, 512), F32), VM((512, 512), F32),
                VM((32, 4, 128), F32), VM((32, 4, 128), F32), VM((NZ, 4, 128), F32), VM((32, 4, 128), F32),
                D((4,)), D((2,)), D((1,)), D((6,)), D((1,)), D((12,)), D((1,)), D((12,)),
                D((1,)), D((8,)), D((3,)), D((3,)),
            ],
            compiler_params=pltpu.CompilerParams(collective_id=0, has_side_effects=True,
                                                 vmem_limit_bytes=48 * 1024 * 1024),
        )(text_states, text_proj, gallery, logit_scale)
        prob, rank = pl.pallas_call(
            normalise_kernel,
            out_shape=(jax.ShapeDtypeStruct((NZ, 32, 16, 512), BF16), jax.ShapeDtypeStruct((32, 128), F32)),
            in_specs=[pl.BlockSpec(memory_space=VM)] * 3,
            out_specs=(pl.BlockSpec(memory_space=pl.ANY), pl.BlockSpec(memory_space=VM)),
            scratch_shapes=[VM((32, NZ, 16, 512), BF16), D((4,))],
            compiler_params=pltpu.CompilerParams(vmem_limit_bytes=24 * 1024 * 1024),
        )(e, fac, rank)
        return prob.reshape(4096, 512), rank.reshape(4096)

    return jax.shard_map(per_device, mesh=mesh,
                         in_specs=(P("ga", None), P(None, None), P("ga", None), P(None)),
                         out_specs=(P(None, "ga"), P(None)), check_vma=False)
```

```python
import jax
import jax.numpy as jnp
from jax import lax
from jax.experimental import pallas as pl
from jax.experimental.pallas import tpu as pltpu
from jax.sharding import PartitionSpec as P

MESH = pl.DeviceIdType.MESH
NX, NY, NZ, NC = 4, 4, 8, 2
F32, BF16 = jnp.float32, jnp.bfloat16
LOG2E = 1.4426950408889634
F32_MAX = 3.4028235e38
scope = jax.named_scope


def rcopy(src, dst, ss, rs, p):
    return pltpu.make_async_remote_copy(src_ref=src, dst_ref=dst, send_sem=ss, recv_sem=rs,
                                        device_id=(p,), device_id_type=MESH)


def gather_score_kernel(x_hbm, w_hbm, g_hbm, t_hbm,
                        e_ref, fac_ref, rank_ref,
                        xs, wv, gv, tv, qown, qsib, da, db, stat, part, zpart, done,
                        in_sem, a_sem, y_send, y_recv, r_send, r_recv, l_send, l_recv,
                        q_send, q_recv, s_send, s_recv):
    me = lax.axis_index("ga")
    c = lax.rem(me, NC)
    x = lax.rem(me // 2, NX)
    y = lax.rem(me // 8, NY)
    z = me // 32
    pi = lax.rem(me, 32)
    core0 = c == 0
    ml = jnp.where(core0, y, x)
    ll = jnp.where(core0, x, y)

    def dev(zz, yy, xx, cc):
        return ((zz * NY + yy) * NX + xx) * NC + cc

    def dev_lm(zz, lc, mc):
        return dev(zz, jnp.where(core0, mc, lc), jnp.where(core0, lc, mc), c)

    def column(lc, mc):
        return lc * 4 + mc

    mine = column(ll, ml)
    own = xs.at[mine, z]
    load_x = pltpu.make_async_copy(x_hbm, own, in_sem.at[0])
    load_w = pltpu.make_async_copy(w_hbm, wv, in_sem.at[1])
    load_g = pltpu.make_async_copy(g_hbm, gv, in_sem.at[2])
    load_t = pltpu.make_async_copy(t_hbm, tv, in_sem.at[3])
    load_x.start()
    load_t.start()
    load_w.start()
    load_g.start()

    sib = dev(z, y, x, 1 - c)
    z_peers = [dev(lax.rem(z + d, NZ), y, x, c) for d in range(1, NZ)]
    m_next = dev_lm(z, ll, lax.rem(ml + 1, 4))
    m_prev = dev_lm(z, ll, lax.rem(ml + 3, 4))
    right = dev_lm(z, lax.rem(ll + 1, 4), ml)
    left = dev_lm(z, lax.rem(ll + 3, 4), ml)

    barrier = pltpu.get_barrier_semaphore()
    with scope("barrier"):
        peers = [sib, right, left, m_next, m_prev] + z_peers
        for p in peers:
            pl.semaphore_signal(barrier, inc=1, device_id=(p,), device_id_type=MESH)
        pl.semaphore_wait(barrier, len(peers))
        load_x.wait()

    FAR_FIRST = (4, 3, 5, 2, 6, 1, 7)
    for d in FAR_FIRST:
        rcopy(own, own, a_sem.at[0], a_sem.at[1], z_peers[d - 1]).start()
    with scope("first"):
        rcopy(xs.at[0, 0:7], xs.at[0, 0:7], a_sem.at[0], a_sem.at[1], sib).wait_recv()

    OFF = (0, 1, 3, 2)

    def col(lc, j, h):
        return xs.at[column(lc, lax.rem(ml + OFF[j], 4)), 4 * h:4 * h + 4]

    def to_right(lc, j, h, far=0):
        return rcopy(col(lc, j, h), col(lc, j, h), r_send.at[0], r_recv.at[far * 8 + j * 2 + h], right)

    def to_left(lc, j, h, far=0):
        return rcopy(col(lc, j, h), col(lc, j, h), l_send.at[0], l_recv.at[far * 4 + j * 2 + h], left)

    def to_mid(j, h, e, p):
        return rcopy(col(ll, j, h), col(ll, j, h), y_send.at[0], y_recv.at[e], p)

    lp, lm, lf = lax.rem(ll + 1, 4), lax.rem(ll + 3, 4), lax.rem(ll + 2, 4)

    def round_ring(j, h):
        to_right(ll, j, h).start()
        to_left(ll, j, h).start()

    for h in range(2):
        to_mid(0, h, h, m_prev).start()
        to_mid(0, 1 - h, 3 - h, m_next).start()
    round_ring(0, 0)
    round_ring(0, 1)

    with scope("second"):
        to_mid(1, 0, 0, sib).wait_recv()
    to_mid(1, 0, 4, m_prev).start()
    round_ring(1, 0)
    with scope("second"):
        to_mid(2, 1, 3, sib).wait_recv()
    to_mid(2, 1, 5, m_next).start()
    round_ring(2, 1)
    with scope("second"):
        to_mid(1, 1, 1, sib).wait_recv()
    round_ring(1, 1)
    with scope("second"):
        to_mid(2, 0, 2, sib).wait_recv()
    round_ring(2, 0)

    def far_column():
        for h in range(2):
            with scope("third"):
                to_mid(3, h, 4 + h, sib).wait_recv()
            round_ring(3, h)

    def event(j):
        for i in range(2):
            h = 1 - i if j == 2 else i
            to_right(lm, j, h).wait_recv()
            if j < 2:
                to_right(lm, j, h, 1).start()
            to_left(lp, j, h).wait_recv()
            if j >= 2:
                to_left(lp, j, h, 1).start()

    UNITS = (((0, 0), (0, 1)), ((3, 0), (1, 0)), ((0, 3), (0, 2)), ((3, 1), (1, 1)),
             ((3, 3), (1, 3)), ((3, 2), (1, 2)), ((2, 0), (2, 1)), ((2, 3), (2, 2)))

    def unit_of(lc, mc, u):
        return [(lax.rem(lc + a, 4), lax.rem(mc + b, 4)) for a, b in UNITS[u]]

    load_w.wait()
    load_g.wait()
    load_t.wait()
    k2 = jnp.minimum(jnp.exp(jnp.full((1, 1), tv[0], F32)) * LOG2E, F32_MAX)
    place = lax.broadcasted_iota(jnp.int32, (1, 512), 1) + me * 512
    pos = place.astype(F32) / (256 * 512.0)

    def project(u):
        rows = jnp.concatenate([xs[column(lc, mc)].reshape(128, 512) for lc, mc in unit_of(ll, ml, u)], axis=0)
        proj = jnp.dot(rows, wv[...], preferred_element_type=F32)
        inv = 1.0 / jnp.sqrt(jnp.sum(proj * proj, axis=1, keepdims=True))
        qown[u] = (proj * inv).astype(BF16)

    def to_sib(u):
        return rcopy(qown.at[u], qsib.at[u], q_send.at[0], q_recv.at[u], sib)

    def dots(buf, qs):
        q = qs[0] if len(qs) == 1 else jnp.concatenate(qs, axis=0)
        buf[0:256 * len(qs)] = lax.dot_general(q, gv[...], (((1,), (1,)), ((), ())), preferred_element_type=F32)

    def soften(buf, groups):
        n = 128 * len(groups)
        lane = lax.broadcasted_iota(jnp.int32, (n, 128), 1)
        d = buf[0:n]
        dm = jnp.max(d, axis=1, keepdims=True)
        ev = jnp.exp2((d - dm) * k2)
        zs = jnp.sum(ev, axis=1, keepdims=True)
        rs = jnp.sum(ev * pos, axis=1, keepdims=True)
        cols = jnp.where(lane == 0, dm, jnp.where(lane == 1, zs, rs))
        for i, gq in enumerate(groups):
            rows = slice(i * 128, i * 128 + 128)
            e_ref[gq] = ev[rows]
            stat[gq] = cols[rows].T[:4]

    def groups_own(u):
        return [jnp.where(core0, mc * 8 + lc * 2, lc * 8 + mc * 2 + 1) for lc, mc in unit_of(ll, ml, u)]

    def groups_sib(u):
        return [jnp.where(core0, lc * 8 + mc * 2 + 1, mc * 8 + lc * 2) for lc, mc in unit_of(ml, ll, u)]

    def groups_both(uo, us):
        return groups_own(uo) + groups_sib(us)

    def antipode(p):
        return lax.rem(p // 8 + 2, 4) * 8 + lax.rem(lax.rem(p, 8) + 4, 8)

    gm = antipode(pi)

    def send_group(gq):
        @pl.when(gq != gm)
        def _():
            rcopy(stat.at[gq], part.at[pi], s_send.at[0], s_recv.at[0], z * 32 + antipode(gq)).start()

        @pl.when(gq == gm)
        def _():
            part[pi] = stat[gm]

    def send_own(u):
        for gq in groups_own(u):
            send_group(gq)

    def send_sib(u):
        for gq in groups_sib(u):
            send_group(gq)

    project(0)
    to_sib(0).start()
    with scope("event0"):
        event(0)
    project(1)
    dots(da, [qown[0]])
    to_sib(1).start()
    far_column()

    def step(k, now, before):
        with scope("events"):
            if 3 <= k <= 5:
                event(k - 2)
            for h in range(2):
                if k == 6:
                    to_right(lf, 0, h, 1).wait_recv()
                    to_right(lf, 1, h, 1).wait_recv()
                if k == 7:
                    to_left(lf, 2, h, 1).wait_recv()
                    to_left(lf, 3, h, 1).wait_recv()

        with scope("sibwait"):
            to_sib(k - 2).wait_recv()
        if k == 7:
            with scope("project"):
                project(k)
            to_sib(k).start()
        with scope("compute"):
            soften(before, groups_own(0) if k == 2 else groups_both(k - 2, k - 3))
            if k < 7:
                project(k)
            dots(now, [qown[k - 1], qsib[k - 2]])
        if k < 7:
            to_sib(k).start()

    for k in range(2, 8):
        step(k, db if k % 2 == 0 else da, da if k % 2 == 0 else db)
        if k >= 6:
            for u in range(0 if k == 6 else 4, k - 2):
                send_own(u)
            for u in (2,) if k == 6 else (0, 1, 3):
                send_sib(u)
    send_own(5)
    send_sib(4)
    with scope("tail6"):
        to_sib(6).wait_recv()
        soften(da, groups_both(6, 5))
        dots(db, [qown[7], qsib[6]])
    send_own(6)
    send_sib(5)
    with scope("tail7"):
        to_sib(7).wait_recv()
        soften(db, groups_both(7, 6))
        dots(da, [qsib[7]])
    send_own(7)
    send_sib(6)
    with scope("tail8"):
        soften(da, groups_sib(7))
    send_sib(7)

    with scope("s1wait"):
        rcopy(part.at[0:31], part.at[0:31], s_send.at[0], s_recv.at[0], sib).wait_recv()

    def merge(ref):
        ms = ref[:, 0, :]
        m = jnp.max(ms, axis=0, keepdims=True)
        wgt = jnp.exp2((ms - m) * k2)
        return m, jnp.sum(wgt * ref[:, 1, :], axis=0, keepdims=True), jnp.sum(wgt * ref[:, 2, :], axis=0, keepdims=True)

    sub = lax.broadcasted_iota(jnp.int32, (4, 128), 0)

    def tile(a, b, d):
        return jnp.where(sub == 0, a, jnp.where(sub == 1, b, d))

    zpart[z] = tile(*merge(part))
    for d in FAR_FIRST:
        rcopy(zpart.at[z], zpart.at[z], s_send.at[1], s_recv.at[1], z_peers[d - 1]).start()
    with scope("s2wait"):
        rcopy(zpart.at[0:7], zpart.at[0:7], s_send.at[1], s_recv.at[1], sib).wait_recv()
    m, zs, rs = merge(zpart)
    done[gm] = tile(m, 1.0 / zs, rs / zs)

    peers = [(dy, dx, dc) for dy in range(4) for dx in range(4) for dc in range(2)][1:]
    peers.sort(key=lambda p: -min(p[0], 4 - p[0]) - min(p[1], 4 - p[1]))
    with scope("s3send"):
        for dy, dx, dc in peers:
            p = dev(z, lax.rem(y + dy, NY), lax.rem(x + dx, NX), lax.rem(c + dc, NC))
            rcopy(done.at[gm], done.at[gm], s_send.at[2], s_recv.at[2], p).start()

    with scope("s3wait"):
        rcopy(done.at[0:31], done.at[0:31], s_send.at[2], s_recv.at[2], sib).wait_recv()
    fac_ref[...] = jnp.exp2((stat[:, 0, :] - done[:, 0, :]) * k2) * done[:, 1, :]
    rank_ref[...] = done[:, 2, :]

    def sent(ref, sem):
        rcopy(ref, ref, sem, sem, sib).wait_send()

    with scope("drain"):
        sent(xs.at[0, 0:7], a_sem.at[0])
        sent(xs.at[0:3], y_send.at[0])
        sent(xs.at[0:6], r_send.at[0])
        sent(xs.at[0:6], l_send.at[0])
        sent(qown, q_send.at[0])
        sent(part.at[0:31], s_send.at[0])
        sent(zpart.at[0:7], s_send.at[1])
        sent(done.at[0:31], s_send.at[2])


def normalise_kernel(e_ref, fac_ref, rank_ref, p_hbm, r_ref, buf, sem):
    def body(i, carry):
        for j in range(8):
            gq = i * 8 + j
            f = jnp.broadcast_to(fac_ref[pl.ds(gq, 1), :], (128, 128)).T
            ev = e_ref[gq]
            p = jnp.concatenate([ev[:, b * 128:(b + 1) * 128] * f for b in range(4)], axis=1)
            buf[gq] = p.astype(BF16).reshape(8, 16, 512)
        for j in range(8):
            gq = i * 8 + j
            pltpu.make_async_copy(buf.at[gq], p_hbm.at[:, gq], sem.at[i]).start()
        return carry

    lax.fori_loop(0, 4, body, 0)

    lane = lax.broadcasted_iota(jnp.int32, (8, 128), 1) // 16
    sub = lax.broadcasted_iota(jnp.int32, (8, 128), 0)
    for yy in range(NY):
        r = rank_ref[yy * 8:yy * 8 + 8]
        nat = r
        for d in range(1, 8):
            moved = pltpu.roll(pltpu.roll(r, 16 * d, 1), 8 - d, 0)
            nat = jnp.where(lax.rem(lane - sub + 8, 8) == d, moved, nat)
        r_ref[pl.ds(yy, 8, stride=4), :] = nat

    for i in range(4):
        pltpu.make_async_copy(buf.at[0:8], p_hbm.at[:, 0:8], sem.at[i]).wait()


def solution(mesh):
    D = pltpu.SemaphoreType.DMA
    VM = pltpu.VMEM

    def per_device(text_states, text_proj, gallery, logit_scale):
        e, fac, rank = pl.pallas_call(
            gather_score_kernel,
            out_shape=(VM((32, 128, 512), F32), VM((32, 128), F32), VM((32, 128), F32)),
            in_specs=[pl.BlockSpec(memory_space=pl.ANY)] * 4,
            out_specs=(pl.BlockSpec(memory_space=VM),) * 3,
            scratch_shapes=[
                VM((16, NZ, 16, 512), BF16), VM((512, 1024), BF16), VM((512, 1024), BF16),
                pltpu.SMEM((1,), F32), VM((8, 256, 1024), BF16), VM((8, 256, 1024), BF16), VM((512, 512), F32), VM((512, 512), F32),
                VM((32, 4, 128), F32), VM((32, 4, 128), F32), VM((NZ, 4, 128), F32), VM((32, 4, 128), F32),
                D((4,)), D((2,)), D((1,)), D((6,)), D((1,)), D((12,)), D((1,)), D((12,)),
                D((1,)), D((8,)), D((3,)), D((3,)),
            ],
            compiler_params=pltpu.CompilerParams(collective_id=0, has_side_effects=True,
                                                 vmem_limit_bytes=48 * 1024 * 1024),
        )(text_states, text_proj, gallery, logit_scale)
        prob, rank = pl.pallas_call(
            normalise_kernel,
            out_shape=(jax.ShapeDtypeStruct((NZ, 32, 16, 512), BF16), jax.ShapeDtypeStruct((32, 128), F32)),
            in_specs=[pl.BlockSpec(memory_space=VM)] * 3,
            out_specs=(pl.BlockSpec(memory_space=pl.ANY), pl.BlockSpec(memory_space=VM)),
            scratch_shapes=[VM((32, NZ, 16, 512), BF16), D((4,))],
            compiler_params=pltpu.CompilerParams(vmem_limit_bytes=24 * 1024 * 1024),
        )(e, fac, rank)
        return prob.reshape(4096, 512), rank.reshape(4096)

    return jax.shard_map(per_device, mesh=mesh,
                         in_specs=(P("ga", None), P(None, None), P("ga", None), P(None)),
                         out_specs=(P(None, "ga"), P(None)), check_vma=False)
```

```python
import jax
import jax.numpy as jnp
from jax import lax
from jax.experimental import pallas as pl
from jax.experimental.pallas import tpu as pltpu
from jax.sharding import PartitionSpec as P

MESH = pl.DeviceIdType.MESH
NX, NY, NZ, NC = 4, 4, 8, 2
F32, BF16 = jnp.float32, jnp.bfloat16
LOG2E = 1.4426950408889634
F32_MAX = 3.4028235e38
scope = jax.named_scope


def rcopy(src, dst, ss, rs, p):
    return pltpu.make_async_remote_copy(src_ref=src, dst_ref=dst, send_sem=ss, recv_sem=rs,
                                        device_id=(p,), device_id_type=MESH)


def gather_score_kernel(x_hbm, w_hbm, g_hbm, t_hbm,
                        e_ref, fac_ref, rank_ref,
                        xs, wv, gv, tv, qown, qsib, da, db, stat, part, zpart, done,
                        in_sem, a_sem, y_send, y_recv, r_send, r_recv, l_send, l_recv,
                        q_send, q_recv, s_send, s_recv):
    me = lax.axis_index("ga")
    c = lax.rem(me, NC)
    x = lax.rem(me // 2, NX)
    y = lax.rem(me // 8, NY)
    z = me // 32
    pi = lax.rem(me, 32)
    core0 = c == 0
    ml = jnp.where(core0, y, x)
    ll = jnp.where(core0, x, y)

    def dev(zz, yy, xx, cc):
        return ((zz * NY + yy) * NX + xx) * NC + cc

    def dev_lm(zz, lc, mc):
        return dev(zz, jnp.where(core0, mc, lc), jnp.where(core0, lc, mc), c)

    def column(lc, mc):
        return lc * 4 + mc

    mine = column(ll, ml)
    own = xs.at[mine, z]
    load_x = pltpu.make_async_copy(x_hbm, own, in_sem.at[0])
    load_w = pltpu.make_async_copy(w_hbm, wv, in_sem.at[1])
    load_g = pltpu.make_async_copy(g_hbm, gv, in_sem.at[2])
    load_t = pltpu.make_async_copy(t_hbm, tv, in_sem.at[3])
    load_x.start()
    load_t.start()
    load_w.start()
    load_g.start()

    sib = dev(z, y, x, 1 - c)
    z_peers = [dev(lax.rem(z + d, NZ), y, x, c) for d in range(1, NZ)]
    m_next = dev_lm(z, ll, lax.rem(ml + 1, 4))
    m_prev = dev_lm(z, ll, lax.rem(ml + 3, 4))
    right = dev_lm(z, lax.rem(ll + 1, 4), ml)
    left = dev_lm(z, lax.rem(ll + 3, 4), ml)

    barrier = pltpu.get_barrier_semaphore()
    with scope("barrier"):
        peers = [sib, right, left, m_next, m_prev] + z_peers
        for p in peers:
            pl.semaphore_signal(barrier, inc=1, device_id=(p,), device_id_type=MESH)
        pl.semaphore_wait(barrier, len(peers))
        load_x.wait()

    FAR_FIRST = (4, 3, 5, 2, 6, 1, 7)
    near = z // 4
    for d in FAR_FIRST:
        same = lax.rem(z + d, NZ) // 4 == near
        rcopy(own, own, a_sem.at[0], a_sem.at[jnp.where(same, 1, 2)], z_peers[d - 1]).start()

    OFF = (0, 1, 3, 2)

    def col(lc, j, h):
        return xs.at[column(lc, lax.rem(ml + OFF[j], 4)), pl.ds(4 * (near if h == 0 else 1 - near), 4)]

    def to_right(lc, j, h, far=0):
        return rcopy(col(lc, j, h), col(lc, j, h), r_send.at[0], r_recv.at[far * 8 + j * 2 + h], right)

    def to_left(lc, j, h, far=0):
        return rcopy(col(lc, j, h), col(lc, j, h), l_send.at[0], l_recv.at[far * 4 + j * 2 + h], left)

    def to_mid(j, h, e, p):
        return rcopy(col(ll, j, h), col(ll, j, h), y_send.at[0], y_recv.at[e], p)

    lp, lm, lf = lax.rem(ll + 1, 4), lax.rem(ll + 3, 4), lax.rem(ll + 2, 4)

    def round_ring(j, h):
        to_right(ll, j, h).start()
        to_left(ll, j, h).start()

    for h in range(2):
        with scope("first"):
            got = xs.at[0, 0:3 + h]
            rcopy(got, got, a_sem.at[0], a_sem.at[1 + h], sib).wait_recv()
        to_mid(0, h, h, m_prev).start()
        to_mid(0, h, 2 + h, m_next).start()
        round_ring(0, h)

    with scope("second"):
        to_mid(1, 0, 0, sib).wait_recv()
    to_mid(1, 0, 4, m_prev).start()
    round_ring(1, 0)
    with scope("second"):
        to_mid(2, 0, 2, sib).wait_recv()
    round_ring(2, 0)
    with scope("second"):
        to_mid(2, 1, 3, sib).wait_recv()
    to_mid(2, 1, 5, m_next).start()
    with scope("second"):
        to_mid(1, 1, 1, sib).wait_recv()
    round_ring(1, 1)
    round_ring(2, 1)

    def far_column():
        for h in range(2):
            with scope("third"):
                to_mid(3, h, 4 + h, sib).wait_recv()
            round_ring(3, h)

    def event(j):
        for h in range(2):
            to_right(lm, j, h).wait_recv()
            if j < 2:
                to_right(lm, j, h, 1).start()
            to_left(lp, j, h).wait_recv()
            if j >= 2:
                to_left(lp, j, h, 1).start()

    UNITS = (((0, 0), (0, 1)), ((3, 0), (1, 0)), ((0, 3), (0, 2)), ((3, 1), (1, 1)),
             ((3, 3), (1, 3)), ((3, 2), (1, 2)), ((2, 0), (2, 1)), ((2, 3), (2, 2)))

    def unit_of(lc, mc, u):
        return [(lax.rem(lc + a, 4), lax.rem(mc + b, 4)) for a, b in UNITS[u]]

    load_w.wait()
    load_g.wait()
    load_t.wait()
    k2 = jnp.minimum(jnp.exp(jnp.full((1, 1), tv[0], F32)) * LOG2E, F32_MAX)
    place = lax.broadcasted_iota(jnp.int32, (1, 512), 1) + me * 512
    pos = place.astype(F32) / (256 * 512.0)

    def project(u):
        rows = jnp.concatenate([xs[column(lc, mc)].reshape(128, 512) for lc, mc in unit_of(ll, ml, u)], axis=0)
        proj = jnp.dot(rows, wv[...], preferred_element_type=F32)
        inv = 1.0 / jnp.sqrt(jnp.sum(proj * proj, axis=1, keepdims=True))
        qown[u] = (proj * inv).astype(BF16)

    def to_sib(u):
        return rcopy(qown.at[u], qsib.at[u], q_send.at[0], q_recv.at[u], sib)

    def dots(buf, qs):
        q = qs[0] if len(qs) == 1 else jnp.concatenate(qs, axis=0)
        buf[0:256 * len(qs)] = lax.dot_general(q, gv[...], (((1,), (1,)), ((), ())), preferred_element_type=F32)

    def soften(buf, groups):
        n = 128 * len(groups)
        lane = lax.broadcasted_iota(jnp.int32, (n, 128), 1)
        d = buf[0:n]
        dm = jnp.max(d, axis=1, keepdims=True)
        ev = jnp.exp2((d - dm) * k2)
        zs = jnp.sum(ev, axis=1, keepdims=True)
        rs = jnp.sum(ev * pos, axis=1, keepdims=True)
        cols = jnp.where(lane == 0, dm, jnp.where(lane == 1, zs, rs))
        for i, gq in enumerate(groups):
            rows = slice(i * 128, i * 128 + 128)
            e_ref[gq] = ev[rows]
            stat[gq] = cols[rows].T[:4]

    def groups_own(u):
        return [jnp.where(core0, mc * 8 + lc * 2, lc * 8 + mc * 2 + 1) for lc, mc in unit_of(ll, ml, u)]

    def groups_sib(u):
        return [jnp.where(core0, lc * 8 + mc * 2 + 1, mc * 8 + lc * 2) for lc, mc in unit_of(ml, ll, u)]

    def groups_both(uo, us):
        return groups_own(uo) + groups_sib(us)

    def antipode(p):
        return lax.rem(p // 8 + 2, 4) * 8 + lax.rem(lax.rem(p, 8) + 4, 8)

    gm = antipode(pi)

    def send_group(gq):
        @pl.when(gq != gm)
        def _():
            rcopy(stat.at[gq], part.at[pi], s_send.at[0], s_recv.at[0], z * 32 + antipode(gq)).start()

        @pl.when(gq == gm)
        def _():
            part[pi] = stat[gm]

    def send_own(u):
        for gq in groups_own(u):
            send_group(gq)

    def send_sib(u):
        for gq in groups_sib(u):
            send_group(gq)

    project(0)
    to_sib(0).start()
    with scope("event0"):
        event(0)
    project(1)
    dots(da, [qown[0]])
    to_sib(1).start()
    far_column()

    def step(k, now, before):
        with scope("events"):
            if 3 <= k <= 5:
                event(k - 2)
            for h in range(2):
                if k == 6:
                    to_right(lf, 0, h, 1).wait_recv()
                    to_right(lf, 1, h, 1).wait_recv()
                if k == 7:
                    to_left(lf, 2, h, 1).wait_recv()
                    to_left(lf, 3, h, 1).wait_recv()

        with scope("sibwait"):
            to_sib(k - 2).wait_recv()
        if k == 7:
            with scope("project"):
                project(k)
            to_sib(k).start()
        with scope("compute"):
            soften(before, groups_own(0) if k == 2 else groups_both(k - 2, k - 3))
            if k < 7:
                project(k)
            dots(now, [qown[k - 1], qsib[k - 2]])
        if k < 7:
            to_sib(k).start()

    for k in range(2, 8):
        step(k, db if k % 2 == 0 else da, da if k % 2 == 0 else db)
        if k >= 6:
            for u in range(0 if k == 6 else 4, k - 2):
                send_own(u)
            for u in (2,) if k == 6 else (0, 1, 3):
                send_sib(u)
    send_own(5)
    send_sib(4)
    with scope("tail6"):
        to_sib(6).wait_recv()
        soften(da, groups_both(6, 5))
        dots(db, [qown[7], qsib[6]])
    send_own(6)
    send_sib(5)
    with scope("tail7"):
        to_sib(7).wait_recv()
        soften(db, groups_both(7, 6))
        dots(da, [qsib[7]])
    send_own(7)
    send_sib(6)
    with scope("tail8"):
        soften(da, groups_sib(7))
    send_sib(7)

    with scope("s1wait"):
        rcopy(part.at[0:31], part.at[0:31], s_send.at[0], s_recv.at[0], sib).wait_recv()

    def merge(ref):
        ms = ref[:, 0, :]
        m = jnp.max(ms, axis=0, keepdims=True)
        wgt = jnp.exp2((ms - m) * k2)
        return m, jnp.sum(wgt * ref[:, 1, :], axis=0, keepdims=True), jnp.sum(wgt * ref[:, 2, :], axis=0, keepdims=True)

    sub = lax.broadcasted_iota(jnp.int32, (4, 128), 0)

    def tile(a, b, d):
        return jnp.where(sub == 0, a, jnp.where(sub == 1, b, d))

    zpart[z] = tile(*merge(part))
    for d in FAR_FIRST:
        rcopy(zpart.at[z], zpart.at[z], s_send.at[1], s_recv.at[1], z_peers[d - 1]).start()
    with scope("s2wait"):
        rcopy(zpart.at[0:7], zpart.at[0:7], s_send.at[1], s_recv.at[1], sib).wait_recv()
    m, zs, rs = merge(zpart)
    done[gm] = tile(m, 1.0 / zs, rs / zs)

    peers = [(dy, dx, dc) for dy in range(4) for dx in range(4) for dc in range(2)][1:]
    peers.sort(key=lambda p: -min(p[0], 4 - p[0]) - min(p[1], 4 - p[1]))
    with scope("s3send"):
        for dy, dx, dc in peers:
            p = dev(z, lax.rem(y + dy, NY), lax.rem(x + dx, NX), lax.rem(c + dc, NC))
            rcopy(done.at[gm], done.at[gm], s_send.at[2], s_recv.at[2], p).start()

    with scope("s3wait"):
        rcopy(done.at[0:31], done.at[0:31], s_send.at[2], s_recv.at[2], sib).wait_recv()
    fac_ref[...] = jnp.exp2((stat[:, 0, :] - done[:, 0, :]) * k2) * done[:, 1, :]
    rank_ref[...] = done[:, 2, :]

    def sent(ref, sem):
        rcopy(ref, ref, sem, sem, sib).wait_send()

    with scope("drain"):
        sent(xs.at[0, 0:7], a_sem.at[0])
        sent(xs.at[0:3], y_send.at[0])
        sent(xs.at[0:6], r_send.at[0])
        sent(xs.at[0:6], l_send.at[0])
        sent(qown, q_send.at[0])
        sent(part.at[0:31], s_send.at[0])
        sent(zpart.at[0:7], s_send.at[1])
        sent(done.at[0:31], s_send.at[2])


def normalise_kernel(e_ref, fac_ref, rank_ref, p_hbm, r_ref, buf, sem):
    def out(i):
        return pltpu.make_async_copy(buf.at[:, pl.ds(8 * i, 8)], p_hbm.at[:, pl.ds(8 * i, 8)], sem.at[i])

    def body(i, carry):
        for j in range(8):
            gq = i * 8 + j
            f = jnp.broadcast_to(fac_ref[pl.ds(gq, 1), :], (128, 128)).T
            ev = e_ref[gq]
            p = jnp.concatenate([ev[:, b * 128:(b + 1) * 128] * f for b in range(4)], axis=1)
            buf[:, gq] = p.astype(BF16).reshape(8, 16, 512)
        out(i).start()
        return carry

    lax.fori_loop(0, 4, body, 0)

    lane = lax.broadcasted_iota(jnp.int32, (8, 128), 1) // 16
    sub = lax.broadcasted_iota(jnp.int32, (8, 128), 0)
    for yy in range(NY):
        r = rank_ref[yy * 8:yy * 8 + 8]
        nat = r
        for d in range(1, 8):
            moved = pltpu.roll(pltpu.roll(r, 16 * d, 1), 8 - d, 0)
            nat = jnp.where(lax.rem(lane - sub + 8, 8) == d, moved, nat)
        r_ref[pl.ds(yy, 8, stride=4), :] = nat

    for i in range(4):
        out(i).wait()


def solution(mesh):
    D = pltpu.SemaphoreType.DMA
    VM = pltpu.VMEM

    def per_device(text_states, text_proj, gallery, logit_scale):
        e, fac, rank = pl.pallas_call(
            gather_score_kernel,
            out_shape=(VM((32, 128, 512), F32), VM((32, 128), F32), VM((32, 128), F32)),
            in_specs=[pl.BlockSpec(memory_space=pl.ANY)] * 4,
            out_specs=(pl.BlockSpec(memory_space=VM),) * 3,
            scratch_shapes=[
                VM((16, NZ, 16, 512), BF16), VM((512, 1024), BF16), VM((512, 1024), BF16),
                pltpu.SMEM((1,), F32), VM((8, 256, 1024), BF16), VM((8, 256, 1024), BF16), VM((512, 512), F32), VM((512, 512), F32),
                VM((32, 4, 128), F32), VM((32, 4, 128), F32), VM((NZ, 4, 128), F32), VM((32, 4, 128), F32),
                D((4,)), D((3,)), D((1,)), D((6,)), D((1,)), D((12,)), D((1,)), D((12,)),
                D((1,)), D((8,)), D((3,)), D((3,)),
            ],
            compiler_params=pltpu.CompilerParams(collective_id=0, has_side_effects=True,
                                                 vmem_limit_bytes=48 * 1024 * 1024),
        )(text_states, text_proj, gallery, logit_scale)
        prob, rank = pl.pallas_call(
            normalise_kernel,
            out_shape=(jax.ShapeDtypeStruct((NZ, 32, 16, 512), BF16), jax.ShapeDtypeStruct((32, 128), F32)),
            in_specs=[pl.BlockSpec(memory_space=VM)] * 3,
            out_specs=(pl.BlockSpec(memory_space=pl.ANY), pl.BlockSpec(memory_space=VM)),
            scratch_shapes=[VM((NZ, 32, 16, 512), BF16), D((4,))],
            compiler_params=pltpu.CompilerParams(vmem_limit_bytes=24 * 1024 * 1024),
        )(e, fac, rank)
        return prob.reshape(4096, 512), rank.reshape(4096)

    return jax.shard_map(per_device, mesh=mesh,
                         in_specs=(P("ga", None), P(None, None), P("ga", None), P(None)),
                         out_specs=(P(None, "ga"), P(None)), check_vma=False)
```

```python
import jax
import jax.numpy as jnp
from jax import lax
from jax.experimental import pallas as pl
from jax.experimental.pallas import tpu as pltpu
from jax.sharding import PartitionSpec as P

MESH = pl.DeviceIdType.MESH
NX, NY, NZ, NC = 4, 4, 8, 2
F32, BF16 = jnp.float32, jnp.bfloat16
LOG2E = 1.4426950408889634
F32_MAX = 3.4028235e38
scope = jax.named_scope


def rcopy(src, dst, ss, rs, p):
    return pltpu.make_async_remote_copy(src_ref=src, dst_ref=dst, send_sem=ss, recv_sem=rs,
                                        device_id=(p,), device_id_type=MESH)


def gather_score_kernel(x_hbm, w_hbm, g_hbm, t_hbm,
                        e_ref, fac_ref, rank_ref,
                        xs, wv, gv, tv, qown, qsib, da, db, stat, part, zpart, done,
                        in_sem, a_sem, y_send, y_recv, r_send, r_recv, l_send, l_recv,
                        q_send, q_recv, s_send, s_recv):
    me = lax.axis_index("ga")
    c = lax.rem(me, NC)
    x = lax.rem(me // 2, NX)
    y = lax.rem(me // 8, NY)
    z = me // 32
    pi = lax.rem(me, 32)
    core0 = c == 0
    ml = jnp.where(core0, y, x)
    ll = jnp.where(core0, x, y)

    def dev(zz, yy, xx, cc):
        return ((zz * NY + yy) * NX + xx) * NC + cc

    def dev_lm(zz, lc, mc):
        return dev(zz, jnp.where(core0, mc, lc), jnp.where(core0, lc, mc), c)

    def column(lc, mc):
        return lc * 4 + mc

    mine = column(ll, ml)
    own = xs.at[mine, z]
    load_x = pltpu.make_async_copy(x_hbm, own, in_sem.at[0])
    load_w = pltpu.make_async_copy(w_hbm, wv, in_sem.at[1])
    load_g = pltpu.make_async_copy(g_hbm, gv, in_sem.at[2])
    load_t = pltpu.make_async_copy(t_hbm, tv, in_sem.at[3])
    load_x.start()
    load_t.start()
    load_w.start()
    load_g.start()

    sib = dev(z, y, x, 1 - c)
    z_peers = [dev(lax.rem(z + d, NZ), y, x, c) for d in range(1, NZ)]
    m_next = dev_lm(z, ll, lax.rem(ml + 1, 4))
    m_prev = dev_lm(z, ll, lax.rem(ml + 3, 4))
    right = dev_lm(z, lax.rem(ll + 1, 4), ml)
    left = dev_lm(z, lax.rem(ll + 3, 4), ml)

    barrier = pltpu.get_barrier_semaphore()
    with scope("barrier"):
        peers = [sib, right, left, m_next, m_prev] + z_peers
        for p in peers:
            pl.semaphore_signal(barrier, inc=1, device_id=(p,), device_id_type=MESH)
        pl.semaphore_wait(barrier, len(peers))
        load_x.wait()

    FAR_FIRST = (4, 3, 5, 2, 6, 1, 7)
    near = z // 4
    for d in FAR_FIRST:
        same = lax.rem(z + d, NZ) // 4 == near
        rcopy(own, own, a_sem.at[0], a_sem.at[jnp.where(same, 1, 2)], z_peers[d - 1]).start()

    OFF = (0, 1, 3, 2)

    def col(lc, j, h):
        return xs.at[column(lc, lax.rem(ml + OFF[j], 4)), pl.ds(4 * (near if h == 0 else 1 - near), 4)]

    def to_right(lc, j, h, far=0):
        return rcopy(col(lc, j, h), col(lc, j, h), r_send.at[0], r_recv.at[far * 8 + j * 2 + h], right)

    def to_left(lc, j, h, far=0):
        return rcopy(col(lc, j, h), col(lc, j, h), l_send.at[0], l_recv.at[far * 4 + j * 2 + h], left)

    def to_mid(j, h, e, p):
        return rcopy(col(ll, j, h), col(ll, j, h), y_send.at[0], y_recv.at[e], p)

    lp, lm, lf = lax.rem(ll + 1, 4), lax.rem(ll + 3, 4), lax.rem(ll + 2, 4)

    def round_ring(j, h):
        to_right(ll, j, h).start()
        to_left(ll, j, h).start()

    for h in range(2):
        with scope("first"):
            got = xs.at[0, 0:3 + h]
            rcopy(got, got, a_sem.at[0], a_sem.at[1 + h], sib).wait_recv()
        to_mid(0, h, h, m_prev).start()
        to_mid(0, h, 2 + h, m_next).start()
        round_ring(0, h)

    def mid_columns():
        with scope("second"):
            to_mid(1, 0, 0, sib).wait_recv()
        to_mid(1, 0, 4, m_prev).start()
        round_ring(1, 0)
        with scope("second"):
            to_mid(2, 0, 2, sib).wait_recv()
        round_ring(2, 0)
        with scope("second"):
            to_mid(2, 1, 3, sib).wait_recv()
        to_mid(2, 1, 5, m_next).start()
        with scope("second"):
            to_mid(1, 1, 1, sib).wait_recv()
        round_ring(1, 1)
        round_ring(2, 1)

    def far_column():
        for h in range(2):
            with scope("third"):
                to_mid(3, h, 4 + h, sib).wait_recv()
            round_ring(3, h)

    def from_left(j):
        for h in range(2):
            to_right(lm, j, h).wait_recv()
            if j < 2:
                to_right(lm, j, h, 1).start()

    def from_right(j):
        for h in range(2):
            to_left(lp, j, h).wait_recv()
            if j >= 2:
                to_left(lp, j, h, 1).start()

    def far_left(j):
        for h in range(2):
            to_right(lf, j, h, 1).wait_recv()

    def far_right(j):
        for h in range(2):
            to_left(lf, j, h, 1).wait_recv()

    UNITS = (((0, 0),), ((0, 1), (0, 3)), ((3, 0), (1, 0)), ((0, 2), (3, 1)), ((1, 1), (3, 3)),
             ((1, 3), (3, 2)), ((1, 2), (2, 0)), ((2, 1), (2, 3)), ((2, 2),))

    def unit_of(lc, mc, u):
        return [(lax.rem(lc + a, 4), lax.rem(mc + b, 4)) for a, b in UNITS[u]]

    def events(k):
        if k == 2:
            from_left(0)
            from_right(0)
        if k == 3:
            far_column()
            from_left(1)
        if k == 4:
            from_right(1)
            from_left(2)
        if k == 5:
            from_right(2)
            from_left(3)
        if k == 6:
            from_right(3)
            far_left(0)
        if k == 7:
            far_left(1)
            far_right(2)
        if k == 8:
            far_right(3)

    load_w.wait()
    load_g.wait()
    load_t.wait()
    k2 = jnp.minimum(jnp.exp(jnp.full((1, 1), tv[0], F32)) * LOG2E, F32_MAX)
    place = lax.broadcasted_iota(jnp.int32, (1, 512), 1) + me * 512
    pos = place.astype(F32) / (256 * 512.0)

    def q_of(ref, u):
        return ref.at[u, 0:128 * len(UNITS[u])]

    def project(u):
        rows = jnp.concatenate([xs[column(lc, mc)].reshape(128, 512) for lc, mc in unit_of(ll, ml, u)], axis=0)
        proj = jnp.dot(rows, wv[...], preferred_element_type=F32)
        inv = 1.0 / jnp.sqrt(jnp.sum(proj * proj, axis=1, keepdims=True))
        q_of(qown, u)[...] = (proj * inv).astype(BF16)

    def to_sib(u):
        return rcopy(q_of(qown, u), q_of(qsib, u), q_send.at[0], q_recv.at[u], sib)

    def dots(buf, uo, us):
        q = jnp.concatenate([q_of(qown, u)[...] for u in uo] + [q_of(qsib, u)[...] for u in us], axis=0)
        buf[0:q.shape[0]] = lax.dot_general(q, gv[...], (((1,), (1,)), ((), ())), preferred_element_type=F32)

    def soften(buf, groups):
        n = 128 * len(groups)
        lane = lax.broadcasted_iota(jnp.int32, (n, 128), 1)
        d = buf[0:n]
        dm = jnp.max(d, axis=1, keepdims=True)
        ev = jnp.exp2((d - dm) * k2)
        zs = jnp.sum(ev, axis=1, keepdims=True)
        rs = jnp.sum(ev * pos, axis=1, keepdims=True)
        cols = jnp.where(lane == 0, dm, jnp.where(lane == 1, zs, rs))
        for i, gq in enumerate(groups):
            rows = slice(i * 128, i * 128 + 128)
            e_ref[gq] = ev[rows]
            stat[gq] = cols[rows].T[:4]

    def groups_own(u):
        return [jnp.where(core0, mc * 8 + lc * 2, lc * 8 + mc * 2 + 1) for lc, mc in unit_of(ll, ml, u)]

    def groups_sib(u):
        return [jnp.where(core0, lc * 8 + mc * 2 + 1, mc * 8 + lc * 2) for lc, mc in unit_of(ml, ll, u)]

    def groups_of(uo, us):
        return sum([groups_own(u) for u in uo] + [groups_sib(u) for u in us], [])

    def antipode(p):
        return lax.rem(p // 8 + 2, 4) * 8 + lax.rem(lax.rem(p, 8) + 4, 8)

    gm = antipode(pi)

    def send_group(gq):
        @pl.when(gq != gm)
        def _():
            rcopy(stat.at[gq], part.at[pi], s_send.at[0], s_recv.at[0], z * 32 + antipode(gq)).start()

        @pl.when(gq == gm)
        def _():
            part[pi] = stat[gm]

    LAST = 8

    def scored(k):
        return [u for u in (k - 1,) if 0 <= u <= LAST], [u for u in (k - 2,) if 0 <= u <= LAST]

    def step(k):
        now, before = (da, db) if k % 2 else (db, da)
        with scope("events"):
            events(k)
        uo, us = scored(k)
        with scope("sibwait"):
            for u in us:
                to_sib(u).wait_recv()
        if k == LAST:
            with scope("project"):
                project(k)
            to_sib(k).start()
        with scope("compute"):
            if k >= 2:
                soften(before, groups_of(*scored(k - 1)))
            if k < LAST:
                project(k)
            if uo or us:
                dots(now, uo, us)
        if k < LAST:
            to_sib(k).start()

    SENDS = {6: ((0, 1, 2, 3), (1,)), 7: ((4,), (2, 3)), 8: ((5, 6), (0, 4, 5)), 9: ((7,), (6,)), 10: ((8,), (7,)),
             11: ((), (8,))}

    def sends(k):
        for u in SENDS[k][0]:
            for gq in groups_own(u):
                send_group(gq)
        for u in SENDS[k][1]:
            for gq in groups_sib(u):
                send_group(gq)

    step(0)
    mid_columns()
    for k in range(1, LAST + 1):
        step(k)
        if k in SENDS:
            sends(k)
    with scope("tail6"):
        to_sib(LAST - 1).wait_recv()
        soften(db, groups_of(*scored(LAST)))
        dots(da, *scored(LAST + 1))
    sends(LAST + 1)
    with scope("tail7"):
        to_sib(LAST).wait_recv()
        soften(da, groups_of(*scored(LAST + 1)))
        dots(db, *scored(LAST + 2))
    sends(LAST + 2)
    with scope("tail8"):
        soften(db, groups_of(*scored(LAST + 2)))
    sends(LAST + 3)

    with scope("s1wait"):
        rcopy(part.at[0:31], part.at[0:31], s_send.at[0], s_recv.at[0], sib).wait_recv()

    def merge(ref):
        ms = ref[:, 0, :]
        m = jnp.max(ms, axis=0, keepdims=True)
        wgt = jnp.exp2((ms - m) * k2)
        return m, jnp.sum(wgt * ref[:, 1, :], axis=0, keepdims=True), jnp.sum(wgt * ref[:, 2, :], axis=0, keepdims=True)

    sub = lax.broadcasted_iota(jnp.int32, (4, 128), 0)

    def tile(a, b, d):
        return jnp.where(sub == 0, a, jnp.where(sub == 1, b, d))

    zpart[z] = tile(*merge(part))
    for d in FAR_FIRST:
        rcopy(zpart.at[z], zpart.at[z], s_send.at[1], s_recv.at[1], z_peers[d - 1]).start()
    with scope("s2wait"):
        rcopy(zpart.at[0:7], zpart.at[0:7], s_send.at[1], s_recv.at[1], sib).wait_recv()
    m, zs, rs = merge(zpart)
    done[gm] = tile(m, 1.0 / zs, rs / zs)

    peers = [(dy, dx, dc) for dy in range(4) for dx in range(4) for dc in range(2)][1:]
    peers.sort(key=lambda p: -min(p[0], 4 - p[0]) - min(p[1], 4 - p[1]))
    with scope("s3send"):
        for dy, dx, dc in peers:
            p = dev(z, lax.rem(y + dy, NY), lax.rem(x + dx, NX), lax.rem(c + dc, NC))
            rcopy(done.at[gm], done.at[gm], s_send.at[2], s_recv.at[2], p).start()

    with scope("s3wait"):
        rcopy(done.at[0:31], done.at[0:31], s_send.at[2], s_recv.at[2], sib).wait_recv()
    fac_ref[...] = jnp.exp2((stat[:, 0, :] - done[:, 0, :]) * k2) * done[:, 1, :]
    rank_ref[...] = done[:, 2, :]

    def sent(ref, sem):
        rcopy(ref, ref, sem, sem, sib).wait_send()

    with scope("drain"):
        sent(xs.at[0, 0:7], a_sem.at[0])
        sent(xs.at[0:3], y_send.at[0])
        sent(xs.at[0:6], r_send.at[0])
        sent(xs.at[0:6], l_send.at[0])
        sent(qown.at[0:8], q_send.at[0])
        sent(part.at[0:31], s_send.at[0])
        sent(zpart.at[0:7], s_send.at[1])
        sent(done.at[0:31], s_send.at[2])


def normalise_kernel(e_ref, fac_ref, rank_ref, p_hbm, r_hbm, buf, nat_ref, sem):
    def out(i):
        return pltpu.make_async_copy(buf.at[:, pl.ds(4 * i, 4)], p_hbm.at[:, pl.ds(4 * i, 4)], sem.at[i])

    def body(i, carry):
        for j in range(4):
            gq = i * 4 + j
            f = jnp.broadcast_to(fac_ref[pl.ds(gq, 1), :], (128, 128)).T
            ev = e_ref[gq]
            p = jnp.concatenate([ev[:, b * 128:(b + 1) * 128] * f for b in range(4)], axis=1)
            buf[:, gq] = p.astype(BF16).reshape(8, 16, 512)
        out(i).start()
        return carry

    lax.fori_loop(0, 8, body, 0)

    lane = lax.broadcasted_iota(jnp.int32, (8, 128), 1) // 16
    sub = lax.broadcasted_iota(jnp.int32, (8, 128), 0)
    for yy in range(NY):
        r = rank_ref[yy * 8:yy * 8 + 8]
        nat = r
        for d in range(1, 8):
            moved = pltpu.roll(pltpu.roll(r, 16 * d, 1), 8 - d, 0)
            nat = jnp.where(lax.rem(lane - sub + 8, 8) == d, moved, nat)
        nat_ref[pl.ds(yy, 8, stride=4), :] = nat
    out_rank = pltpu.make_async_copy(nat_ref, r_hbm, sem.at[8])
    out_rank.start()

    for i in range(8):
        out(i).wait()
    out_rank.wait()


def solution(mesh):
    D = pltpu.SemaphoreType.DMA
    VM = pltpu.VMEM

    def per_device(text_states, text_proj, gallery, logit_scale):
        e, fac, rank = pl.pallas_call(
            gather_score_kernel,
            out_shape=(VM((32, 128, 512), F32), VM((32, 128), F32), VM((32, 128), F32)),
            in_specs=[pl.BlockSpec(memory_space=pl.ANY)] * 4,
            out_specs=(pl.BlockSpec(memory_space=VM),) * 3,
            scratch_shapes=[
                VM((16, NZ, 16, 512), BF16), VM((512, 1024), BF16), VM((512, 1024), BF16),
                pltpu.SMEM((1,), F32), VM((9, 256, 1024), BF16), VM((9, 256, 1024), BF16), VM((512, 512), F32), VM((512, 512), F32),
                VM((32, 4, 128), F32), VM((32, 4, 128), F32), VM((NZ, 4, 128), F32), VM((32, 4, 128), F32),
                D((4,)), D((3,)), D((1,)), D((6,)), D((1,)), D((12,)), D((1,)), D((12,)),
                D((1,)), D((9,)), D((3,)), D((3,)),
            ],
            compiler_params=pltpu.CompilerParams(collective_id=0, has_side_effects=True,
                                                 vmem_limit_bytes=48 * 1024 * 1024),
        )(text_states, text_proj, gallery, logit_scale)
        prob, rank = pl.pallas_call(
            normalise_kernel,
            out_shape=(jax.ShapeDtypeStruct((NZ, 32, 16, 512), BF16), jax.ShapeDtypeStruct((32, 128), F32)),
            in_specs=[pl.BlockSpec(memory_space=VM)] * 3,
            out_specs=(pl.BlockSpec(memory_space=pl.ANY),) * 2,
            scratch_shapes=[VM((NZ, 32, 16, 512), BF16), VM((32, 128), F32), D((9,))],
            compiler_params=pltpu.CompilerParams(vmem_limit_bytes=24 * 1024 * 1024),
        )(e, fac, rank)
        return prob.reshape(4096, 512), rank.reshape(4096)

    return jax.shard_map(per_device, mesh=mesh,
                         in_specs=(P("ga", None), P(None, None), P("ga", None), P(None)),
                         out_specs=(P(None, "ga"), P(None)), check_vma=False)
```

```python
import jax
import jax.numpy as jnp
from jax import lax
from jax.experimental import pallas as pl
from jax.experimental.pallas import tpu as pltpu
from jax.sharding import PartitionSpec as P

MESH = pl.DeviceIdType.MESH
NX, NY, NZ, NC = 4, 4, 8, 2
F32, BF16 = jnp.float32, jnp.bfloat16
LOG2E = 1.4426950408889634
F32_MAX = 3.4028235e38
scope = jax.named_scope


def rcopy(src, dst, ss, rs, p):
    return pltpu.make_async_remote_copy(src_ref=src, dst_ref=dst, send_sem=ss, recv_sem=rs,
                                        device_id=(p,), device_id_type=MESH)


def gather_score_kernel(x_hbm, w_hbm, g_hbm, t_hbm,
                        e_ref, fac_ref, rank_ref,
                        xs, wv, gv, tv, qown, qsib, da, db, stat, part, zpart, done,
                        in_sem, a_sem, y_send, y_recv, r_send, r_recv, l_send, l_recv,
                        q_send, q_recv, s_send, s_recv):
    me = lax.axis_index("ga")
    c = lax.rem(me, NC)
    x = lax.rem(me // 2, NX)
    y = lax.rem(me // 8, NY)
    z = me // 32
    pi = lax.rem(me, 32)
    core0 = c == 0
    ml = jnp.where(core0, y, x)
    ll = jnp.where(core0, x, y)

    def dev(zz, yy, xx, cc):
        return ((zz * NY + yy) * NX + xx) * NC + cc

    def dev_lm(zz, lc, mc):
        return dev(zz, jnp.where(core0, mc, lc), jnp.where(core0, lc, mc), c)

    def column(lc, mc):
        return lc * 4 + mc

    mine = column(ll, ml)
    own = xs.at[mine, z]
    load_x = pltpu.make_async_copy(x_hbm, own, in_sem.at[0])
    load_w = pltpu.make_async_copy(w_hbm, wv, in_sem.at[1])
    load_g = pltpu.make_async_copy(g_hbm, gv, in_sem.at[2])
    load_t = pltpu.make_async_copy(t_hbm, tv, in_sem.at[3])
    load_x.start()
    load_t.start()
    load_w.start()
    load_g.start()

    sib = dev(z, y, x, 1 - c)
    z_peers = [dev(lax.rem(z + d, NZ), y, x, c) for d in range(1, NZ)]
    m_next = dev_lm(z, ll, lax.rem(ml + 1, 4))
    m_prev = dev_lm(z, ll, lax.rem(ml + 3, 4))
    right = dev_lm(z, lax.rem(ll + 1, 4), ml)
    left = dev_lm(z, lax.rem(ll + 3, 4), ml)

    barrier = pltpu.get_barrier_semaphore()
    with scope("barrier"):
        peers = [sib, right, left, m_next, m_prev] + z_peers
        for p in peers:
            pl.semaphore_signal(barrier, inc=1, device_id=(p,), device_id_type=MESH)
        pl.semaphore_wait(barrier, len(peers))
        load_x.wait()

    FAR_FIRST = (4, 3, 5, 2, 6, 1, 7)
    near = z // 4
    for d in FAR_FIRST:
        same = lax.rem(z + d, NZ) // 4 == near
        rcopy(own, own, a_sem.at[0], a_sem.at[jnp.where(same, 1, 2)], z_peers[d - 1]).start()

    OFF = (0, 1, 3, 2)

    def col(lc, j, h):
        return xs.at[column(lc, lax.rem(ml + OFF[j], 4)), pl.ds(4 * (near if h == 0 else 1 - near), 4)]

    def to_right(lc, j, h, far=0):
        return rcopy(col(lc, j, h), col(lc, j, h), r_send.at[0], r_recv.at[far * 8 + j * 2 + h], right)

    def to_left(lc, j, h, far=0):
        return rcopy(col(lc, j, h), col(lc, j, h), l_send.at[0], l_recv.at[far * 4 + j * 2 + h], left)

    def to_mid(j, h, e, p):
        return rcopy(col(ll, j, h), col(ll, j, h), y_send.at[0], y_recv.at[e], p)

    lp, lm, lf = lax.rem(ll + 1, 4), lax.rem(ll + 3, 4), lax.rem(ll + 2, 4)

    def round_ring(j, h):
        to_right(ll, j, h).start()
        to_left(ll, j, h).start()

    for h in range(2):
        with scope("first"):
            got = xs.at[0, 0:3 + h]
            rcopy(got, got, a_sem.at[0], a_sem.at[1 + h], sib).wait_recv()
        to_mid(0, h, h, m_prev).start()
        to_mid(0, h, 2 + h, m_next).start()
        round_ring(0, h)

    with scope("second"):
        to_mid(1, 0, 0, sib).wait_recv()
    to_mid(1, 0, 4, m_prev).start()
    round_ring(1, 0)
    with scope("second"):
        to_mid(2, 0, 2, sib).wait_recv()
    round_ring(2, 0)
    with scope("second"):
        to_mid(2, 1, 3, sib).wait_recv()
    to_mid(2, 1, 5, m_next).start()
    with scope("second"):
        to_mid(1, 1, 1, sib).wait_recv()
    round_ring(1, 1)
    round_ring(2, 1)

    def far_column():
        for h in range(2):
            with scope("third"):
                to_mid(3, h, 4 + h, sib).wait_recv()
            round_ring(3, h)

    def event(j):
        for h in range(2):
            to_right(lm, j, h).wait_recv()
            if j < 2:
                to_right(lm, j, h, 1).start()
            to_left(lp, j, h).wait_recv()
            if j >= 2:
                to_left(lp, j, h, 1).start()

    UNITS = (((0, 0), (0, 1)), ((3, 0), (1, 0)), ((0, 3), (0, 2)), ((3, 1), (1, 1)),
             ((3, 3), (1, 3)), ((3, 2), (1, 2)), ((2, 0), (2, 1)), ((2, 3), (2, 2)))

    def unit_of(lc, mc, u):
        return [(lax.rem(lc + a, 4), lax.rem(mc + b, 4)) for a, b in UNITS[u]]

    load_w.wait()
    load_g.wait()
    load_t.wait()
    k2 = jnp.minimum(jnp.exp(jnp.full((1, 1), tv[0], F32)) * LOG2E, F32_MAX)
    place = lax.broadcasted_iota(jnp.int32, (1, 512), 1) + me * 512
    pos = place.astype(F32) / (256 * 512.0)

    def project(u):
        rows = jnp.concatenate([xs[column(lc, mc)].reshape(128, 512) for lc, mc in unit_of(ll, ml, u)], axis=0)
        proj = jnp.dot(rows, wv[...], preferred_element_type=F32)
        inv = 1.0 / jnp.sqrt(jnp.sum(proj * proj, axis=1, keepdims=True))
        qown[u] = (proj * inv).astype(BF16)

    def to_sib(u):
        return rcopy(qown.at[u], qsib.at[u], q_send.at[0], q_recv.at[u], sib)

    def dots(buf, qs):
        q = qs[0] if len(qs) == 1 else jnp.concatenate(qs, axis=0)
        buf[0:256 * len(qs)] = lax.dot_general(q, gv[...], (((1,), (1,)), ((), ())), preferred_element_type=F32)

    def soften(buf, groups):
        n = 128 * len(groups)
        lane = lax.broadcasted_iota(jnp.int32, (n, 128), 1)
        d = buf[0:n]
        dm = jnp.max(d, axis=1, keepdims=True)
        ev = jnp.exp2((d - dm) * k2)
        zs = jnp.sum(ev, axis=1, keepdims=True)
        rs = jnp.sum(ev * pos, axis=1, keepdims=True)
        cols = jnp.where(lane == 0, dm, jnp.where(lane == 1, zs, rs))
        for i, gq in enumerate(groups):
            rows = slice(i * 128, i * 128 + 128)
            e_ref[gq] = ev[rows]
            stat[gq] = cols[rows].T[:4]

    def groups_own(u):
        return [jnp.where(core0, mc * 8 + lc * 2, lc * 8 + mc * 2 + 1) for lc, mc in unit_of(ll, ml, u)]

    def groups_sib(u):
        return [jnp.where(core0, lc * 8 + mc * 2 + 1, mc * 8 + lc * 2) for lc, mc in unit_of(ml, ll, u)]

    def groups_both(uo, us):
        return groups_own(uo) + groups_sib(us)

    def antipode(p):
        return lax.rem(p // 8 + 2, 4) * 8 + lax.rem(lax.rem(p, 8) + 4, 8)

    gm = antipode(pi)

    def send_group(gq):
        @pl.when(gq != gm)
        def _():
            rcopy(stat.at[gq], part.at[pi], s_send.at[0], s_recv.at[0], z * 32 + antipode(gq)).start()

        @pl.when(gq == gm)
        def _():
            part[pi] = stat[gm]

    def send_own(u):
        for gq in groups_own(u):
            send_group(gq)

    def send_sib(u):
        for gq in groups_sib(u):
            send_group(gq)

    project(0)
    to_sib(0).start()
    with scope("event0"):
        event(0)
    project(1)
    dots(da, [qown[0]])
    to_sib(1).start()
    far_column()

    def step(k, now, before):
        with scope("events"):
            if 3 <= k <= 5:
                event(k - 2)
            for h in range(2):
                if k == 6:
                    to_right(lf, 0, h, 1).wait_recv()
                    to_right(lf, 1, h, 1).wait_recv()
                if k == 7:
                    to_left(lf, 2, h, 1).wait_recv()
                    to_left(lf, 3, h, 1).wait_recv()

        with scope("sibwait"):
            to_sib(k - 2).wait_recv()
        if k == 7:
            with scope("project"):
                project(k)
            to_sib(k).start()
        with scope("compute"):
            soften(before, groups_own(0) if k == 2 else groups_both(k - 2, k - 3))
            if k < 7:
                project(k)
            dots(now, [qown[k - 1], qsib[k - 2]])
        if k < 7:
            to_sib(k).start()

    for k in range(2, 8):
        step(k, db if k % 2 == 0 else da, da if k % 2 == 0 else db)
        if k >= 6:
            for u in range(0 if k == 6 else 4, k - 2):
                send_own(u)
            for u in (2,) if k == 6 else (0, 1, 3):
                send_sib(u)
    send_own(5)
    send_sib(4)
    with scope("tail6"):
        to_sib(6).wait_recv()
        soften(da, groups_both(6, 5))
        dots(db, [qown[7], qsib[6]])
    send_own(6)
    send_sib(5)
    with scope("tail7"):
        to_sib(7).wait_recv()
        soften(db, groups_both(7, 6))
        dots(da, [qsib[7]])
    send_own(7)
    send_sib(6)
    with scope("tail8"):
        soften(da, groups_sib(7))
    send_sib(7)

    with scope("s1wait"):
        rcopy(part.at[0:31], part.at[0:31], s_send.at[0], s_recv.at[0], sib).wait_recv()

    def merge(ref):
        ms = ref[:, 0, :]
        m = jnp.max(ms, axis=0, keepdims=True)
        wgt = jnp.exp2((ms - m) * k2)
        return m, jnp.sum(wgt * ref[:, 1, :], axis=0, keepdims=True), jnp.sum(wgt * ref[:, 2, :], axis=0, keepdims=True)

    sub = lax.broadcasted_iota(jnp.int32, (4, 128), 0)

    def tile(a, b, d):
        return jnp.where(sub == 0, a, jnp.where(sub == 1, b, d))

    zpart[z] = tile(*merge(part))
    for d in FAR_FIRST:
        rcopy(zpart.at[z], zpart.at[z], s_send.at[1], s_recv.at[1], z_peers[d - 1]).start()
    with scope("s2wait"):
        rcopy(zpart.at[0:7], zpart.at[0:7], s_send.at[1], s_recv.at[1], sib).wait_recv()
    m, zs, rs = merge(zpart)
    done[gm] = tile(m, 1.0 / zs, rs / zs)

    peers = [(dy, dx, dc) for dy in range(4) for dx in range(4) for dc in range(2)][1:]
    peers.sort(key=lambda p: -min(p[0], 4 - p[0]) - min(p[1], 4 - p[1]))
    with scope("s3send"):
        for dy, dx, dc in peers:
            p = dev(z, lax.rem(y + dy, NY), lax.rem(x + dx, NX), lax.rem(c + dc, NC))
            rcopy(done.at[gm], done.at[gm], s_send.at[2], s_recv.at[2], p).start()

    with scope("s3wait"):
        rcopy(done.at[0:31], done.at[0:31], s_send.at[2], s_recv.at[2], sib).wait_recv()
    fac_ref[...] = jnp.exp2((stat[:, 0, :] - done[:, 0, :]) * k2) * done[:, 1, :]
    rank_ref[...] = done[:, 2, :]

    def sent(ref, sem):
        rcopy(ref, ref, sem, sem, sib).wait_send()

    with scope("drain"):
        sent(xs.at[0, 0:7], a_sem.at[0])
        sent(xs.at[0:3], y_send.at[0])
        sent(xs.at[0:6], r_send.at[0])
        sent(xs.at[0:6], l_send.at[0])
        sent(qown, q_send.at[0])
        sent(part.at[0:31], s_send.at[0])
        sent(zpart.at[0:7], s_send.at[1])
        sent(done.at[0:31], s_send.at[2])


def normalise_kernel(e_ref, fac_ref, rank_ref, p_hbm, r_hbm, buf, nat_ref, sem):
    def out(i):
        return pltpu.make_async_copy(buf.at[:, pl.ds(4 * i, 4)], p_hbm.at[:, pl.ds(4 * i, 4)], sem.at[i])

    def body(i, carry):
        for j in range(4):
            gq = i * 4 + j
            f = jnp.broadcast_to(fac_ref[pl.ds(gq, 1), :], (128, 128)).T
            ev = e_ref[gq]
            p = jnp.concatenate([ev[:, b * 128:(b + 1) * 128] * f for b in range(4)], axis=1)
            buf[:, gq] = p.astype(BF16).reshape(8, 16, 512)
        out(i).start()
        return carry

    lax.fori_loop(0, 8, body, 0)

    lane = lax.broadcasted_iota(jnp.int32, (8, 128), 1) // 16
    sub = lax.broadcasted_iota(jnp.int32, (8, 128), 0)
    for yy in range(NY):
        r = rank_ref[yy * 8:yy * 8 + 8]
        nat = r
        for d in range(1, 8):
            moved = pltpu.roll(pltpu.roll(r, 16 * d, 1), 8 - d, 0)
            nat = jnp.where(lax.rem(lane - sub + 8, 8) == d, moved, nat)
        nat_ref[pl.ds(yy, 8, stride=4), :] = nat
    out_rank = pltpu.make_async_copy(nat_ref, r_hbm, sem.at[8])
    out_rank.start()

    for i in range(8):
        out(i).wait()
    out_rank.wait()


def solution(mesh):
    D = pltpu.SemaphoreType.DMA
    VM = pltpu.VMEM

    def per_device(text_states, text_proj, gallery, logit_scale):
        e, fac, rank = pl.pallas_call(
            gather_score_kernel,
            out_shape=(VM((32, 128, 512), F32), VM((32, 128), F32), VM((32, 128), F32)),
            in_specs=[pl.BlockSpec(memory_space=pl.ANY)] * 4,
            out_specs=(pl.BlockSpec(memory_space=VM),) * 3,
            scratch_shapes=[
                VM((16, NZ, 16, 512), BF16), VM((512, 1024), BF16), VM((512, 1024), BF16),
                pltpu.SMEM((1,), F32), VM((8, 256, 1024), BF16), VM((8, 256, 1024), BF16), VM((512, 512), F32), VM((512, 512), F32),
                VM((32, 4, 128), F32), VM((32, 4, 128), F32), VM((NZ, 4, 128), F32), VM((32, 4, 128), F32),
                D((4,)), D((3,)), D((1,)), D((6,)), D((1,)), D((12,)), D((1,)), D((12,)),
                D((1,)), D((8,)), D((3,)), D((3,)),
            ],
            compiler_params=pltpu.CompilerParams(collective_id=0, has_side_effects=True,
                                                 vmem_limit_bytes=48 * 1024 * 1024),
        )(text_states, text_proj, gallery, logit_scale)
        prob, rank = pl.pallas_call(
            normalise_kernel,
            out_shape=(jax.ShapeDtypeStruct((NZ, 32, 16, 512), BF16), jax.ShapeDtypeStruct((32, 128), F32)),
            in_specs=[pl.BlockSpec(memory_space=VM)] * 3,
            out_specs=(pl.BlockSpec(memory_space=pl.ANY),) * 2,
            scratch_shapes=[VM((NZ, 32, 16, 512), BF16), VM((32, 128), F32), D((9,))],
            compiler_params=pltpu.CompilerParams(vmem_limit_bytes=24 * 1024 * 1024),
        )(e, fac, rank)
        return prob.reshape(4096, 512), rank.reshape(4096)

    return jax.shard_map(per_device, mesh=mesh,
                         in_specs=(P("ga", None), P(None, None), P("ga", None), P(None)),
                         out_specs=(P(None, "ga"), P(None)), check_vma=False)
```

```python
import jax
import jax.numpy as jnp
from jax import lax
from jax.experimental import pallas as pl
from jax.experimental.pallas import tpu as pltpu
from jax.sharding import PartitionSpec as P

MESH = pl.DeviceIdType.MESH
NX, NY, NZ, NC = 4, 4, 8, 2
F32, BF16 = jnp.float32, jnp.bfloat16
LOG2E = 1.4426950408889634
F32_MAX = 3.4028235e38
scope = jax.named_scope


def rcopy(src, dst, ss, rs, p):
    return pltpu.make_async_remote_copy(src_ref=src, dst_ref=dst, send_sem=ss, recv_sem=rs,
                                        device_id=(p,), device_id_type=MESH)


def gather_score_kernel(x_hbm, w_hbm, g_hbm, t_hbm,
                        e_ref, fac_ref, rank_ref,
                        xs, wv, gv, tv, qown, qsib, da, db, stat, part, zpart, done,
                        in_sem, a_sem, f_sem, y_send, y_recv, r_send, r_recv, l_send, l_recv,
                        q_send, q_recv, s_send, s_recv):
    me = lax.axis_index("ga")
    c = lax.rem(me, NC)
    x = lax.rem(me // 2, NX)
    y = lax.rem(me // 8, NY)
    z = me // 32
    pi = lax.rem(me, 32)
    core0 = c == 0
    ml = jnp.where(core0, y, x)
    ll = jnp.where(core0, x, y)

    def dev(zz, yy, xx, cc):
        return ((zz * NY + yy) * NX + xx) * NC + cc

    def dev_lm(zz, lc, mc):
        return dev(zz, jnp.where(core0, mc, lc), jnp.where(core0, lc, mc), c)

    def column(lc, mc):
        return lc * 4 + mc

    mine = column(ll, ml)
    own = xs.at[mine, z]
    load_x = pltpu.make_async_copy(x_hbm, own, in_sem.at[0])
    load_w = pltpu.make_async_copy(w_hbm, wv, in_sem.at[1])
    load_g = pltpu.make_async_copy(g_hbm, gv, in_sem.at[2])
    load_t = pltpu.make_async_copy(t_hbm, tv, in_sem.at[3])
    load_x.start()
    load_t.start()
    load_w.start()
    load_g.start()

    sib = dev(z, y, x, 1 - c)
    z_peers = [dev(lax.rem(z + d, NZ), y, x, c) for d in range(1, NZ)]
    m_next = dev_lm(z, ll, lax.rem(ml + 1, 4))
    m_prev = dev_lm(z, ll, lax.rem(ml + 3, 4))
    right = dev_lm(z, lax.rem(ll + 1, 4), ml)
    left = dev_lm(z, lax.rem(ll + 3, 4), ml)

    across = dev_lm(z, lax.rem(ll + 2, 4), ml)

    barrier = pltpu.get_barrier_semaphore()
    with scope("barrier"):
        peers = [sib, right, left, m_next, m_prev, across] + z_peers
        for p in peers:
            pl.semaphore_signal(barrier, inc=1, device_id=(p,), device_id_type=MESH)
        pl.semaphore_wait(barrier, len(peers))
        load_x.wait()

    FAR_FIRST = (4, 3, 5, 2, 6, 1, 7)
    near = z // 4
    for d in FAR_FIRST:
        same = lax.rem(z + d, NZ) // 4 == near
        rcopy(own, own, a_sem.at[0], a_sem.at[jnp.where(same, 1, 2)], z_peers[d - 1]).start()

    rcopy(own, own, f_sem.at[0], f_sem.at[1], across).start()

    OFF = (0, 1, 3, 2)

    def col(lc, j, h):
        return xs.at[column(lc, lax.rem(ml + OFF[j], 4)), pl.ds(4 * (near if h == 0 else 1 - near), 4)]

    def to_right(lc, j, h, far=0):
        return rcopy(col(lc, j, h), col(lc, j, h), r_send.at[0], r_recv.at[far * 8 + j * 2 + h], right)

    def to_left(lc, j, h, far=0):
        return rcopy(col(lc, j, h), col(lc, j, h), l_send.at[0], l_recv.at[far * 4 + j * 2 + h], left)

    def to_mid(j, h, e, p):
        return rcopy(col(ll, j, h), col(ll, j, h), y_send.at[0], y_recv.at[e], p)

    lp, lm, lf = lax.rem(ll + 1, 4), lax.rem(ll + 3, 4), lax.rem(ll + 2, 4)

    def round_ring(j, h):
        to_right(ll, j, h).start()
        to_left(ll, j, h).start()

    for h in range(2):
        with scope("first"):
            got = xs.at[0, 0:3 + h]
            rcopy(got, got, a_sem.at[0], a_sem.at[1 + h], sib).wait_recv()
        to_mid(0, h, h, m_prev).start()
        to_mid(0, h, 2 + h, m_next).start()
        round_ring(0, h)

    opposite = xs.at[column(lf, ml), z]
    rcopy(opposite, opposite, f_sem.at[0], f_sem.at[1], sib).wait_recv()
    for d in FAR_FIRST:
        rcopy(opposite, opposite, f_sem.at[0], f_sem.at[2], z_peers[d - 1]).start()

    def across_column():
        rcopy(xs.at[0, 0:7], xs.at[0, 0:7], f_sem.at[0], f_sem.at[2], sib).wait_recv()

    def mid_columns():
        with scope("second"):
            to_mid(1, 0, 0, sib).wait_recv()
        to_mid(1, 0, 4, m_prev).start()
        round_ring(1, 0)
        with scope("second"):
            to_mid(2, 0, 2, sib).wait_recv()
        round_ring(2, 0)
        with scope("second"):
            to_mid(2, 1, 3, sib).wait_recv()
        to_mid(2, 1, 5, m_next).start()
        with scope("second"):
            to_mid(1, 1, 1, sib).wait_recv()
        round_ring(1, 1)
        round_ring(2, 1)

    def far_column():
        for h in range(2):
            with scope("third"):
                to_mid(3, h, 4 + h, sib).wait_recv()
            round_ring(3, h)

    def from_left(j):
        for h in range(2):
            to_right(lm, j, h).wait_recv()
            if j == 1:
                to_right(lm, j, h, 1).start()

    def from_right(j):
        for h in range(2):
            to_left(lp, j, h).wait_recv()
            if j >= 2:
                to_left(lp, j, h, 1).start()

    def far_left(j):
        for h in range(2):
            to_right(lf, j, h, 1).wait_recv()

    def far_right(j):
        for h in range(2):
            to_left(lf, j, h, 1).wait_recv()

    UNITS = (((0, 0), (0, 1)), ((3, 0), (1, 0)), ((0, 3), (2, 0)), ((0, 2),), ((3, 1), (1, 1)),
             ((3, 3), (1, 3)), ((3, 2), (1, 2)), ((2, 1), (2, 3)), ((2, 2),))

    def unit_of(lc, mc, u):
        return [(lax.rem(lc + a, 4), lax.rem(mc + b, 4)) for a, b in UNITS[u]]

    def events(k):
        if k == 0:
            mid_columns()
        if k == 1:
            from_left(0)
            from_right(0)
        if k == 2:
            across_column()
        if k == 3:
            far_column()
        if 4 <= k <= 6:
            from_left(k - 3)
            from_right(k - 3)
        if k == 7:
            far_left(1)
            far_right(2)
        if k == 8:
            far_right(3)

    load_w.wait()
    load_g.wait()
    load_t.wait()
    k2 = jnp.minimum(jnp.exp(jnp.full((1, 1), tv[0], F32)) * LOG2E, F32_MAX)
    place = lax.broadcasted_iota(jnp.int32, (1, 512), 1) + me * 512
    pos = place.astype(F32) / (256 * 512.0)

    def q_of(ref, u):
        return ref.at[u, 0:128 * len(UNITS[u])]

    def project(u):
        rows = jnp.concatenate([xs[column(lc, mc)].reshape(128, 512) for lc, mc in unit_of(ll, ml, u)], axis=0)
        proj = jnp.dot(rows, wv[...], preferred_element_type=F32)
        inv = 1.0 / jnp.sqrt(jnp.sum(proj * proj, axis=1, keepdims=True))
        q_of(qown, u)[...] = (proj * inv).astype(BF16)

    def to_sib(u):
        return rcopy(q_of(qown, u), q_of(qsib, u), q_send.at[0], q_recv.at[u], sib)

    def dots(buf, uo, us):
        q = jnp.concatenate([q_of(qown, u)[...] for u in uo] + [q_of(qsib, u)[...] for u in us], axis=0)
        buf[0:q.shape[0]] = lax.dot_general(q, gv[...], (((1,), (1,)), ((), ())), preferred_element_type=F32)

    def soften(buf, groups):
        n = 128 * len(groups)
        lane = lax.broadcasted_iota(jnp.int32, (n, 128), 1)
        d = buf[0:n]
        dm = jnp.max(d, axis=1, keepdims=True)
        ev = jnp.exp2((d - dm) * k2)
        zs = jnp.sum(ev, axis=1, keepdims=True)
        rs = jnp.sum(ev * pos, axis=1, keepdims=True)
        cols = jnp.where(lane == 0, dm, jnp.where(lane == 1, zs, rs))
        for i, gq in enumerate(groups):
            rows = slice(i * 128, i * 128 + 128)
            e_ref[gq] = ev[rows]
            stat[gq] = cols[rows].T[:4]

    def groups_own(u):
        return [jnp.where(core0, mc * 8 + lc * 2, lc * 8 + mc * 2 + 1) for lc, mc in unit_of(ll, ml, u)]

    def groups_sib(u):
        return [jnp.where(core0, lc * 8 + mc * 2 + 1, mc * 8 + lc * 2) for lc, mc in unit_of(ml, ll, u)]

    def groups_of(uo, us):
        return sum([groups_own(u) for u in uo] + [groups_sib(u) for u in us], [])

    def antipode(p):
        return lax.rem(p // 8 + 2, 4) * 8 + lax.rem(lax.rem(p, 8) + 4, 8)

    gm = antipode(pi)

    def send_group(gq):
        @pl.when(gq != gm)
        def _():
            rcopy(stat.at[gq], part.at[pi], s_send.at[0], s_recv.at[0], z * 32 + antipode(gq)).start()

        @pl.when(gq == gm)
        def _():
            part[pi] = stat[gm]

    LAST = 8

    def scored(k):
        return [u for u in (k - 1,) if 0 <= u <= LAST], [u for u in (k - 2,) if 0 <= u <= LAST]

    def step(k):
        now, before = (da, db) if k % 2 else (db, da)
        with scope("events"):
            events(k)
        uo, us = scored(k)
        with scope("sibwait"):
            for u in us:
                to_sib(u).wait_recv()
        if k == LAST:
            with scope("project"):
                project(k)
            to_sib(k).start()
        with scope("compute"):
            if k >= 2:
                soften(before, groups_of(*scored(k - 1)))
            if k < LAST:
                project(k)
            if uo or us:
                dots(now, uo, us)
        if k < LAST:
            to_sib(k).start()

    SENDS = {6: ((0, 1, 2, 3), (2,)), 7: ((4,), (1, 3)), 8: ((5, 6), (0, 4, 5)), 9: ((7,), (6,)), 10: ((8,), (7,)),
             11: ((), (8,))}

    def sends(k):
        for u in SENDS[k][0]:
            for gq in groups_own(u):
                send_group(gq)
        for u in SENDS[k][1]:
            for gq in groups_sib(u):
                send_group(gq)

    for k in range(LAST + 1):
        step(k)
        if k in SENDS:
            sends(k)
    with scope("tail6"):
        to_sib(LAST - 1).wait_recv()
        soften(db, groups_of(*scored(LAST)))
        dots(da, *scored(LAST + 1))
    sends(LAST + 1)
    with scope("tail7"):
        to_sib(LAST).wait_recv()
        soften(da, groups_of(*scored(LAST + 1)))
        dots(db, *scored(LAST + 2))
    sends(LAST + 2)
    with scope("tail8"):
        soften(db, groups_of(*scored(LAST + 2)))
    sends(LAST + 3)

    with scope("s1wait"):
        rcopy(part.at[0:31], part.at[0:31], s_send.at[0], s_recv.at[0], sib).wait_recv()

    def merge(ref):
        ms = ref[:, 0, :]
        m = jnp.max(ms, axis=0, keepdims=True)
        wgt = jnp.exp2((ms - m) * k2)
        return m, jnp.sum(wgt * ref[:, 1, :], axis=0, keepdims=True), jnp.sum(wgt * ref[:, 2, :], axis=0, keepdims=True)

    sub = lax.broadcasted_iota(jnp.int32, (4, 128), 0)

    def tile(a, b, d):
        return jnp.where(sub == 0, a, jnp.where(sub == 1, b, d))

    zpart[z] = tile(*merge(part))
    for d in FAR_FIRST:
        rcopy(zpart.at[z], zpart.at[z], s_send.at[1], s_recv.at[1], z_peers[d - 1]).start()
    with scope("s2wait"):
        rcopy(zpart.at[0:7], zpart.at[0:7], s_send.at[1], s_recv.at[1], sib).wait_recv()
    m, zs, rs = merge(zpart)
    done[gm] = tile(m, 1.0 / zs, rs / zs)

    peers = [(dy, dx, dc) for dy in range(4) for dx in range(4) for dc in range(2)][1:]
    peers.sort(key=lambda p: -min(p[0], 4 - p[0]) - min(p[1], 4 - p[1]))
    with scope("s3send"):
        for dy, dx, dc in peers:
            p = dev(z, lax.rem(y + dy, NY), lax.rem(x + dx, NX), lax.rem(c + dc, NC))
            rcopy(done.at[gm], done.at[gm], s_send.at[2], s_recv.at[2], p).start()

    with scope("s3wait"):
        rcopy(done.at[0:31], done.at[0:31], s_send.at[2], s_recv.at[2], sib).wait_recv()
    fac_ref[...] = jnp.exp2((stat[:, 0, :] - done[:, 0, :]) * k2) * done[:, 1, :]
    rank_ref[...] = done[:, 2, :]

    def sent(ref, sem):
        rcopy(ref, ref, sem, sem, sib).wait_send()

    with scope("drain"):
        sent(xs.at[0, 0:7], a_sem.at[0])
        sent(xs.at[0:3], y_send.at[0])
        sent(xs.at[0], f_sem.at[0])
        sent(xs.at[0:5], r_send.at[0])
        sent(xs.at[0:6], l_send.at[0])
        sent(qown.at[0:8], q_send.at[0])
        sent(part.at[0:31], s_send.at[0])
        sent(zpart.at[0:7], s_send.at[1])
        sent(done.at[0:31], s_send.at[2])


def normalise_kernel(e_ref, fac_ref, rank_ref, p_hbm, r_hbm, buf, nat_ref, sem):
    def out(i):
        return pltpu.make_async_copy(buf.at[:, pl.ds(4 * i, 4)], p_hbm.at[:, pl.ds(4 * i, 4)], sem.at[i])

    def body(i, carry):
        for j in range(4):
            gq = i * 4 + j
            f = jnp.broadcast_to(fac_ref[pl.ds(gq, 1), :], (128, 128)).T
            ev = e_ref[gq]
            p = jnp.concatenate([ev[:, b * 128:(b + 1) * 128] * f for b in range(4)], axis=1)
            buf[:, gq] = p.astype(BF16).reshape(8, 16, 512)
        out(i).start()
        return carry

    lax.fori_loop(0, 8, body, 0)

    lane = lax.broadcasted_iota(jnp.int32, (8, 128), 1) // 16
    sub = lax.broadcasted_iota(jnp.int32, (8, 128), 0)
    for yy in range(NY):
        r = rank_ref[yy * 8:yy * 8 + 8]
        nat = r
        for d in range(1, 8):
            moved = pltpu.roll(pltpu.roll(r, 16 * d, 1), 8 - d, 0)
            nat = jnp.where(lax.rem(lane - sub + 8, 8) == d, moved, nat)
        nat_ref[pl.ds(yy, 8, stride=4), :] = nat
    out_rank = pltpu.make_async_copy(nat_ref, r_hbm, sem.at[8])
    out_rank.start()

    for i in range(8):
        out(i).wait()
    out_rank.wait()


def solution(mesh):
    D = pltpu.SemaphoreType.DMA
    VM = pltpu.VMEM

    def per_device(text_states, text_proj, gallery, logit_scale):
        e, fac, rank = pl.pallas_call(
            gather_score_kernel,
            out_shape=(VM((32, 128, 512), F32), VM((32, 128), F32), VM((32, 128), F32)),
            in_specs=[pl.BlockSpec(memory_space=pl.ANY)] * 4,
            out_specs=(pl.BlockSpec(memory_space=VM),) * 3,
            scratch_shapes=[
                VM((16, NZ, 16, 512), BF16), VM((512, 1024), BF16), VM((512, 1024), BF16),
                pltpu.SMEM((1,), F32), VM((9, 256, 1024), BF16), VM((9, 256, 1024), BF16), VM((512, 512), F32), VM((512, 512), F32),
                VM((32, 4, 128), F32), VM((32, 4, 128), F32), VM((NZ, 4, 128), F32), VM((32, 4, 128), F32),
                D((4,)), D((3,)), D((3,)), D((1,)), D((6,)), D((1,)), D((12,)), D((1,)), D((12,)),
                D((1,)), D((9,)), D((3,)), D((3,)),
            ],
            compiler_params=pltpu.CompilerParams(collective_id=0, has_side_effects=True,
                                                 vmem_limit_bytes=48 * 1024 * 1024),
        )(text_states, text_proj, gallery, logit_scale)
        prob, rank = pl.pallas_call(
            normalise_kernel,
            out_shape=(jax.ShapeDtypeStruct((NZ, 32, 16, 512), BF16), jax.ShapeDtypeStruct((32, 128), F32)),
            in_specs=[pl.BlockSpec(memory_space=VM)] * 3,
            out_specs=(pl.BlockSpec(memory_space=pl.ANY),) * 2,
            scratch_shapes=[VM((NZ, 32, 16, 512), BF16), VM((32, 128), F32), D((9,))],
            compiler_params=pltpu.CompilerParams(vmem_limit_bytes=24 * 1024 * 1024),
        )(e, fac, rank)
        return prob.reshape(4096, 512), rank.reshape(4096)

    return jax.shard_map(per_device, mesh=mesh,
                         in_specs=(P("ga", None), P(None, None), P("ga", None), P(None)),
                         out_specs=(P(None, "ga"), P(None)), check_vma=False)
```

```python
import jax
import jax.numpy as jnp
from jax import lax
from jax.experimental import pallas as pl
from jax.experimental.pallas import tpu as pltpu
from jax.sharding import PartitionSpec as P

MESH = pl.DeviceIdType.MESH
NX, NY, NZ, NC = 4, 4, 8, 2
F32, BF16 = jnp.float32, jnp.bfloat16
LOG2E = 1.4426950408889634
F32_MAX = 3.4028235e38
scope = jax.named_scope


def rcopy(src, dst, ss, rs, p):
    return pltpu.make_async_remote_copy(src_ref=src, dst_ref=dst, send_sem=ss, recv_sem=rs,
                                        device_id=(p,), device_id_type=MESH)


def gather_score_kernel(x_hbm, w_hbm, g_hbm, t_hbm,
                        e_ref, fac_ref, rank_ref,
                        xs, wv, gv, tv, qown, qsib, da, db, stat, part, zpart, done,
                        in_sem, a_sem, f_sem, y_send, y_recv, r_send, r_recv, l_send, l_recv,
                        q_send, q_recv, s_send, s_recv):
    me = lax.axis_index("ga")
    c = lax.rem(me, NC)
    x = lax.rem(me // 2, NX)
    y = lax.rem(me // 8, NY)
    z = me // 32
    pi = lax.rem(me, 32)
    core0 = c == 0
    ml = jnp.where(core0, y, x)
    ll = jnp.where(core0, x, y)

    def dev(zz, yy, xx, cc):
        return ((zz * NY + yy) * NX + xx) * NC + cc

    def dev_lm(zz, lc, mc):
        return dev(zz, jnp.where(core0, mc, lc), jnp.where(core0, lc, mc), c)

    def column(lc, mc):
        return lc * 4 + mc

    mine = column(ll, ml)
    own = xs.at[mine, z]
    load_x = pltpu.make_async_copy(x_hbm, own, in_sem.at[0])
    load_w = pltpu.make_async_copy(w_hbm, wv, in_sem.at[1])
    load_g = pltpu.make_async_copy(g_hbm, gv, in_sem.at[2])
    load_t = pltpu.make_async_copy(t_hbm, tv, in_sem.at[3])
    load_x.start()
    load_t.start()
    load_w.start()
    load_g.start()

    sib = dev(z, y, x, 1 - c)
    z_peers = [dev(lax.rem(z + d, NZ), y, x, c) for d in range(1, NZ)]
    m_next = dev_lm(z, ll, lax.rem(ml + 1, 4))
    m_prev = dev_lm(z, ll, lax.rem(ml + 3, 4))
    right = dev_lm(z, lax.rem(ll + 1, 4), ml)
    left = dev_lm(z, lax.rem(ll + 3, 4), ml)

    across = dev_lm(z, lax.rem(ll + 2, 4), ml)

    barrier = pltpu.get_barrier_semaphore()
    with scope("barrier"):
        peers = [sib, right, left, m_next, m_prev, across] + z_peers
        for p in peers:
            pl.semaphore_signal(barrier, inc=1, device_id=(p,), device_id_type=MESH)
        pl.semaphore_wait(barrier, len(peers))
        load_x.wait()

    FAR_FIRST = (4, 3, 5, 2, 6, 1, 7)
    near = z // 4
    for d in FAR_FIRST:
        same = lax.rem(z + d, NZ) // 4 == near
        rcopy(own, own, a_sem.at[0], a_sem.at[jnp.where(same, 1, 2)], z_peers[d - 1]).start()

    rcopy(own, own, f_sem.at[0], f_sem.at[1], across).start()

    OFF = (0, 1, 3, 2)

    def col(lc, j, h):
        return xs.at[column(lc, lax.rem(ml + OFF[j], 4)), pl.ds(4 * (near if h == 0 else 1 - near), 4)]

    def to_right(lc, j, h, far=0):
        return rcopy(col(lc, j, h), col(lc, j, h), r_send.at[0], r_recv.at[far * 8 + j * 2 + h], right)

    def to_left(lc, j, h, far=0):
        return rcopy(col(lc, j, h), col(lc, j, h), l_send.at[0], l_recv.at[far * 4 + j * 2 + h], left)

    def to_mid(j, h, e, p):
        return rcopy(col(ll, j, h), col(ll, j, h), y_send.at[0], y_recv.at[e], p)

    lp, lm, lf = lax.rem(ll + 1, 4), lax.rem(ll + 3, 4), lax.rem(ll + 2, 4)

    def round_ring(j, h):
        to_right(ll, j, h).start()
        to_left(ll, j, h).start()

    for h in range(2):
        with scope("first"):
            got = xs.at[0, 0:3 + h]
            rcopy(got, got, a_sem.at[0], a_sem.at[1 + h], sib).wait_recv()
        to_mid(0, h, h, m_prev).start()
        to_mid(0, h, 2 + h, m_next).start()
        round_ring(0, h)

    opposite = xs.at[column(lf, ml), z]
    rcopy(opposite, opposite, f_sem.at[0], f_sem.at[1], sib).wait_recv()
    for d in FAR_FIRST:
        rcopy(opposite, opposite, f_sem.at[0], f_sem.at[2], z_peers[d - 1]).start()

    def across_column():
        rcopy(xs.at[0, 0:7], xs.at[0, 0:7], f_sem.at[0], f_sem.at[2], sib).wait_recv()

    def mid_columns():
        with scope("second"):
            to_mid(1, 0, 0, sib).wait_recv()
        to_mid(1, 0, 4, m_prev).start()
        round_ring(1, 0)
        with scope("second"):
            to_mid(2, 0, 2, sib).wait_recv()
        round_ring(2, 0)
        with scope("second"):
            to_mid(2, 1, 3, sib).wait_recv()
        to_mid(2, 1, 5, m_next).start()
        with scope("second"):
            to_mid(1, 1, 1, sib).wait_recv()
        round_ring(1, 1)
        round_ring(2, 1)

    def far_column():
        for h in range(2):
            with scope("third"):
                to_mid(3, h, 4 + h, sib).wait_recv()
            round_ring(3, h)

    def from_left(j):
        for h in range(2):
            to_right(lm, j, h).wait_recv()
            if j == 1:
                to_right(lm, j, h, 1).start()

    def from_right(j):
        for h in range(2):
            to_left(lp, j, h).wait_recv()
            if j >= 2:
                to_left(lp, j, h, 1).start()

    def far_left(j):
        for h in range(2):
            to_right(lf, j, h, 1).wait_recv()

    def far_right(j):
        for h in range(2):
            to_left(lf, j, h, 1).wait_recv()

    UNITS = (((0, 0), (0, 1)), ((3, 0), (1, 0)), ((0, 3), (2, 0)), ((0, 2),), ((3, 1), (1, 1)),
             ((3, 3), (1, 3)), ((3, 2), (1, 2)), ((2, 1), (2, 3)), ((2, 2),))

    def unit_of(lc, mc, u):
        return [(lax.rem(lc + a, 4), lax.rem(mc + b, 4)) for a, b in UNITS[u]]

    def events(k):
        if k == 0:
            mid_columns()
        if k == 1:
            from_left(0)
            from_right(0)
        if k == 2:
            across_column()
        if k == 3:
            far_column()
        if 4 <= k <= 6:
            from_left(k - 3)
            from_right(k - 3)
        if k == 7:
            far_left(1)
            far_right(2)
        if k == 8:
            far_right(3)

    load_w.wait()
    load_g.wait()
    load_t.wait()
    k2 = jnp.minimum(jnp.exp(jnp.full((1, 1), tv[0], F32)) * LOG2E, F32_MAX)
    place = lax.broadcasted_iota(jnp.int32, (1, 512), 1) + me * 512
    pos = place.astype(F32) / (256 * 512.0)

    def q_of(ref, u):
        return ref.at[u, 0:128 * len(UNITS[u])]

    def project(u):
        rows = jnp.concatenate([xs[column(lc, mc)].reshape(128, 512) for lc, mc in unit_of(ll, ml, u)], axis=0)
        proj = jnp.dot(rows, wv[...], preferred_element_type=F32)
        inv = 1.0 / jnp.sqrt(jnp.sum(proj * proj, axis=1, keepdims=True))
        q_of(qown, u)[...] = (proj * inv).astype(BF16)

    def to_sib(u):
        return rcopy(q_of(qown, u), q_of(qsib, u), q_send.at[0], q_recv.at[u], sib)

    def dots(buf, uo, us):
        q = jnp.concatenate([q_of(qown, u)[...] for u in uo] + [q_of(qsib, u)[...] for u in us], axis=0)
        buf[0:q.shape[0]] = lax.dot_general(q, gv[...], (((1,), (1,)), ((), ())), preferred_element_type=F32)

    def soften(buf, groups):
        n = 128 * len(groups)
        lane = lax.broadcasted_iota(jnp.int32, (n, 128), 1)
        d = buf[0:n]
        dm = jnp.max(d, axis=1, keepdims=True)
        ev = jnp.exp2((d - dm) * k2)
        zs = jnp.sum(ev, axis=1, keepdims=True)
        rs = jnp.sum(ev * pos, axis=1, keepdims=True)
        cols = jnp.where(lane == 0, dm, jnp.where(lane == 1, zs, rs))
        for i, gq in enumerate(groups):
            rows = slice(i * 128, i * 128 + 128)
            e_ref[gq] = ev[rows]
            stat[gq] = cols[rows].T[:4]

    def groups_own(u):
        return [jnp.where(core0, mc * 8 + lc * 2, lc * 8 + mc * 2 + 1) for lc, mc in unit_of(ll, ml, u)]

    def groups_sib(u):
        return [jnp.where(core0, lc * 8 + mc * 2 + 1, mc * 8 + lc * 2) for lc, mc in unit_of(ml, ll, u)]

    def groups_of(uo, us):
        return sum([groups_own(u) for u in uo] + [groups_sib(u) for u in us], [])

    def antipode(p):
        return lax.rem(p // 8 + 2, 4) * 8 + lax.rem(lax.rem(p, 8) + 4, 8)

    gm = antipode(pi)

    def send_group(gq):
        @pl.when(gq != gm)
        def _():
            rcopy(stat.at[gq], part.at[pi], s_send.at[0], s_recv.at[0], z * 32 + antipode(gq)).start()

        @pl.when(gq == gm)
        def _():
            part[pi] = stat[gm]

    LAST = 8

    def scored(k):
        return [u for u in (k - 1,) if 0 <= u <= LAST], [u for u in (k - 2,) if 0 <= u <= LAST]

    def step(k):
        now, before = (da, db) if k % 2 else (db, da)
        with scope("events"):
            events(k)
        uo, us = scored(k)
        with scope("sibwait"):
            for u in us:
                to_sib(u).wait_recv()
        if k >= LAST - 1:
            with scope("project"):
                project(k)
            to_sib(k).start()
        with scope("compute"):
            if k >= 2:
                soften(before, groups_of(*scored(k - 1)))
            if k < LAST - 1:
                project(k)
            if uo or us:
                dots(now, uo, us)
        if k < LAST - 1:
            to_sib(k).start()

    SENDS = {6: ((0, 1, 2, 3), (2,)), 7: ((4,), (1, 3)), 8: ((5, 6), (0, 4, 5)), 9: ((7,), (6,)), 10: ((8,), (7,)),
             11: ((), (8,))}

    def sends(k):
        for u in SENDS[k][0]:
            for gq in groups_own(u):
                send_group(gq)
        for u in SENDS[k][1]:
            for gq in groups_sib(u):
                send_group(gq)

    for k in range(LAST + 1):
        step(k)
        if k in SENDS:
            sends(k)
    with scope("tail6"):
        to_sib(LAST - 1).wait_recv()
        soften(db, groups_of(*scored(LAST)))
        dots(da, *scored(LAST + 1))
    sends(LAST + 1)
    with scope("tail7"):
        to_sib(LAST).wait_recv()
        soften(da, groups_of(*scored(LAST + 1)))
        dots(db, *scored(LAST + 2))
    sends(LAST + 2)
    with scope("tail8"):
        soften(db, groups_of(*scored(LAST + 2)))
    sends(LAST + 3)

    with scope("s1wait"):
        rcopy(part.at[0:31], part.at[0:31], s_send.at[0], s_recv.at[0], sib).wait_recv()

    def merge(ref):
        ms = ref[:, 0, :]
        m = jnp.max(ms, axis=0, keepdims=True)
        wgt = jnp.exp2((ms - m) * k2)
        return m, jnp.sum(wgt * ref[:, 1, :], axis=0, keepdims=True), jnp.sum(wgt * ref[:, 2, :], axis=0, keepdims=True)

    sub = lax.broadcasted_iota(jnp.int32, (4, 128), 0)

    def tile(a, b, d):
        return jnp.where(sub == 0, a, jnp.where(sub == 1, b, d))

    zpart[z] = tile(*merge(part))
    for d in FAR_FIRST:
        rcopy(zpart.at[z], zpart.at[z], s_send.at[1], s_recv.at[1], z_peers[d - 1]).start()
    with scope("s2wait"):
        rcopy(zpart.at[0:7], zpart.at[0:7], s_send.at[1], s_recv.at[1], sib).wait_recv()
    m, zs, rs = merge(zpart)
    done[gm] = tile(m, 1.0 / zs, rs / zs)

    peers = [(dy, dx, dc) for dy in range(4) for dx in range(4) for dc in range(2)][1:]
    peers.sort(key=lambda p: -min(p[0], 4 - p[0]) - min(p[1], 4 - p[1]))
    with scope("s3send"):
        for dy, dx, dc in peers:
            p = dev(z, lax.rem(y + dy, NY), lax.rem(x + dx, NX), lax.rem(c + dc, NC))
            rcopy(done.at[gm], done.at[gm], s_send.at[2], s_recv.at[2], p).start()

    with scope("s3wait"):
        rcopy(done.at[0:31], done.at[0:31], s_send.at[2], s_recv.at[2], sib).wait_recv()
    fac_ref[...] = jnp.exp2((stat[:, 0, :] - done[:, 0, :]) * k2) * done[:, 1, :]
    rank_ref[...] = done[:, 2, :]

    def sent(ref, sem):
        rcopy(ref, ref, sem, sem, sib).wait_send()

    with scope("drain"):
        sent(xs.at[0, 0:7], a_sem.at[0])
        sent(xs.at[0:3], y_send.at[0])
        sent(xs.at[0], f_sem.at[0])
        sent(xs.at[0:5], r_send.at[0])
        sent(xs.at[0:6], l_send.at[0])
        sent(qown.at[0:8], q_send.at[0])
        sent(part.at[0:31], s_send.at[0])
        sent(zpart.at[0:7], s_send.at[1])
        sent(done.at[0:31], s_send.at[2])


def normalise_kernel(e_ref, fac_ref, rank_ref, p_hbm, r_hbm, buf, nat_ref, sem):
    def out(i):
        return pltpu.make_async_copy(buf.at[:, pl.ds(4 * i, 4)], p_hbm.at[:, pl.ds(4 * i, 4)], sem.at[i])

    def body(i, carry):
        for j in range(4):
            gq = i * 4 + j
            f = jnp.broadcast_to(fac_ref[pl.ds(gq, 1), :], (128, 128)).T
            ev = e_ref[gq]
            p = jnp.concatenate([ev[:, b * 128:(b + 1) * 128] * f for b in range(4)], axis=1)
            buf[:, gq] = p.astype(BF16).reshape(8, 16, 512)
        out(i).start()
        return carry

    lax.fori_loop(0, 8, body, 0)

    lane = lax.broadcasted_iota(jnp.int32, (8, 128), 1) // 16
    sub = lax.broadcasted_iota(jnp.int32, (8, 128), 0)
    for yy in range(NY):
        r = rank_ref[yy * 8:yy * 8 + 8]
        nat = r
        for d in range(1, 8):
            moved = pltpu.roll(pltpu.roll(r, 16 * d, 1), 8 - d, 0)
            nat = jnp.where(lax.rem(lane - sub + 8, 8) == d, moved, nat)
        nat_ref[pl.ds(yy, 8, stride=4), :] = nat
    out_rank = pltpu.make_async_copy(nat_ref, r_hbm, sem.at[8])
    out_rank.start()

    for i in range(8):
        out(i).wait()
    out_rank.wait()


def solution(mesh):
    D = pltpu.SemaphoreType.DMA
    VM = pltpu.VMEM

    def per_device(text_states, text_proj, gallery, logit_scale):
        e, fac, rank = pl.pallas_call(
            gather_score_kernel,
            out_shape=(VM((32, 128, 512), F32), VM((32, 128), F32), VM((32, 128), F32)),
            in_specs=[pl.BlockSpec(memory_space=pl.ANY)] * 4,
            out_specs=(pl.BlockSpec(memory_space=VM),) * 3,
            scratch_shapes=[
                VM((16, NZ, 16, 512), BF16), VM((512, 1024), BF16), VM((512, 1024), BF16),
                pltpu.SMEM((1,), F32), VM((9, 256, 1024), BF16), VM((9, 256, 1024), BF16), VM((512, 512), F32), VM((512, 512), F32),
                VM((32, 4, 128), F32), VM((32, 4, 128), F32), VM((NZ, 4, 128), F32), VM((32, 4, 128), F32),
                D((4,)), D((3,)), D((3,)), D((1,)), D((6,)), D((1,)), D((12,)), D((1,)), D((12,)),
                D((1,)), D((9,)), D((3,)), D((3,)),
            ],
            compiler_params=pltpu.CompilerParams(collective_id=0, has_side_effects=True,
                                                 vmem_limit_bytes=48 * 1024 * 1024),
        )(text_states, text_proj, gallery, logit_scale)
        prob, rank = pl.pallas_call(
            normalise_kernel,
            out_shape=(jax.ShapeDtypeStruct((NZ, 32, 16, 512), BF16), jax.ShapeDtypeStruct((32, 128), F32)),
            in_specs=[pl.BlockSpec(memory_space=VM)] * 3,
            out_specs=(pl.BlockSpec(memory_space=pl.ANY),) * 2,
            scratch_shapes=[VM((NZ, 32, 16, 512), BF16), VM((32, 128), F32), D((9,))],
            compiler_params=pltpu.CompilerParams(vmem_limit_bytes=24 * 1024 * 1024),
        )(e, fac, rank)
        return prob.reshape(4096, 512), rank.reshape(4096)

    return jax.shard_map(per_device, mesh=mesh,
                         in_specs=(P("ga", None), P(None, None), P("ga", None), P(None)),
                         out_specs=(P(None, "ga"), P(None)), check_vma=False)
```
